256 devices in a mesh: gx: 32 (over x, z), gy: 4 (over y), gz: 2 (over core).
Axes of the slice: x: 4, y: 4, z: 8, core: 2. Of those that a mesh axis runs over, the one named last changes fastest.
Arguments:
- coarse_field: float32 [3, 1024, 128, 512], P(None, 'gx', 'gy', 'gz'), may hold values from -6 to 6
- fine_field: float32 [3, 1024, 16, 256], P(None, ('gx', 'gy', 'gz')), may hold values from -6 to 6
- viscosity: float32 [1024, 16, 256], P(('gx', 'gy', 'gz')), may hold values from 0.1 to 1
- corners: int32 [512, 3], replicated, may hold values from 0 to 1016, as said below
- grid_slot: int32 [512], replicated, may hold values from 0 to 1023, as said below
- neighbors: int32 [512, 2], replicated, may hold values from -1 to 511, as said below
Outputs:
- fine_out: float32 [3, 1024, 16, 256], P(None, ('gx', 'gy', 'gz'))
- coarse_out: float32 [3, 1024, 128, 512], P(None, 'gx', 'gy', 'gz')
The draws below stay inside these ranges and needn't reach their ends.
Inputs may be any that keep to these rules, and one draw needn't show every extreme that they name: Each box is 8 coarse cells on a side, its corner coordinates are multiples of 8, it lies inside the domain and inside one coarse brick of 32 x 32 x 256 cells, and different grids have different boxes. A brick holds either no box or exactly 4 boxes, which share their y and z corners and are grids of one wake. `grid_slot`: different grids have different slots. A grid's slot lies on a device with the same gz index as the brick that holds its box. Every device holds at most 4 grids, some device holds 4 grids in every draw, and all grids of one device lie in one brick. `neighbors`: entry 0 is the grid of the same wake whose box touches the grid's lower x face, entry 1 the one touching its upper x face, or -1 where there is none.
All inputs are finite; a program needn't handle non-finite values.
Results may differ from the reference program's by a relative error of at most 0.00005.
Values sent between devices are 32-bit elements; how exact they have to be, the bound alone decides.
No kernel may reach another device: no remote copies, remote signals or barrier semaphores. Data moves between devices by JAX's collectives and lax.ppermute only.
A program may use at most 128 MiB of HBM per device.

```python
import math
import jax
import jax.numpy as jnp
from jax import lax

B = 8
F = 16
CY = 32
CZ = 256
SLOTS = 4
WAKE = 8
NX = 1024
NY = 128
NZ = 512
N_GX = 32
N_GY = 4
N_GZ = 2


def wind_layout(key):
    root_random_key = jax.random.fold_in(key, 4242)
    groups = N_GX * N_GY
    turbines = groups // 4
    half_x = N_GX // 2
    pair_count = groups // 2
    rows_z = CZ // B
    grid_count = turbines * WAKE
    corner_parts = []
    slot_parts = []
    near_parts = []
    for z_layer in range(N_GZ):
        subkeys = jax.random.split(jax.random.fold_in(root_random_key, z_layer), 7)
        pair_order = jax.random.permutation(subkeys[0], pair_count).astype(jnp.int32)
        first_pair = jax.random.randint(subkeys[1], (), half_x, pair_count, dtype=jnp.int32)
        found_at = jnp.argmax(pair_order == first_pair).astype(jnp.int32)
        pair_order = pair_order.at[found_at].set(pair_order[0]).at[0].set(first_pair)
        chosen = pair_order[:turbines]
        brick_row = chosen // half_x
        brick_first = 2 * (chosen % half_x)
        edge_z = rows_z - 1 if z_layer % 2 == 0 else 0
        inner_y = jax.random.randint(subkeys[2], (turbines,), 0, CY // B, dtype=jnp.int32).at[0].set(0)
        inner_z = jax.random.randint(subkeys[5], (turbines,), 0, rows_z, dtype=jnp.int32).at[0].set(edge_z)
        row_y = brick_row * (CY // B) + inner_y
        row_z = inner_z + z_layer * rows_z
        start_x = brick_first * SLOTS
        along_wake = jnp.arange(WAKE, dtype=jnp.int32)
        lattice_x = (start_x[:, None] + along_wake[None, :]).reshape(-1)
        lattice_y = jnp.repeat(row_y, WAKE)
        lattice_z = jnp.repeat(row_z, WAKE)
        corner_parts.append((jnp.stack([lattice_x, lattice_y, lattice_z], axis=1) * B).astype(jnp.int32))
        local_ids = jnp.arange(grid_count, dtype=jnp.int32)
        global_ids = local_ids + z_layer * grid_count
        in_wake = local_ids % WAKE
        near_parts.append(jnp.stack([jnp.where(in_wake > 0, global_ids - 1, -1), jnp.where(in_wake < WAKE - 1, global_ids + 1, -1)], axis=1).astype(jnp.int32))
        devices = jax.random.permutation(subkeys[3], groups).astype(jnp.int32)
        across = (devices[0] + groups // 2) % groups
        across_at = jnp.argmax(devices == across).astype(jnp.int32)
        devices = devices.at[across_at].set(devices[2]).at[2].set(across)
        second_share = jax.random.randint(subkeys[6], (), 1, SLOTS + 1, dtype=jnp.int32)
        shares = jax.random.randint(subkeys[4], (groups // 2,), 0, SLOTS + 1, dtype=jnp.int32).at[0].set(SLOTS).at[1].set(second_share)
        half_id = local_ids // SLOTS
        inside = local_ids % SLOTS
        share_limit = shares[half_id]
        owner_group = jnp.where(inside < share_limit, devices[2 * half_id], devices[2 * half_id + 1])
        owner_slot = jnp.where(inside < share_limit, inside, inside - share_limit)
        slot_parts.append(((owner_group * N_GZ + z_layer) * SLOTS + owner_slot).astype(jnp.int32))
    corner_table = jnp.concatenate(corner_parts, axis=0)
    slot_table = jnp.concatenate(slot_parts, axis=0)
    near_all = jnp.concatenate(near_parts, axis=0)
    total_count = corner_table.shape[0]
    renumbered_slots = jax.random.permutation(jax.random.fold_in(root_random_key, 777), total_count).astype(jnp.int32)
    inverse_permutation = jnp.argsort(renumbered_slots).astype(jnp.int32)
    mapped_neighbor_slots = jnp.where(near_all >= 0, inverse_permutation[jnp.maximum(near_all, 0)], -1).astype(jnp.int32)
    return (corner_table[renumbered_slots], slot_table[renumbered_slots], mapped_neighbor_slots[renumbered_slots])


def draw_corners(key, part):
    return wind_layout(key)[0]


def draw_grid_slot(key, part):
    return wind_layout(key)[1]


def draw_neighbors(key, part):
    return wind_layout(key)[2]


def steps_of(key, dims, pieces, least, high):
    def one(axis_at, shards_of):
        heights = jax.random.uniform(jax.random.fold_in(jax.random.fold_in(key, 6), axis_at), (shards_of,), jnp.float32, least / len(pieces), high / len(pieces))
        return jnp.repeat(jnp.exp(heights), dims[axis_at] // shards_of).reshape((-1,) + (1,) * (len(dims) - axis_at - 1))

    factor_of = one(*pieces[0])
    for cut in pieces[1:]:
        factor_of = factor_of * one(*cut)
    return factor_of


def centred(own_key, shape, scale, reach, pieces=(), held_as=jnp.bfloat16):
    result = scale * jax.random.normal(own_key, shape, jnp.float32)
    if pieces:
        result = result * steps_of(own_key, shape, pieces, -0.22, 0.18)
    return jnp.clip(result, -reach, reach).astype(held_as)


def setup_inputs(seed: int = 0) -> dict:
    keys = jax.random.split(jax.random.key(seed), 7)
    return {
        "coarse_field": centred(keys[0], (3, NX, NY, NZ), 1.0, 6.0, ((1, 32), (2, 4), (3, 2)), jnp.float32),
        "fine_field": centred(keys[1], (3, N_GX * N_GY * N_GZ * SLOTS, F, F * F), 1.0, 6.0, ((1, 256),), jnp.float32),
        "viscosity": jnp.clip(jnp.exp(math.log(1.0) - 2.3025851 * jax.random.uniform(keys[2], (N_GX * N_GY * N_GZ * SLOTS, F, F * F), jnp.float32) ** steps_of(keys[2], (N_GX * N_GY * N_GZ * SLOTS, F, F * F), ((0, 256),), -0.2, 0.2)), 0.1, 1.0),
        "corners": draw_corners(jax.random.fold_in(keys[6], 71), 0),
        "grid_slot": draw_grid_slot(jax.random.fold_in(keys[6], 71), 0),
        "neighbors": draw_neighbors(jax.random.fold_in(keys[6], 71), 0),
    }


step_rate = 0.15


def tables():
    side = B + 2
    fine_index = jnp.arange(F, dtype=jnp.int32)
    coarse_index = jnp.arange(side, dtype=jnp.int32)
    center = fine_index // 2 + 1
    other = jnp.where(fine_index % 2 == 0, center - 1, center + 1)
    tangent = 0.75 * (coarse_index[None, :] == center[:, None]).astype(jnp.float32) + 0.25 * (coarse_index[None, :] == other[:, None]).astype(jnp.float32)
    low_side = 0.75 * (coarse_index == 0).astype(jnp.float32) + 0.25 * (coarse_index == 1).astype(jnp.float32)
    high_side = 0.75 * (coarse_index == side - 1).astype(jnp.float32) + 0.25 * (coarse_index == side - 2).astype(jnp.float32)
    return tangent, low_side, high_side


def advance(volume, visc_cells, ghost_faces, lower_plane, upper_plane):
    components = volume.shape[0]
    slots_here = volume.shape[1]
    cells_edge = volume.shape[2]
    plane_size = volume.shape[3]
    lane_ids = jnp.arange(plane_size, dtype=jnp.int32)
    lane_y = lane_ids // cells_edge
    lane_z = lane_ids % cells_edge
    x_minus = jnp.concatenate([lower_plane[:, :, None], volume[:, :, :-1]], axis=2)
    x_plus = jnp.concatenate([volume[:, :, 1:], upper_plane[:, :, None]], axis=2)
    shape_four = (components, slots_here, cells_edge, cells_edge)
    y_low = jnp.tile(ghost_faces[:, :, 2].reshape(shape_four), (1, 1, 1, cells_edge))
    y_high = jnp.tile(ghost_faces[:, :, 3].reshape(shape_four), (1, 1, 1, cells_edge))
    z_low = jnp.repeat(ghost_faces[:, :, 4].reshape(shape_four), cells_edge, axis=3)
    z_high = jnp.repeat(ghost_faces[:, :, 5].reshape(shape_four), cells_edge, axis=3)
    zero_row = jnp.zeros_like(volume[..., :cells_edge])
    zero_cell = jnp.zeros_like(volume[..., :1])
    y_minus = jnp.where(lane_y == 0, y_low, jnp.concatenate([zero_row, volume[..., :-cells_edge]], axis=-1))
    y_plus = jnp.where(lane_y == cells_edge - 1, y_high, jnp.concatenate([volume[..., cells_edge:], zero_row], axis=-1))
    z_minus = jnp.where(lane_z == 0, z_low, jnp.concatenate([zero_cell, volume[..., :-1]], axis=-1))
    z_plus = jnp.where(lane_z == cells_edge - 1, z_high, jnp.concatenate([volume[..., 1:], zero_cell], axis=-1))
    neighbor_sum = x_minus + x_plus + y_minus + y_plus + z_minus + z_plus - 6.0 * volume
    return volume + step_rate * visc_cells[None] * neighbor_sum


def reference(coarse_field, fine_field, viscosity, corners, grid_slot, neighbors):
    slot_total = fine_field.shape[1]
    grid_total = corners.shape[0]
    grid_ids = jnp.arange(grid_total, dtype=jnp.int32)
    slot_ids = jnp.arange(slot_total, dtype=jnp.int32)
    slot_match = grid_slot[None, :] == slot_ids[:, None]
    slot_active = jnp.any(slot_match, axis=1)
    slot_grid = jnp.sum(jnp.where(slot_match, grid_ids[None, :], 0), axis=1).astype(jnp.int32)
    box_corner = corners[slot_grid].astype(jnp.int32)
    padded = jnp.pad(coarse_field, ((0, 0), (1, 1), (1, 1), (1, 1)))
    zero_start = jnp.zeros((), jnp.int32)

    def cut_cube(corner):
        return lax.dynamic_slice(padded, (zero_start, corner[0], corner[1], corner[2]), (3, B + 2, B + 2, B + 2))

    cubes = jax.vmap(cut_cube)(box_corner)
    tangent, low_side, high_side = tables()
    highest = lax.Precision.HIGHEST
    face_list = [
        jnp.einsum('nkabc,a,sb,tc->knst', cubes, low_side, tangent, tangent, precision=highest),
        jnp.einsum('nkabc,a,sb,tc->knst', cubes, high_side, tangent, tangent, precision=highest),
        jnp.einsum('nkabc,sa,b,tc->knst', cubes, tangent, low_side, tangent, precision=highest),
        jnp.einsum('nkabc,sa,b,tc->knst', cubes, tangent, high_side, tangent, precision=highest),
        jnp.einsum('nkabc,sa,tb,c->knst', cubes, tangent, tangent, low_side, precision=highest),
        jnp.einsum('nkabc,sa,tb,c->knst', cubes, tangent, tangent, high_side, precision=highest),
    ]
    ghost_faces = jnp.stack([face.reshape(3, slot_total, F * F) for face in face_list], axis=2)
    near_grid = neighbors[slot_grid]
    near_slot = grid_slot[jnp.maximum(near_grid, 0)]
    from_low = fine_field[:, near_slot[:, 0], F - 1, :]
    from_high = fine_field[:, near_slot[:, 1], 0, :]
    has_near = (near_grid >= 0) & slot_active[:, None]
    lower_plane = jnp.where(has_near[None, :, 0, None], from_low, ghost_faces[:, :, 0])
    upper_plane = jnp.where(has_near[None, :, 1, None], from_high, ghost_faces[:, :, 1])
    advanced = advance(fine_field, viscosity, ghost_faces, lower_plane, upper_plane)
    fine_out = jnp.where(slot_active[None, :, None, None], advanced, 0.0)
    averages = advanced.reshape(3, slot_total, B, 2, B, 2, B, 2).mean(axis=(3, 5, 7))

    def place_box(index, field_now):
        corner = box_corner[index]
        start = (zero_start, corner[0], corner[1], corner[2])
        current = lax.dynamic_slice(field_now, start, (3, B, B, B))
        value = jnp.where(slot_active[index], averages[:, index], current)
        return lax.dynamic_update_slice(field_now, value, start)

    coarse_out = lax.fori_loop(0, slot_total, place_box, coarse_field)
    return fine_out, coarse_out
```

```python
import functools

import jax
import jax.numpy as jnp
import numpy as np
from jax import lax
from jax.experimental import pallas as pl
from jax.experimental.pallas import tpu as pltpu
from jax.sharding import Mesh
from jax.sharding import PartitionSpec as P

B = 8
F = 16
SLOTS = 4
SIDE = B + 2
LINE_X = 4
LINE_Z = 8
LINE_Y = 4
PLANE = LINE_X * LINE_Y
HALO = 7
SEND = HALO + 8
HIGHEST = lax.Precision.HIGHEST
step_rate = 0.15
f32 = jnp.float32
i32 = jnp.int32
GX = ("gx_0", "gx_1")
GX_GY_GZ = ("gx_0", "gx_1", "gy", "gz")

ROW_SLOT, ROW_HOME, ROW_LOW, ROW_HIGH, ROW_OWNER, ROW_ANCHOR = range(6)
SELF_TARGET = 8


def tangent_matrix():
    fine = np.arange(F)
    coarse = np.arange(SIDE)
    center = fine // 2 + 1
    other = np.where(fine % 2 == 0, center - 1, center + 1)
    return 0.75 * (coarse[None] == center[:, None]) + 0.25 * (coarse[None] == other[:, None])


def constant_matrices():
    tangent = tangent_matrix()
    along_x = np.zeros((64, 40))
    for fine in range(64):
        center = fine // 2
        other = center - 1 if fine % 2 == 0 else center + 1
        along_x[fine, center] += 0.75
        along_x[fine, 32 if other < 0 else 33 if other > 31 else other] += 0.25
    faces = np.zeros((128, 3, F, F))
    for k in range(3):
        for c in range(SIDE):
            faces[k * 10 + c, k, 0, :] += tangent[:, c]
            faces[30 + k * 10 + c, k, F - 1, :] += tangent[:, c]
            faces[60 + k * 10 + c, k, :, 0] += tangent[:, c]
            faces[90 + k * 10 + c, k, :, F - 1] += tangent[:, c]
    ends = np.zeros((128, F * F))
    ends[: SIDE * SIDE] = np.einsum("sa,tb->abst", tangent, tangent).reshape(SIDE * SIDE, F * F)
    pool = np.zeros((2, F, F, 128))
    for y in range(F):
        for z in range(F):
            for half in range(2):
                pool[half, y, z, half * 64 + (y // 2) * B + z // 2] = 0.125
    return (
        along_x.astype(np.float32),
        faces.reshape(128, 3 * F * F).astype(np.float32),
        ends.astype(np.float32),
        pool.reshape(2, F * F, 128).astype(np.float32),
    )


def position():
    return tuple(lax.axis_index(name) for name in GX_GY_GZ)


def make_table(corners_ref, slots_ref, near_ref, table_ref):
    my_x, my_z, my_y, my_c = position()
    cx, cy, cz = corners_ref[0:1, :], corners_ref[1:2, :], corners_ref[2:3, :]
    gs = slots_ref[0:1, :]
    grids = gs.shape[1]
    low, high = near_ref[0:1, :], near_ref[1:2, :]
    gx, gy, gz = cx >> 5, cy >> 5, cz >> 8
    box = (cx >> 3) & 3
    home = gx * LINE_Y + gy
    brick_key = (home * 2 + gz) * SLOTS + box
    word = (1 + box * 2 + home * 8 + (low + 1) * 1024).astype(f32)
    sub = lax.broadcasted_iota(i32, (64, 1), 0)
    eye = (lax.broadcasted_iota(i32, (64, 128), 0) == lax.broadcasted_iota(i32, (64, 128), 1)).astype(f32)

    def to_row(column):
        return jnp.sum(eye * column, axis=0, keepdims=True)

    def pick(match, values):
        return jnp.sum(jnp.where(match, values, 0.0), axis=1, keepdims=True)

    def device_of(j):
        return (((j >> 2) * LINE_Z + my_z) * LINE_Y + (j & 3)) * 2 + my_c

    keys = device_of(sub >> 2) * SLOTS + (sub & 3)
    held = keys == gs
    words = pick(held, word)
    high_grid = pick(held, (high + 1).astype(f32)).astype(i32)
    low_grid = words.astype(i32) >> 10
    grid_ids = lax.broadcasted_iota(i32, (1, grids), 1) + 1
    slot_plus = (gs + 1).astype(f32)
    low_slot = pick(low_grid == grid_ids, slot_plus)
    high_slot = pick(high_grid == grid_ids, slot_plus)
    owner = pick(keys == brick_key, slot_plus)
    sub16 = lax.broadcasted_iota(i32, (16, 1), 0)
    on_device = device_of(sub16) == (gs >> 2)
    homes = jnp.max(jnp.where(on_device, (home + 1).astype(f32), 0.0), axis=1, keepdims=True)
    homes = jnp.concatenate([homes, jnp.zeros((48, 1), f32)], axis=0)
    sub24 = lax.broadcasted_iota(i32, (24, 1), 0)
    target_x = my_x * LINE_Z + my_z + jnp.where(sub24 >= 12, 1, jnp.where(sub24 >= 6, 0, -1))
    target_x = jnp.where(sub24 >= 18, -1, target_x)
    in_x = sub24 - jnp.where(sub24 >= 12, 12, jnp.where(sub24 >= 6, 6, 0))
    target_y = my_y + (in_x >> 1) - 1
    target_z = jnp.where((in_x & 1) == 0, my_c, 1 - my_c)
    near_brick = (target_x == gx) & (target_y == gy) & (target_z == gz)
    place = ((cy & 31) * 256 + (cz & 255)).astype(f32)
    anchors = jnp.max(jnp.where(near_brick, place, -1.0), axis=1, keepdims=True)
    anchors = jnp.concatenate([anchors, jnp.zeros((40, 1), f32)], axis=0)
    rows = [to_row(v) for v in (words, homes, low_slot, high_slot, owner, anchors)]
    for r, row in enumerate(rows):
        table_ref[r : r + 1, :] = row.astype(i32)
    table_ref[6:8, :] = jnp.zeros((2, 128), i32)


def pack_kernel(
    corners_ref, slots_ref, near_ref, fine_ref, coarse_ref,
    table_ref, own_ref, other_ref, planes_ref, copy_ref,
    brick, table, load_sems, store_sems, table_sem,
):
    loads, stores = [], []
    for k in range(3):
        for half in range(2):
            rows, lanes = pl.ds(k * 1024, 1024), pl.ds(half * 128, 128)
            inner = brick.at[half, rows]
            loads.append(pltpu.make_async_copy(coarse_ref.at[rows, lanes], inner, load_sems.at[k * 2 + half]))
            stores.append(pltpu.make_async_copy(inner, copy_ref.at[rows, lanes], store_sems.at[k * 2 + half]))
    for copy in loads:
        copy.start()
    make_table(corners_ref, slots_ref, near_ref, table_ref)
    fetch = pltpu.make_async_copy(table_ref, table, table_sem)
    fetch.start()
    own_ref[...] = jnp.zeros_like(own_ref)
    other_ref[...] = jnp.zeros_like(other_ref)
    planes_ref[...] = jnp.zeros_like(planes_ref)
    for side in range(2):
        for s in range(SLOTS):
            for k in range(3):
                row = (k * SLOTS + s) * F + (F - 1 if side == 0 else 0)
                for half in range(2):
                    at = (side * SLOTS + s) * 8 + half * 3 + k
                    planes_ref[at : at + 1, :] = fine_ref[row : row + 1, half * 128 : half * 128 + 128]
    fetch.wait()
    for load, store in zip(loads, stores):
        load.wait()
        store.start()

    my_c = lax.axis_index("gz")
    lane = lax.broadcasted_iota(i32, (1, 128), 1)
    sub3 = lax.broadcasted_iota(i32, (3, 1), 0)

    def shifted(start, count, stride, z_base, valid):
        rows = jnp.concatenate(
            [brick.at[half][pl.ds(start, count, stride=stride), :] for half in range(2)], axis=1
        )
        rows = pltpu.roll(rows, (256 - z_base) & 255, 1)[:, :128]
        at = z_base + lane
        keep = (lane < SIDE) & (at >= 0) & (at < 256) & valid
        return jnp.where(keep, rows, 0.0)

    def layers(dy, y0):
        if dy == 0:
            for t in range(SIDE):
                y = y0 - 1 + t
                valid = True if 0 < t < SIDE - 1 else (y >= 0) & (y < 32)
                yield t, jnp.clip(y, 0, 31), valid
        elif dy == 1:
            yield 0, 31, y0 == 0
        else:
            yield SIDE - 1, 0, y0 == 24

    weights = {0: (0.75, 0), 1: (0.25, 0), SIDE - 2: (0.25, 30), SIDE - 1: (0.75, 30)}

    def ends_of(u):
        low = 0.75 * u[:, 0:1] + 0.25 * u[:, 1:2]
        high = 0.75 * u[:, 9:10] + 0.25 * u[:, 8:9]
        return low, high

    def main_rows(dy, y0, z_base):
        total = jnp.zeros((32, 128), f32)
        for t, y, valid in layers(dy, y0):
            for k in range(3):
                u = shifted(k * 1024 + y, 32, 32, z_base, valid)
                low, high = ends_of(u)
                total = jnp.where(lane == 60 + 10 * k + t, low, total)
                total = jnp.where(lane == 90 + 10 * k + t, high, total)
                if t in weights:
                    w, face = weights[t]
                    total = total + w * (pltpu.roll(u, face + 10 * k, 1) if face + k else u)
        return total

    def edge_rows(x, dy, y0, z_base, with_row):
        flat = jnp.zeros((3, 128), f32)
        row = jnp.zeros((3, 128), f32)
        for t, y, valid in layers(dy, y0):
            u = shifted(x * 32 + y, 3, 1024, z_base, valid)
            flat = flat + (pltpu.roll(u, 10 * t, 1) if t else u)
            if with_row:
                low, high = ends_of(u)
                row = jnp.where(lane == 60 + 10 * sub3 + t, low, row)
                row = jnp.where(lane == 90 + 10 * sub3 + t, high, row)
                if t in weights:
                    w, face = weights[t]
                    spread = jnp.where(
                        sub3 == 0,
                        pltpu.roll(u, face, 1) if face else u,
                        jnp.where(sub3 == 1, pltpu.roll(u, face + 10, 1), pltpu.roll(u, face + 20, 1)),
                    )
                    row = row + w * spread
        return flat, jnp.sum(row, axis=0, keepdims=True)

    for dz in range(2):
        out = other_ref if dz else own_ref
        z_shift = 256 * (1 - 2 * my_c) if dz else 0
        for dy in (-1, 0, 1):
            base = (dy + 1) * HALO * 8
            for dx in (0, -1, 1):
                place = table[ROW_ANCHOR, (dx + 1) * 6 + (dy + 1) * 2 + dz]
                y0, z0 = place >> 8, place & 255
                z_base = z0 - 1 + z_shift
                near = place >= 0
                if dy == 1:
                    near &= y0 == 0
                if dy == -1:
                    near &= y0 == 24
                if dz:
                    near &= z0 == jnp.where(my_c == 0, 0, 248)

                @pl.when(near)
                def _(out=out, base=base, dx=dx, dy=dy, y0=y0, z_base=z_base):
                    if dx == 0:
                        out[base : base + 32, :] = main_rows(dy, y0, z_base)
                        for x, at in ((0, 0), (31, 3)):
                            flat, _row = edge_rows(x, dy, y0, z_base, False)
                            out[base + 32 + at : base + 35 + at, :] = 0.25 * flat
                    else:
                        x, at, tile = (0, 3, 40) if dx == -1 else (31, 0, 48)
                        flat, row = edge_rows(x, dy, y0, z_base, True)
                        out[base + tile + at : base + tile + at + 3, :] = 0.75 * flat
                        out[base + tile + 6 : base + tile + 7, :] = row

    for store in stores:
        store.wait()


def split_slot(slot):
    device = slot >> 2
    return device >> 6, (device >> 3) & 7, (device >> 1) & 3, slot & 3


def route_kernel(table, held, out):
    for j in range(PLANE):
        home = jnp.maximum(table[ROW_HOME, j] - 1, 0)
        gx = home >> 2
        z = gx & 7
        out[j, 0:40] = held[z, 0:40]
        out[j, 40:48] = held[(z + 7) & 7, 48:56]
        out[j, 48:56] = held[(z + 1) & 7, 40:48]
        for s in range(SLOTS):
            for side, row in enumerate((ROW_LOW, ROW_HIGH)):
                _, z, _, local = split_slot(jnp.maximum(table[row, j * 4 + s] - 1, 0))
                start = pl.multiple_of((HALO + side * SLOTS + local) * 8, 8)
                at = (HALO + side * SLOTS + s) * 8
                out[j, at : at + 8] = held[z, pl.ds(start, 8)]


def update_kernel(
    table, rcv, fine_ref, visc_ref, along_x, faces, ends, pool,
    fine_out, means_out,
    sums, planes, advanced, pooled,
):
    my_x, _, my_y, _ = position()
    me = my_x * LINE_Y + my_y
    home = jnp.maximum(table[ROW_HOME, me] - 1, 0)
    gx, hy = home >> 2, home & 3
    at_home = (gx >> 3) * LINE_Y + hy
    at_low = (jnp.maximum(gx - 1, 0) >> 3) * LINE_Y + hy
    at_high = (jnp.minimum(gx + 1, 31) >> 3) * LINE_Y + hy
    low = jnp.where(gx > 0, rcv[at_low, 40:48], 0.0)
    high = jnp.where(gx < 31, rcv[at_high, 48:56], 0.0)
    sub8 = lax.broadcasted_iota(i32, (8, 1), 0)
    beyond = jnp.where(sub8 == 0, low[6:7], jnp.where(sub8 == 1, high[6:7], 0.0))
    body = jnp.concatenate([rcv[at_home, 0:32], beyond], axis=0)
    dot = functools.partial(jnp.dot, precision=HIGHEST, preferred_element_type=f32)
    sums[...] = dot(dot(along_x[...], body), faces[...])
    flat = rcv[at_home, 32:40] + jnp.where(sub8 < 3, low, 0.0) + jnp.where((sub8 >= 3) & (sub8 < 6), high, 0.0)
    planes[...] = dot(flat, ends[...])
    lane = lax.broadcasted_iota(i32, (1, F * F), 1)
    sub = lax.broadcasted_iota(i32, (F, 1), 0)
    lane_z = lane & (F - 1)
    for s in range(SLOTS):
        word = table[ROW_SLOT, me * 4 + s]
        active = (word & 1) == 1
        box_start = pl.multiple_of(((word >> 1) & 3) * F, F)
        low_slot = table[ROW_LOW, me * 4 + s] - 1
        high_slot = table[ROW_HIGH, me * 4 + s] - 1
        lx, _, ly, _ = split_slot(jnp.maximum(low_slot, 0))
        hx, _, hy2, _ = split_slot(jnp.maximum(high_slot, 0))
        low_at, high_at = (HALO + s) * 8, (HALO + SLOTS + s) * 8
        low_tile = rcv[lx * LINE_Y + ly, low_at : low_at + 8]
        high_tile = rcv[hx * LINE_Y + hy2, high_at : high_at + 8]
        visc = step_rate * visc_ref[s * F : s * F + F, :]
        for k in range(3):
            row = (k * SLOTS + s) * F
            cells = fine_ref[row : row + F, :]
            lower = jnp.concatenate([low_tile[k : k + 1], low_tile[3 + k : 4 + k]], axis=1)
            upper = jnp.concatenate([high_tile[k : k + 1], high_tile[3 + k : 4 + k]], axis=1)
            lower = jnp.where(low_slot >= 0, lower, planes[k : k + 1, :])
            upper = jnp.where(high_slot >= 0, upper, planes[3 + k : 4 + k, :])
            total = sums[pl.ds(box_start, F), k * 256 : k * 256 + 256] - 6.0 * cells
            total = total + jnp.where(sub == 0, lower, pltpu.roll(cells, 1, 0))
            total = total + jnp.where(sub == F - 1, upper, pltpu.roll(cells, F - 1, 0))
            total = total + jnp.where(lane < F, 0.0, pltpu.roll(cells, F, 1))
            total = total + jnp.where(lane >= F * F - F, 0.0, pltpu.roll(cells, F * F - F, 1))
            total = total + jnp.where(lane_z == 0, 0.0, pltpu.roll(cells, 1, 1))
            total = total + jnp.where(lane_z == F - 1, 0.0, pltpu.roll(cells, F * F - 1, 1))
            result = cells + visc * total
            fine_out[row : row + F, :] = jnp.where(active, result, 0.0)
            at = s * 48 + k * F
            advanced[at : at + F, :] = result
    for p in range(2):
        at = p * 96
        pooled[p * 48 : p * 48 + 48, :] = dot(advanced[at : at + 48, :], pool[0]) + dot(
            advanced[at + 48 : at + 96, :], pool[1]
        )
    means = pooled[pl.ds(0, 48, stride=2), :] + pooled[pl.ds(1, 48, stride=2), :]
    for z in range(LINE_Z):
        means_out[z] = means


def return_kernel(table, held, out):
    first = lax.broadcasted_iota(i32, (1, 128), 1) < 64
    for j in range(PLANE):
        for p in range(2):
            picks = []
            for h in range(2):
                _, z, _, local = split_slot(jnp.maximum(table[ROW_OWNER, j * 4 + 2 * p + h] - 1, 0))
                start = pl.multiple_of((local >> 1) * 24, 8)
                rows = held[z, pl.ds(start, 24)]
                picks.append(jnp.where((local & 1) == h, rows, pltpu.roll(rows, 64, 1)))
            out[j, p * 24 : p * 24 + 24] = jnp.where(first, picks[0], picks[1])


def place_kernel(table, rcv, coarse_ref, coarse_out, window, spread, sem):
    my_x, _, my_y, _ = position()
    me = my_x * LINE_Y + my_y
    place = table[ROW_ANCHOR, SELF_TARGET]

    @pl.when(place >= 0)
    def _():
        y0 = pl.multiple_of(place >> 8, 8)
        z0 = place & 255
        z_tile = pl.multiple_of((z0 >> 7) * 128, 128)
        z_in = z0 & 127
        region = coarse_out.at[:, pl.ds(y0, 8), pl.ds(z_tile, 128)]
        load = pltpu.make_async_copy(region, window, sem.at[0])
        load.start()
        for i in range(SLOTS):
            ox, _, oy, _ = split_slot(jnp.maximum(table[ROW_OWNER, me * 4 + i] - 1, 0))
            at = ox * LINE_Y + oy
            for k in range(3):
                start = ((i // 2) * 3 + k) * 8
                values = rcv[at, start : start + 8]
                for b in range(B):
                    shift = (z_in + 256 - (b * B + 64 * (i % 2))) & 127
                    spread[pl.ds((k * 32 + i * B) * B + b, B, stride=B), :] = pltpu.roll(values, shift, 1)
        load.wait()
        lane = lax.broadcasted_iota(i32, (1, 1, 128), 2)
        fresh = spread[...].reshape(96, 8, 128)
        window[...] = jnp.where((lane >= z_in) & (lane < z_in + B), fresh, window[...])
        store = pltpu.make_async_copy(window, region, sem.at[1])
        store.start()
        store.wait()


def vmem():
    return pl.BlockSpec(memory_space=pltpu.VMEM)


def smem():
    return pl.BlockSpec(memory_space=pltpu.SMEM)


def anywhere():
    return pl.BlockSpec(memory_space=pl.ANY)


def shape(*dims, dtype=f32):
    return jax.ShapeDtypeStruct(dims, dtype)


def on_device(coarse_field, fine_field, viscosity, corners, grid_slot, neighbors):
    fine = fine_field.reshape(3 * SLOTS * F, F * F)
    table, own, other, planes, copied = pl.pallas_call(
        pack_kernel,
        out_shape=(
            shape(8, 128, dtype=i32),
            shape(3 * HALO * 8, 128),
            shape(3 * HALO * 8, 128),
            shape(64, 128),
            shape(3072, 256),
        ),
        in_specs=[vmem(), vmem(), vmem(), vmem(), anywhere()],
        out_specs=(vmem(), vmem(), vmem(), vmem(), anywhere()),
        scratch_shapes=[
            pltpu.VMEM((2, 3072, 128), f32),
            pltpu.SMEM((8, 128), i32),
            pltpu.SemaphoreType.DMA((6,)),
            pltpu.SemaphoreType.DMA((6,)),
            pltpu.SemaphoreType.DMA(()),
        ],
        name="pack",
    )(corners.T, grid_slot[None, :], neighbors.T, fine, coarse_field.reshape(3072, 256))
    halo = own + lax.ppermute(other, "gz", [(0, 1), (1, 0)])
    halo = halo.reshape(3, HALO * 8, 128)
    above = lax.ppermute(halo[2], "gy", [(i, i + 1) for i in range(LINE_Y - 1)])
    below = lax.ppermute(halo[0], "gy", [(i + 1, i) for i in range(LINE_Y - 1)])
    payload = jnp.concatenate([halo[1] + above + below, planes], axis=0)
    held = lax.all_to_all(jnp.broadcast_to(payload, (LINE_Z, SEND * 8, 128)), "gx_1", 0, 0)
    routed = pl.pallas_call(
        route_kernel,
        out_shape=shape(PLANE, SEND * 8, 128),
        in_specs=[smem(), vmem()],
        out_specs=vmem(),
        name="route",
    )(table, held)
    received = lax.all_to_all(routed, ("gx_0", "gy"), 0, 0)
    fine_out, means = pl.pallas_call(
        update_kernel,
        out_shape=(shape(3 * SLOTS * F, F * F), shape(LINE_Z, 48, 128)),
        in_specs=[smem()] + [vmem()] * 7,
        out_specs=(vmem(), vmem()),
        scratch_shapes=[
            pltpu.VMEM((64, 768), f32),
            pltpu.VMEM((8, 256), f32),
            pltpu.VMEM((192, 256), f32),
            pltpu.VMEM((96, 128), f32),
        ],
        name="update",
    )(table, received, fine, viscosity.reshape(SLOTS * F, F * F), *map(jnp.asarray, constant_matrices()))
    held_means = lax.all_to_all(means, "gx_1", 0, 0)
    back = pl.pallas_call(
        return_kernel,
        out_shape=shape(PLANE, 48, 128),
        in_specs=[smem(), vmem()],
        out_specs=vmem(),
        name="send_back",
    )(table, held_means)
    returned = lax.all_to_all(back, ("gx_0", "gy"), 0, 0)
    coarse_out = pl.pallas_call(
        place_kernel,
        out_shape=shape(96, 32, 256),
        in_specs=[smem(), vmem(), anywhere()],
        out_specs=anywhere(),
        input_output_aliases={2: 0},
        scratch_shapes=[
            pltpu.VMEM((96, 8, 128), f32),
            pltpu.VMEM((768, 128), f32),
            pltpu.SemaphoreType.DMA((2,)),
        ],
        name="place",
    )(table, returned, copied.reshape(96, 32, 256))
    return fine_out.reshape(fine_field.shape), coarse_out.reshape(coarse_field.shape)


def solution(mesh):
    split = Mesh(
        mesh.devices.reshape(LINE_X, LINE_Z, mesh.shape["gy"], mesh.shape["gz"]), ("gx_0", "gx_1", "gy", "gz")
    )
    in_specs = (
        P(None, GX, "gy", "gz"),
        P(None, GX_GY_GZ, None, None),
        P(GX_GY_GZ, None, None),
        P(),
        P(),
        P(),
    )
    out_specs = (P(None, GX_GY_GZ, None, None), P(None, GX, "gy", "gz"))
    return jax.shard_map(
        on_device, mesh=split, in_specs=in_specs, out_specs=out_specs, check_vma=False
    )
```

```python
import functools

import jax
import jax.numpy as jnp
import numpy as np
from jax import lax
from jax.experimental import pallas as pl
from jax.experimental.pallas import tpu as pltpu
from jax.sharding import Mesh
from jax.sharding import PartitionSpec as P

B = 8
F = 16
SLOTS = 4
SIDE = B + 2
LINE_X = 4
LINE_Z = 8
LINE_Y = 4
PLANE = LINE_X * LINE_Y
HALO = 7
SEND = HALO + 8
HIGHEST = lax.Precision.HIGHEST
step_rate = 0.15
f32 = jnp.float32
i32 = jnp.int32
GX = ("gx_0", "gx_1")
GX_GY_GZ = ("gx_0", "gx_1", "gy", "gz")

ROW_SLOT, ROW_HOME, ROW_LOW, ROW_HIGH, ROW_OWNER, ROW_ANCHOR = range(6)
SELF_TARGET = 8


def tangent_matrix():
    fine = np.arange(F)
    coarse = np.arange(SIDE)
    center = fine // 2 + 1
    other = np.where(fine % 2 == 0, center - 1, center + 1)
    return 0.75 * (coarse[None] == center[:, None]) + 0.25 * (coarse[None] == other[:, None])


def constant_matrices():
    tangent = tangent_matrix()
    along_x = np.zeros((64, 40))
    for fine in range(64):
        center = fine // 2
        other = center - 1 if fine % 2 == 0 else center + 1
        along_x[fine, center] += 0.75
        along_x[fine, 32 if other < 0 else 33 if other > 31 else other] += 0.25
    faces = np.zeros((128, 3, F, F))
    for k in range(3):
        for c in range(SIDE):
            faces[k * 10 + c, k, 0, :] += tangent[:, c]
            faces[30 + k * 10 + c, k, F - 1, :] += tangent[:, c]
            faces[60 + k * 10 + c, k, :, 0] += tangent[:, c]
            faces[90 + k * 10 + c, k, :, F - 1] += tangent[:, c]
    ends = np.zeros((128, F * F))
    ends[: SIDE * SIDE] = np.einsum("sa,tb->abst", tangent, tangent).reshape(SIDE * SIDE, F * F)
    pool = np.zeros((2, F, F, 128))
    for y in range(F):
        for z in range(F):
            for half in range(2):
                pool[half, y, z, half * 64 + (y // 2) * B + z // 2] = 0.125
    return (
        along_x.astype(np.float32),
        faces.reshape(128, 3 * F * F).astype(np.float32),
        ends.astype(np.float32),
        pool.reshape(2, F * F, 128).astype(np.float32),
    )


def position():
    return tuple(lax.axis_index(name) for name in GX_GY_GZ)


def make_table(corners_ref, slots_ref, near_ref, table_ref):
    my_x, my_z, my_y, my_c = position()
    cx, cy, cz = corners_ref[0:1, :], corners_ref[1:2, :], corners_ref[2:3, :]
    gs = slots_ref[0:1, :]
    grids = gs.shape[1]
    low, high = near_ref[0:1, :], near_ref[1:2, :]
    gx, gy, gz = cx >> 5, cy >> 5, cz >> 8
    box = (cx >> 3) & 3
    home = gx * LINE_Y + gy
    brick_key = (home * 2 + gz) * SLOTS + box
    word = (1 + box * 2 + home * 8 + (low + 1) * 1024).astype(f32)
    sub = lax.broadcasted_iota(i32, (64, 1), 0)
    eye = (lax.broadcasted_iota(i32, (64, 128), 0) == lax.broadcasted_iota(i32, (64, 128), 1)).astype(f32)

    def to_row(column):
        return jnp.sum(eye * column, axis=0, keepdims=True)

    def pick(match, values):
        return jnp.sum(jnp.where(match, values, 0.0), axis=1, keepdims=True)

    def device_of(j):
        return (((j >> 2) * LINE_Z + my_z) * LINE_Y + (j & 3)) * 2 + my_c

    keys = device_of(sub >> 2) * SLOTS + (sub & 3)
    held = keys == gs
    words = pick(held, word)
    high_grid = pick(held, (high + 1).astype(f32)).astype(i32)
    low_grid = words.astype(i32) >> 10
    grid_ids = lax.broadcasted_iota(i32, (1, grids), 1) + 1
    slot_plus = (gs + 1).astype(f32)
    low_slot = pick(low_grid == grid_ids, slot_plus)
    high_slot = pick(high_grid == grid_ids, slot_plus)
    owner = pick(keys == brick_key, slot_plus)
    sub16 = lax.broadcasted_iota(i32, (16, 1), 0)
    on_device = device_of(sub16) == (gs >> 2)
    homes = jnp.max(jnp.where(on_device, (home + 1).astype(f32), 0.0), axis=1, keepdims=True)
    homes = jnp.concatenate([homes, jnp.zeros((48, 1), f32)], axis=0)
    sub24 = lax.broadcasted_iota(i32, (24, 1), 0)
    target_x = my_x * LINE_Z + my_z + jnp.where(sub24 >= 12, 1, jnp.where(sub24 >= 6, 0, -1))
    target_x = jnp.where(sub24 >= 18, -1, target_x)
    in_x = sub24 - jnp.where(sub24 >= 12, 12, jnp.where(sub24 >= 6, 6, 0))
    target_y = my_y + (in_x >> 1) - 1
    target_z = jnp.where((in_x & 1) == 0, my_c, 1 - my_c)
    near_brick = (target_x == gx) & (target_y == gy) & (target_z == gz)
    place = ((cy & 31) * 256 + (cz & 255)).astype(f32)
    anchors = jnp.max(jnp.where(near_brick, place, -1.0), axis=1, keepdims=True)
    anchors = jnp.concatenate([anchors, jnp.zeros((40, 1), f32)], axis=0)
    rows = [to_row(v) for v in (words, homes, low_slot, high_slot, owner, anchors)]
    for r, row in enumerate(rows):
        table_ref[r : r + 1, :] = row.astype(i32)
    table_ref[6:8, :] = jnp.zeros((2, 128), i32)


def pack_kernel(
    corners_ref, slots_ref, near_ref, fine_ref, brick,
    table_ref, own_ref, other_ref, planes_ref,
    table, table_sem,
):
    make_table(corners_ref, slots_ref, near_ref, table_ref)
    fetch = pltpu.make_async_copy(table_ref, table, table_sem)
    fetch.start()
    own_ref[...] = jnp.zeros_like(own_ref)
    other_ref[...] = jnp.zeros_like(other_ref)
    planes_ref[...] = jnp.zeros_like(planes_ref)
    for side in range(2):
        for s in range(SLOTS):
            for k in range(3):
                row = (k * SLOTS + s) * F + (F - 1 if side == 0 else 0)
                for half in range(2):
                    at = (side * SLOTS + s) * 8 + half * 3 + k
                    planes_ref[at : at + 1, :] = fine_ref[row : row + 1, half * 128 : half * 128 + 128]
    fetch.wait()

    my_c = lax.axis_index("gz")
    lane = lax.broadcasted_iota(i32, (1, 128), 1)
    sub3 = lax.broadcasted_iota(i32, (3, 1), 0)

    def shifted(start, count, stride, z_base, valid):
        rows = jnp.concatenate(
            [brick[pl.ds(start + 8 * half, count, stride=stride), :] for half in range(2)], axis=1
        )
        rows = pltpu.roll(rows, (256 - z_base) & 255, 1)[:, :128]
        at = z_base + lane
        keep = (lane < SIDE) & (at >= 0) & (at < 256) & valid
        return jnp.where(keep, rows, 0.0)

    def tile_row(y):
        return (y >> 3) * 16 + (y & 7)

    def layers(dy, y0):
        if dy == 0:
            for t in range(SIDE):
                y = y0 - 1 + t
                valid = True if 0 < t < SIDE - 1 else (y >= 0) & (y < 32)
                yield t, jnp.clip(y, 0, 31), valid
        elif dy == 1:
            yield 0, 31, y0 == 0
        else:
            yield SIDE - 1, 0, y0 == 24

    weights = {0: (0.75, 0), 1: (0.25, 0), SIDE - 2: (0.25, 30), SIDE - 1: (0.75, 30)}

    def ends_of(u):
        low = 0.75 * u[:, 0:1] + 0.25 * u[:, 1:2]
        high = 0.75 * u[:, 9:10] + 0.25 * u[:, 8:9]
        return low, high

    def main_rows(dy, y0, z_base):
        total = jnp.zeros((32, 128), f32)
        for t, y, valid in layers(dy, y0):
            for k in range(3):
                u = shifted(k * 2048 + tile_row(y), 32, 64, z_base, valid)
                low, high = ends_of(u)
                total = jnp.where(lane == 60 + 10 * k + t, low, total)
                total = jnp.where(lane == 90 + 10 * k + t, high, total)
                if t in weights:
                    w, face = weights[t]
                    total = total + w * (pltpu.roll(u, face + 10 * k, 1) if face + k else u)
        return total

    def edge_rows(x, dy, y0, z_base, with_row):
        flat = jnp.zeros((3, 128), f32)
        row = jnp.zeros((3, 128), f32)
        for t, y, valid in layers(dy, y0):
            u = shifted(x * 64 + tile_row(y), 3, 2048, z_base, valid)
            flat = flat + (pltpu.roll(u, 10 * t, 1) if t else u)
            if with_row:
                low, high = ends_of(u)
                row = jnp.where(lane == 60 + 10 * sub3 + t, low, row)
                row = jnp.where(lane == 90 + 10 * sub3 + t, high, row)
                if t in weights:
                    w, face = weights[t]
                    spread = jnp.where(
                        sub3 == 0,
                        pltpu.roll(u, face, 1) if face else u,
                        jnp.where(sub3 == 1, pltpu.roll(u, face + 10, 1), pltpu.roll(u, face + 20, 1)),
                    )
                    row = row + w * spread
        return flat, jnp.sum(row, axis=0, keepdims=True)

    for dz in range(2):
        out = other_ref if dz else own_ref
        z_shift = 256 * (1 - 2 * my_c) if dz else 0
        for dy in (-1, 0, 1):
            base = (dy + 1) * HALO * 8
            for dx in (0, -1, 1):
                place = table[ROW_ANCHOR, (dx + 1) * 6 + (dy + 1) * 2 + dz]
                y0, z0 = place >> 8, place & 255
                z_base = z0 - 1 + z_shift
                near = place >= 0
                if dy == 1:
                    near &= y0 == 0
                if dy == -1:
                    near &= y0 == 24
                if dz:
                    near &= z0 == jnp.where(my_c == 0, 0, 248)

                @pl.when(near)
                def _(out=out, base=base, dx=dx, dy=dy, y0=y0, z_base=z_base):
                    if dx == 0:
                        out[base : base + 32, :] = main_rows(dy, y0, z_base)
                        for x, at in ((0, 0), (31, 3)):
                            flat, _row = edge_rows(x, dy, y0, z_base, False)
                            out[base + 32 + at : base + 35 + at, :] = 0.25 * flat
                    else:
                        x, at, tile = (0, 3, 40) if dx == -1 else (31, 0, 48)
                        flat, row = edge_rows(x, dy, y0, z_base, True)
                        out[base + tile + at : base + tile + at + 3, :] = 0.75 * flat
                        out[base + tile + 6 : base + tile + 7, :] = row


def split_slot(slot):
    device = slot >> 2
    return device >> 6, (device >> 3) & 7, (device >> 1) & 3, slot & 3


def route_kernel(table, held, out):
    for j in range(PLANE):
        home = jnp.maximum(table[ROW_HOME, j] - 1, 0)
        gx = home >> 2
        z = gx & 7
        out[j, 0:40] = held[z, 0:40]
        out[j, 40:48] = held[(z + 7) & 7, 48:56]
        out[j, 48:56] = held[(z + 1) & 7, 40:48]
        for s in range(SLOTS):
            for side, row in enumerate((ROW_LOW, ROW_HIGH)):
                _, z, _, local = split_slot(jnp.maximum(table[row, j * 4 + s] - 1, 0))
                start = pl.multiple_of((HALO + side * SLOTS + local) * 8, 8)
                at = (HALO + side * SLOTS + s) * 8
                out[j, at : at + 8] = held[z, pl.ds(start, 8)]


def update_kernel(
    table, rcv, fine_ref, visc_ref, along_x, faces, ends, pool,
    fine_out, means_out,
    sums, planes, advanced, pooled,
):
    my_x, _, my_y, _ = position()
    me = my_x * LINE_Y + my_y
    home = jnp.maximum(table[ROW_HOME, me] - 1, 0)
    gx, hy = home >> 2, home & 3
    at_home = (gx >> 3) * LINE_Y + hy
    at_low = (jnp.maximum(gx - 1, 0) >> 3) * LINE_Y + hy
    at_high = (jnp.minimum(gx + 1, 31) >> 3) * LINE_Y + hy
    low = jnp.where(gx > 0, rcv[at_low, 40:48], 0.0)
    high = jnp.where(gx < 31, rcv[at_high, 48:56], 0.0)
    sub8 = lax.broadcasted_iota(i32, (8, 1), 0)
    beyond = jnp.where(sub8 == 0, low[6:7], jnp.where(sub8 == 1, high[6:7], 0.0))
    body = jnp.concatenate([rcv[at_home, 0:32], beyond], axis=0)
    dot = functools.partial(jnp.dot, precision=HIGHEST, preferred_element_type=f32)
    sums[...] = dot(dot(along_x[...], body), faces[...])
    flat = rcv[at_home, 32:40] + jnp.where(sub8 < 3, low, 0.0) + jnp.where((sub8 >= 3) & (sub8 < 6), high, 0.0)
    planes[...] = dot(flat, ends[...])
    lane = lax.broadcasted_iota(i32, (1, F * F), 1)
    sub = lax.broadcasted_iota(i32, (F, 1), 0)
    lane_z = lane & (F - 1)
    for s in range(SLOTS):
        word = table[ROW_SLOT, me * 4 + s]
        active = (word & 1) == 1
        box_start = pl.multiple_of(((word >> 1) & 3) * F, F)
        low_slot = table[ROW_LOW, me * 4 + s] - 1
        high_slot = table[ROW_HIGH, me * 4 + s] - 1
        lx, _, ly, _ = split_slot(jnp.maximum(low_slot, 0))
        hx, _, hy2, _ = split_slot(jnp.maximum(high_slot, 0))
        low_at, high_at = (HALO + s) * 8, (HALO + SLOTS + s) * 8
        low_tile = rcv[lx * LINE_Y + ly, low_at : low_at + 8]
        high_tile = rcv[hx * LINE_Y + hy2, high_at : high_at + 8]
        visc = step_rate * visc_ref[s * F : s * F + F, :]
        for k in range(3):
            row = (k * SLOTS + s) * F
            cells = fine_ref[row : row + F, :]
            lower = jnp.concatenate([low_tile[k : k + 1], low_tile[3 + k : 4 + k]], axis=1)
            upper = jnp.concatenate([high_tile[k : k + 1], high_tile[3 + k : 4 + k]], axis=1)
            lower = jnp.where(low_slot >= 0, lower, planes[k : k + 1, :])
            upper = jnp.where(high_slot >= 0, upper, planes[3 + k : 4 + k, :])
            total = sums[pl.ds(box_start, F), k * 256 : k * 256 + 256] - 6.0 * cells
            total = total + jnp.where(sub == 0, lower, pltpu.roll(cells, 1, 0))
            total = total + jnp.where(sub == F - 1, upper, pltpu.roll(cells, F - 1, 0))
            total = total + jnp.where(lane < F, 0.0, pltpu.roll(cells, F, 1))
            total = total + jnp.where(lane >= F * F - F, 0.0, pltpu.roll(cells, F * F - F, 1))
            total = total + jnp.where(lane_z == 0, 0.0, pltpu.roll(cells, 1, 1))
            total = total + jnp.where(lane_z == F - 1, 0.0, pltpu.roll(cells, F * F - 1, 1))
            result = cells + visc * total
            fine_out[row : row + F, :] = jnp.where(active, result, 0.0)
            at = s * 48 + k * F
            advanced[at : at + F, :] = result
    for p in range(2):
        at = p * 96
        pooled[p * 48 : p * 48 + 48, :] = dot(advanced[at : at + 48, :], pool[0]) + dot(
            advanced[at + 48 : at + 96, :], pool[1]
        )
    means = pooled[pl.ds(0, 48, stride=2), :] + pooled[pl.ds(1, 48, stride=2), :]
    for z in range(LINE_Z):
        means_out[z] = means


def return_kernel(table, held, out):
    first = lax.broadcasted_iota(i32, (1, 128), 1) < 64
    for j in range(PLANE):
        for p in range(2):
            picks = []
            for h in range(2):
                _, z, _, local = split_slot(jnp.maximum(table[ROW_OWNER, j * 4 + 2 * p + h] - 1, 0))
                start = pl.multiple_of((local >> 1) * 24, 8)
                rows = held[z, pl.ds(start, 24)]
                picks.append(jnp.where((local & 1) == h, rows, pltpu.roll(rows, 64, 1)))
            out[j, p * 24 : p * 24 + 24] = jnp.where(first, picks[0], picks[1])


def place_kernel(table, rcv, coarse_ref, coarse_out, window, spread, sem):
    my_x, _, my_y, _ = position()
    me = my_x * LINE_Y + my_y
    place = table[ROW_ANCHOR, SELF_TARGET]

    @pl.when(place >= 0)
    def _():
        y0 = pl.multiple_of(place >> 8, 8)
        z0 = place & 255
        z_tile = pl.multiple_of((z0 >> 7) * 128, 128)
        z_in = z0 & 127
        region = coarse_out.at[:, pl.ds(y0, 8), pl.ds(z_tile, 128)]
        load = pltpu.make_async_copy(region, window, sem.at[0])
        load.start()
        for i in range(SLOTS):
            ox, _, oy, _ = split_slot(jnp.maximum(table[ROW_OWNER, me * 4 + i] - 1, 0))
            at = ox * LINE_Y + oy
            for k in range(3):
                start = ((i // 2) * 3 + k) * 8
                values = rcv[at, start : start + 8]
                for b in range(B):
                    shift = (z_in + 256 - (b * B + 64 * (i % 2))) & 127
                    spread[pl.ds((k * 32 + i * B) * B + b, B, stride=B), :] = pltpu.roll(values, shift, 1)
        load.wait()
        lane = lax.broadcasted_iota(i32, (1, 1, 128), 2)
        fresh = spread[...].reshape(96, 8, 128)
        window[...] = jnp.where((lane >= z_in) & (lane < z_in + B), fresh, window[...])
        store = pltpu.make_async_copy(window, region, sem.at[1])
        store.start()
        store.wait()


def vmem():
    return pl.BlockSpec(memory_space=pltpu.VMEM)


def smem():
    return pl.BlockSpec(memory_space=pltpu.SMEM)


def anywhere():
    return pl.BlockSpec(memory_space=pl.ANY)


def shape(*dims, dtype=f32):
    return jax.ShapeDtypeStruct(dims, dtype)


def on_device(coarse_field, fine_field, viscosity, corners, grid_slot, neighbors):
    fine = fine_field.reshape(3 * SLOTS * F, F * F)
    tiles = coarse_field.reshape(3, 32, 4, 8, 2, 128).transpose(0, 1, 2, 4, 3, 5).reshape(6144, 128)
    table, own, other, planes = pl.pallas_call(
        pack_kernel,
        out_shape=(
            shape(8, 128, dtype=i32),
            shape(3 * HALO * 8, 128),
            shape(3 * HALO * 8, 128),
            shape(64, 128),
        ),
        in_specs=[vmem()] * 5,
        out_specs=(vmem(), vmem(), vmem(), vmem()),
        scratch_shapes=[pltpu.SMEM((8, 128), i32), pltpu.SemaphoreType.DMA(())],
        name="pack", compiler_params=pltpu.CompilerParams(vmem_limit_bytes=24 << 20),
    )(corners.T, grid_slot[None, :], neighbors.T, fine, tiles)
    halo = own + lax.ppermute(other, "gz", [(0, 1), (1, 0)])
    halo = halo.reshape(3, HALO * 8, 128)
    above = lax.ppermute(halo[2], "gy", [(i, i + 1) for i in range(LINE_Y - 1)])
    below = lax.ppermute(halo[0], "gy", [(i + 1, i) for i in range(LINE_Y - 1)])
    payload = jnp.concatenate([halo[1] + above + below, planes], axis=0)
    held = lax.all_to_all(jnp.broadcast_to(payload, (LINE_Z, SEND * 8, 128)), "gx_1", 0, 0)
    routed = pl.pallas_call(
        route_kernel,
        out_shape=shape(PLANE, SEND * 8, 128),
        in_specs=[smem(), vmem()],
        out_specs=vmem(),
        name="route", compiler_params=pltpu.CompilerParams(vmem_limit_bytes=8 << 20),
    )(table, held)
    received = lax.all_to_all(routed, ("gx_0", "gy"), 0, 0)
    fine_out, means = pl.pallas_call(
        update_kernel,
        out_shape=(shape(3 * SLOTS * F, F * F), shape(LINE_Z, 48, 128)),
        in_specs=[smem()] + [vmem()] * 7,
        out_specs=(vmem(), vmem()),
        scratch_shapes=[
            pltpu.VMEM((64, 768), f32),
            pltpu.VMEM((8, 256), f32),
            pltpu.VMEM((192, 256), f32),
            pltpu.VMEM((96, 128), f32),
        ],
        name="update", compiler_params=pltpu.CompilerParams(vmem_limit_bytes=16 << 20),
    )(table, received, fine, viscosity.reshape(SLOTS * F, F * F), *map(jnp.asarray, constant_matrices()))
    held_means = lax.all_to_all(means, "gx_1", 0, 0)
    back = pl.pallas_call(
        return_kernel,
        out_shape=shape(PLANE, 48, 128),
        in_specs=[smem(), vmem()],
        out_specs=vmem(),
        name="send_back", compiler_params=pltpu.CompilerParams(vmem_limit_bytes=8 << 20),
    )(table, held_means)
    returned = lax.all_to_all(back, ("gx_0", "gy"), 0, 0)
    coarse_out = pl.pallas_call(
        place_kernel,
        out_shape=shape(96, 32, 256),
        in_specs=[smem(), vmem(), anywhere()],
        out_specs=anywhere(),
        input_output_aliases={2: 0},
        scratch_shapes=[
            pltpu.VMEM((96, 8, 128), f32),
            pltpu.VMEM((768, 128), f32),
            pltpu.SemaphoreType.DMA((2,)),
        ],
        name="place", compiler_params=pltpu.CompilerParams(vmem_limit_bytes=8 << 20),
    )(table, returned, coarse_field.reshape(96, 32, 256))
    return fine_out.reshape(fine_field.shape), coarse_out.reshape(coarse_field.shape)


def solution(mesh):
    split = Mesh(
        mesh.devices.reshape(LINE_X, LINE_Z, mesh.shape["gy"], mesh.shape["gz"]), ("gx_0", "gx_1", "gy", "gz")
    )
    in_specs = (
        P(None, GX, "gy", "gz"),
        P(None, GX_GY_GZ, None, None),
        P(GX_GY_GZ, None, None),
        P(),
        P(),
        P(),
    )
    out_specs = (P(None, GX_GY_GZ, None, None), P(None, GX, "gy", "gz"))
    return jax.shard_map(
        on_device, mesh=split, in_specs=in_specs, out_specs=out_specs, check_vma=False
    )
```

```python
import functools

import jax
import jax.numpy as jnp
import numpy as np
from jax import lax
from jax.experimental import pallas as pl
from jax.experimental.pallas import tpu as pltpu
from jax.sharding import Mesh
from jax.sharding import PartitionSpec as P

B = 8
F = 16
SLOTS = 4
SIDE = B + 2
LINE_X = 4
LINE_Z = 8
LINE_Y = 4
PLANE = LINE_X * LINE_Y
HALO = 48
SEND = 72
HIGHEST = lax.Precision.HIGHEST
step_rate = 0.15
f32 = jnp.float32
i32 = jnp.int32
GX = ("gx_0", "gx_1")
GX_GY_GZ = ("gx_0", "gx_1", "gy", "gz")

ROW_SLOT, ROW_HOME, ROW_LOW, ROW_HIGH, ROW_OWNER, ROW_ANCHOR, ROW_ROUTE, ROW_SENDS = range(8)
SELF_TARGET = 8


def tangent_matrix():
    fine = np.arange(F)
    coarse = np.arange(SIDE)
    center = fine // 2 + 1
    other = np.where(fine % 2 == 0, center - 1, center + 1)
    return 0.75 * (coarse[None] == center[:, None]) + 0.25 * (coarse[None] == other[:, None])


def constant_matrices():
    tangent = tangent_matrix()
    along_x = np.zeros((64, 40))
    for fine in range(64):
        center = fine // 2
        other = center - 1 if fine % 2 == 0 else center + 1
        along_x[fine, center] += 0.75
        along_x[fine, 32 if other < 0 else 33 if other > 31 else other] += 0.25
    faces = np.zeros((128, 3, F, F))
    for k in range(3):
        for c in range(SIDE):
            faces[k * 10 + c, k, 0, :] += tangent[:, c]
            faces[30 + k * 10 + c, k, F - 1, :] += tangent[:, c]
            faces[60 + k * 10 + c, k, :, 0] += tangent[:, c]
            faces[90 + k * 10 + c, k, :, F - 1] += tangent[:, c]
    ends = np.zeros((128, F * F))
    ends[: SIDE * SIDE] = np.einsum("sa,tb->abst", tangent, tangent).reshape(SIDE * SIDE, F * F)
    pool = np.zeros((2, F, F, 128))
    for y in range(F):
        for z in range(F):
            for half in range(2):
                pool[half, y, z, half * 64 + (y // 2) * B + z // 2] = 0.125
    return (
        along_x.astype(np.float32),
        faces.reshape(128, 3 * F * F).astype(np.float32),
        ends.astype(np.float32),
        pool.reshape(2, F * F, 128).astype(np.float32),
    )


def pack_constants():
    out = np.zeros((40, 128))
    for k in range(3):
        for y in range(B):
            out[k * B + y, 60 + 10 * k + 1 + y] = 1.0
            out[k * B + y, 90 + 10 * k + 1 + y] = 1.0
        out[k * B, 10 * k : 10 * k + 10] = 0.25
        out[k * B + B - 1, 30 + 10 * k : 40 + 10 * k] = 0.25
        out[24 + k, 10 * k : 10 * k + 10] = 0.75
        out[24 + k, [60 + 10 * k, 90 + 10 * k]] = 1.0
        out[27 + k, 30 + 10 * k : 40 + 10 * k] = 0.75
        out[27 + k, [69 + 10 * k, 99 + 10 * k]] = 1.0
    lanes = np.arange(128)
    out[32] = np.where(lanes < 60, lanes % 10, np.where(lanes < 90, 0, np.where(lanes < 120, 9, -999)))
    out[33] = np.where(lanes < 60, -999, np.where(lanes < 90, 1, np.where(lanes < 120, 8, -999)))
    out[34] = np.where(lanes < 60, 1.0, 0.75)
    out[35] = 0.25
    return out.astype(np.float32)


def position():
    return tuple(lax.axis_index(name) for name in GX_GY_GZ)


def make_table(corners_ref, slots_ref, near_ref, table_ref):
    my_x, my_z, my_y, my_c = position()
    cx, cy, cz = corners_ref[0:1, :], corners_ref[1:2, :], corners_ref[2:3, :]
    gs = slots_ref[0:1, :]
    grids = gs.shape[1]
    low, high = near_ref[0:1, :], near_ref[1:2, :]
    gx, gy, gz = cx >> 5, cy >> 5, cz >> 8
    box = (cx >> 3) & 3
    home = gx * LINE_Y + gy
    brick_key = (home * 2 + gz) * SLOTS + box
    word = (1 + box * 2 + home * 8 + (low + 1) * 1024).astype(f32)
    sub = lax.broadcasted_iota(i32, (64, 1), 0)
    eye = (lax.broadcasted_iota(i32, (64, 128), 0) == lax.broadcasted_iota(i32, (64, 128), 1)).astype(f32)

    def to_row(column):
        return jnp.sum(eye * column, axis=0, keepdims=True)

    def pick(match, values):
        return jnp.sum(jnp.where(match, values, 0.0), axis=1, keepdims=True)

    def device_of(j):
        return (((j >> 2) * LINE_Z + my_z) * LINE_Y + (j & 3)) * 2 + my_c

    keys = device_of(sub >> 2) * SLOTS + (sub & 3)
    held = keys == gs
    words = pick(held, word)
    high_grid = pick(held, (high + 1).astype(f32)).astype(i32)
    low_grid = words.astype(i32) >> 10
    grid_ids = lax.broadcasted_iota(i32, (1, grids), 1) + 1
    slot_plus = (gs + 1).astype(f32)
    low_slot = pick(low_grid == grid_ids, slot_plus).astype(i32)
    high_slot = pick(high_grid == grid_ids, slot_plus).astype(i32)
    devices = gs >> 2
    bit = (jnp.int32(1) << box).astype(f32)

    def boxes_on(device):
        return pick(device == devices, bit).astype(i32)

    mine = device_of(sub >> 2)
    my_mask = boxes_on(mine)
    my_box = (words.astype(i32) >> 1) & 3
    lanes = lax.broadcasted_iota(i32, (64, 128), 1)
    same_j = (sub >> 2) == (lanes >> 2)
    route_row = jnp.zeros((1, 128), f32)
    sends_row = jnp.zeros((1, 128), f32)
    near_words = []
    for side, slot in enumerate((low_slot, high_slot)):
        device = (slot - 1) >> 2
        near_mask = boxes_on(device)
        near_box = (my_box + (3, 1)[side]) & 3
        outer = (slot > 0) & (device != mine)

        def before(mask, at):
            return ((mask & ((jnp.int32(1) << at) - 1)) != 0).astype(i32)

        def after(mask, at):
            return ((mask >> (at + 1)) != 0).astype(i32)

        if side == 0:
            here, there = before(my_mask, my_box), 2 + after(near_mask, near_box)
        else:
            here, there = 2 + after(my_mask, my_box), before(near_mask, near_box)
        target = jnp.where(same_j & ((lanes & 3) == here) & outer, 1.0, 0.0)
        code = (((device >> 3) & 7) * 4 + there + 1).astype(f32)
        route_row = route_row + jnp.sum(target * code, axis=0, keepdims=True)
        sends_row = sends_row + jnp.sum(target * ((sub & 3) + 1).astype(f32), axis=0, keepdims=True)
        plane = (device >> 6) * LINE_Y + ((device >> 1) & 3)
        word = jnp.where(outer, 2 + here * 4 + plane * 16, 1 + ((slot - 1) & 3) * 4)
        near_words.append(jnp.where(slot > 0, word, 0).astype(f32))
    owner = pick(keys == brick_key, slot_plus)
    sub16 = lax.broadcasted_iota(i32, (16, 1), 0)
    on_device = device_of(sub16) == (gs >> 2)
    homes = jnp.max(jnp.where(on_device, (home + 1).astype(f32), 0.0), axis=1, keepdims=True)
    homes = jnp.concatenate([homes, jnp.zeros((48, 1), f32)], axis=0)
    sub24 = lax.broadcasted_iota(i32, (24, 1), 0)
    target_x = my_x * LINE_Z + my_z + jnp.where(sub24 >= 12, 1, jnp.where(sub24 >= 6, 0, -1))
    target_x = jnp.where(sub24 >= 18, -1, target_x)
    in_x = sub24 - jnp.where(sub24 >= 12, 12, jnp.where(sub24 >= 6, 6, 0))
    target_y = my_y + (in_x >> 1) - 1
    target_z = jnp.where((in_x & 1) == 0, my_c, 1 - my_c)
    near_brick = (target_x == gx) & (target_y == gy) & (target_z == gz)
    place = ((cy & 31) * 256 + (cz & 255)).astype(f32)
    anchors = jnp.max(jnp.where(near_brick, place, -1.0), axis=1, keepdims=True)
    anchors = jnp.concatenate([anchors, jnp.zeros((40, 1), f32)], axis=0)
    rows = [to_row(v) for v in (words, homes, *near_words, owner, anchors)] + [route_row, sends_row]
    for r, row in enumerate(rows):
        table_ref[r : r + 1, :] = row.astype(i32)


def pack_kernel(
    corners_ref, slots_ref, near_ref, fine_ref, brick, const,
    table_ref, own_ref, other_ref, planes_ref,
    table, table_sem,
):
    make_table(corners_ref, slots_ref, near_ref, table_ref)
    fetch = pltpu.make_async_copy(table_ref, table, table_sem)
    fetch.start()
    own_ref[...] = jnp.zeros_like(own_ref)
    other_ref[...] = jnp.zeros_like(other_ref)
    planes_ref[...] = jnp.zeros_like(planes_ref)
    fetch.wait()
    me = lax.axis_index("gx_0") * LINE_Y + lax.axis_index("gy")
    for e in range(4):
        s = jnp.maximum(table[ROW_SENDS, me * 4 + e] - 1, 0)
        for k in range(3):
            tile = fine_ref[pl.ds(pl.multiple_of((k * SLOTS + s) * F + (0 if e < 2 else 8), 8), 8), :]
            row = tile[0:1] if e < 2 else tile[7:8]
            for half in range(2):
                at = e * 8 + half * 3 + k
                planes_ref[at : at + 1, :] = row[:, half * 128 : half * 128 + 128]

    my_c = lax.axis_index("gz")
    lane = lax.broadcasted_iota(i32, (1, 128), 1)
    sub3 = lax.broadcasted_iota(i32, (3, 1), 0)

    def shifted(start, count, stride, z_base, valid):
        rows = jnp.concatenate(
            [brick[pl.ds(start + 8 * half, count, stride=stride), :] for half in range(2)], axis=1
        )
        rows = pltpu.roll(rows, (256 - z_base) & 255, 1)[:, :128]
        at = z_base + lane
        keep = (lane < SIDE) & (at >= 0) & (at < 256) & valid
        return jnp.where(keep, rows, 0.0)

    def tile_row(y):
        return (y >> 3) * 16 + (y & 7)

    def layers(dy, y0):
        if dy == 0:
            for t in range(SIDE):
                y = y0 - 1 + t
                valid = True if 0 < t < SIDE - 1 else (y >= 0) & (y < 32)
                yield t, jnp.clip(y, 0, 31), valid
        elif dy == 1:
            yield 0, 31, y0 == 0
        else:
            yield SIDE - 1, 0, y0 == 24

    weights = {0: (0.75, 0), 1: (0.25, 0), SIDE - 2: (0.25, 30), SIDE - 1: (0.75, 30)}

    def ends_of(u):
        low = 0.75 * u[:, 0:1] + 0.25 * u[:, 1:2]
        high = 0.75 * u[:, 9:10] + 0.25 * u[:, 8:9]
        return low, high

    def main_rows(dy, y0, z_base):
        total = jnp.zeros((32, 128), f32)
        for t, y, valid in layers(dy, y0):
            for k in range(3):
                u = shifted(k * 2048 + tile_row(y), 32, 64, z_base, valid)
                low, high = ends_of(u)
                total = jnp.where(lane == 60 + 10 * k + t, low, total)
                total = jnp.where(lane == 90 + 10 * k + t, high, total)
                if t in weights:
                    w, face = weights[t]
                    total = total + w * (pltpu.roll(u, face + 10 * k, 1) if face + k else u)
        return total

    def all_rows(y0, z_base):
        offset = lax.broadcasted_iota(i32, (256, 1), 0) - z_base
        offset = offset.astype(f32)
        window = jnp.where(offset == const[32:33, :], const[34:35, :], 0.0)
        window = window + jnp.where(offset == const[33:34, :], const[35:36, :], 0.0)
        start = (y0 >> 3) * 16
        low_y, high_y = jnp.maximum(y0 - 1, 0), jnp.minimum(y0 + B, 31)
        sides = []
        for half in range(2):
            parts = [brick[pl.ds(pl.multiple_of(n * 64 + start + half * 8, 8), 8), :] for n in range(96)]
            for y in (low_y, high_y):
                parts.append(brick[pl.ds(tile_row(y) + half * 8, 96, stride=64), :])
            sides.append(jnp.concatenate(parts, axis=0))
        cells = jnp.dot(
            jnp.concatenate(sides, axis=1), window, precision=HIGHEST, preferred_element_type=f32
        )
        inner = cells[:768].reshape(3, 32, B, 128)
        total = inner[0] * const[0:8, :][None]
        total = total + inner[1] * const[8:16, :][None]
        total = total + inner[2] * const[16:24, :][None]
        rows = jnp.sum(total, axis=1)
        for k in range(3):
            low = jnp.where(y0 > 0, const[24 + k : 25 + k, :], 0.0)
            high = jnp.where(y0 < 24, const[27 + k : 28 + k, :], 0.0)
            rows = rows + low * cells[768 + 32 * k : 800 + 32 * k] + high * cells[864 + 32 * k : 896 + 32 * k]
        return rows

    def edge_rows(x, dy, y0, z_base, with_row):
        flat = jnp.zeros((3, 128), f32)
        row = jnp.zeros((3, 128), f32)
        for t, y, valid in layers(dy, y0):
            u = shifted(x * 64 + tile_row(y), 3, 2048, z_base, valid)
            flat = flat + (pltpu.roll(u, 10 * t, 1) if t else u)
            if with_row:
                low, high = ends_of(u)
                row = jnp.where(lane == 60 + 10 * sub3 + t, low, row)
                row = jnp.where(lane == 90 + 10 * sub3 + t, high, row)
                if t in weights:
                    w, face = weights[t]
                    spread = jnp.where(
                        sub3 == 0,
                        pltpu.roll(u, face, 1) if face else u,
                        jnp.where(sub3 == 1, pltpu.roll(u, face + 10, 1), pltpu.roll(u, face + 20, 1)),
                    )
                    row = row + w * spread
        return flat, jnp.sum(row, axis=0, keepdims=True)

    for dz in range(2):
        out = other_ref if dz else own_ref
        z_shift = 256 * (1 - 2 * my_c) if dz else 0
        for dy in (-1, 0, 1):
            base = (dy + 1) * HALO
            for dx in (0, -1, 1):
                place = table[ROW_ANCHOR, (dx + 1) * 6 + (dy + 1) * 2 + dz]
                y0, z0 = place >> 8, place & 255
                z_base = z0 - 1 + z_shift
                near = place >= 0
                if dy == 1:
                    near &= y0 == 0
                if dy == -1:
                    near &= y0 == 24
                if dz:
                    near &= z0 == jnp.where(my_c == 0, 0, 248)

                @pl.when(near)
                def _(out=out, base=base, dx=dx, dy=dy, y0=y0, z_base=z_base):
                    if dx == 0:
                        out[base : base + 32, :] = main_rows(dy, y0, z_base) if dy else all_rows(y0, z_base)
                        for x, at in ((0, 0), (31, 3)):
                            flat, _row = edge_rows(x, dy, y0, z_base, False)
                            out[base + 32 + at : base + 35 + at, :] = 0.25 * flat
                    else:
                        x, at = (0, base + 44) if dx == -1 else (31, base + 40)
                        flat, row = edge_rows(x, dy, y0, z_base, True)
                        out[at : at + 3, :] = 0.75 * flat
                        out[at + 3 : at + 4, :] = row


def split_slot(slot):
    device = slot >> 2
    return device >> 6, (device >> 3) & 7, (device >> 1) & 3, slot & 3


def join_kernel(middle, above, below, planes, out):
    total = middle[...] + above[...] + below[...]
    sub = lax.broadcasted_iota(i32, (8, 1), 0)
    tiles = []
    for e in range(4):
        pair = jnp.where(sub == 6, total[40 + 2 * e : 41 + 2 * e], total[41 + 2 * e : 42 + 2 * e])
        tiles.append(jnp.where(sub < 6, planes[e * 8 : e * 8 + 8, :], pair))
    payload = jnp.concatenate([total[:40]] + tiles, axis=0)
    for z in range(LINE_Z):
        out[z] = payload


def route_kernel(table, held, out):
    sub = lax.broadcasted_iota(i32, (8, 1), 0)
    for j in range(PLANE):
        home = jnp.maximum(table[ROW_HOME, j] - 1, 0)
        z = (home >> 2) & 7
        out[j, 0:40] = held[z, 0:40]
        for e in range(4):
            code = jnp.maximum(table[ROW_ROUTE, j * 4 + e] - 1, 0)
            start = pl.multiple_of(40 + (code & 3) * 8, 8)
            at = 40 + e * 8
            piece = held[(z + (7 if e < 2 else 1)) & 7, at : at + 8]
            out[j, at : at + 8] = jnp.where(sub < 6, held[code >> 2, pl.ds(start, 8)], piece)


def update_kernel(
    table, rcv, fine_ref, visc_ref, along_x, faces, ends, pool,
    fine_out, means_out,
    sums, planes, advanced, pooled,
):
    my_x, _, my_y, _ = position()
    me = my_x * LINE_Y + my_y
    home = jnp.maximum(table[ROW_HOME, me] - 1, 0)
    gx, hy = home >> 2, home & 3
    at_home = (gx >> 3) * LINE_Y + hy
    at_low = (jnp.maximum(gx - 1, 0) >> 3) * LINE_Y + hy
    at_high = (jnp.minimum(gx + 1, 31) >> 3) * LINE_Y + hy
    sub8 = lax.broadcasted_iota(i32, (8, 1), 0)

    def piece_rows(at, tile, inside):
        pair = [jnp.where(inside, rcv[at, tile + 8 * i : tile + 8 * i + 8], 0.0) for i in range(2)]
        return pair[0][6:7], pair[0][7:8], pair[1][6:7], pair[1][7:8]

    low = piece_rows(at_low, 40, gx > 0)
    high = piece_rows(at_high, 56, gx < 31)
    beyond = jnp.where(sub8 == 0, low[3], jnp.where(sub8 == 1, high[3], 0.0))
    body = jnp.concatenate([rcv[at_home, 0:32], beyond], axis=0)
    dot = functools.partial(jnp.dot, precision=HIGHEST, preferred_element_type=f32)
    sums[...] = dot(dot(along_x[...], body), faces[...])
    flat = rcv[at_home, 32:40]
    for i, row in enumerate(low[:3] + high[:3]):
        flat = flat + jnp.where(sub8 == i, row, 0.0)
    planes[...] = dot(flat, ends[...])
    lane = lax.broadcasted_iota(i32, (1, F * F), 1)
    sub = lax.broadcasted_iota(i32, (F, 1), 0)
    lane_z = lane & (F - 1)
    for s in range(SLOTS):
        word = table[ROW_SLOT, me * 4 + s]
        active = (word & 1) == 1
        box_start = pl.multiple_of(((word >> 1) & 3) * F, F)
        low_word = table[ROW_LOW, me * 4 + s]
        high_word = table[ROW_HIGH, me * 4 + s]
        low_tile = rcv[low_word >> 4, pl.ds(pl.multiple_of(40 + ((low_word >> 2) & 3) * 8, 8), 8)]
        high_tile = rcv[high_word >> 4, pl.ds(pl.multiple_of(40 + ((high_word >> 2) & 3) * 8, 8), 8)]
        visc = step_rate * visc_ref[s * F : s * F + F, :]
        for k in range(3):
            row = (k * SLOTS + s) * F
            cells = fine_ref[row : row + F, :]
            lower = jnp.concatenate([low_tile[k : k + 1], low_tile[3 + k : 4 + k]], axis=1)
            upper = jnp.concatenate([high_tile[k : k + 1], high_tile[3 + k : 4 + k]], axis=1)
            low_row = pl.multiple_of((k * SLOTS + ((low_word >> 2) & 3)) * F + 8, 8)
            high_row = pl.multiple_of((k * SLOTS + ((high_word >> 2) & 3)) * F, 8)
            lower = jnp.where((low_word & 3) == 1, fine_ref[pl.ds(low_row, 8), :][7:8], lower)
            upper = jnp.where((high_word & 3) == 1, fine_ref[pl.ds(high_row, 8), :][0:1], upper)
            lower = jnp.where(low_word > 0, lower, planes[k : k + 1, :])
            upper = jnp.where(high_word > 0, upper, planes[3 + k : 4 + k, :])
            total = sums[pl.ds(box_start, F), k * 256 : k * 256 + 256] - 6.0 * cells
            total = total + jnp.where(sub == 0, lower, pltpu.roll(cells, 1, 0))
            total = total + jnp.where(sub == F - 1, upper, pltpu.roll(cells, F - 1, 0))
            total = total + jnp.where(lane < F, 0.0, pltpu.roll(cells, F, 1))
            total = total + jnp.where(lane >= F * F - F, 0.0, pltpu.roll(cells, F * F - F, 1))
            total = total + jnp.where(lane_z == 0, 0.0, pltpu.roll(cells, 1, 1))
            total = total + jnp.where(lane_z == F - 1, 0.0, pltpu.roll(cells, F * F - 1, 1))
            result = cells + visc * total
            fine_out[row : row + F, :] = jnp.where(active, result, 0.0)
            at = s * 48 + k * F
            advanced[at : at + F, :] = result
    for p in range(2):
        at = p * 96
        pooled[p * 48 : p * 48 + 48, :] = dot(advanced[at : at + 48, :], pool[0]) + dot(
            advanced[at + 48 : at + 96, :], pool[1]
        )
    means = pooled[pl.ds(0, 48, stride=2), :] + pooled[pl.ds(1, 48, stride=2), :]
    for z in range(LINE_Z):
        means_out[z] = means


def return_kernel(table, held, out):
    first = lax.broadcasted_iota(i32, (1, 128), 1) < 64
    for j in range(PLANE):
        for p in range(2):
            picks = []
            for h in range(2):
                _, z, _, local = split_slot(jnp.maximum(table[ROW_OWNER, j * 4 + 2 * p + h] - 1, 0))
                start = pl.multiple_of((local >> 1) * 24, 8)
                rows = held[z, pl.ds(start, 24)]
                picks.append(jnp.where((local & 1) == h, rows, pltpu.roll(rows, 64, 1)))
            out[j, p * 24 : p * 24 + 24] = jnp.where(first, picks[0], picks[1])


def place_kernel(table, rcv, coarse_ref, coarse_out, window, spread, sem):
    my_x, _, my_y, _ = position()
    me = my_x * LINE_Y + my_y
    place = table[ROW_ANCHOR, SELF_TARGET]

    @pl.when(place >= 0)
    def _():
        y0 = pl.multiple_of(place >> 8, 8)
        z0 = place & 255
        z_tile = pl.multiple_of((z0 >> 7) * 128, 128)
        z_in = z0 & 127
        region = coarse_out.at[:, pl.ds(y0, 8), pl.ds(z_tile, 128)]
        load = pltpu.make_async_copy(region, window, sem.at[0])
        load.start()
        for i in range(SLOTS):
            ox, _, oy, _ = split_slot(jnp.maximum(table[ROW_OWNER, me * 4 + i] - 1, 0))
            at = ox * LINE_Y + oy
            for k in range(3):
                start = ((i // 2) * 3 + k) * 8
                values = rcv[at, start : start + 8]
                for b in range(B):
                    shift = (z_in + 256 - (b * B + 64 * (i % 2))) & 127
                    spread[pl.ds((k * 32 + i * B) * B + b, B, stride=B), :] = pltpu.roll(values, shift, 1)
        load.wait()
        lane = lax.broadcasted_iota(i32, (1, 1, 128), 2)
        fresh = spread[...].reshape(96, 8, 128)
        window[...] = jnp.where((lane >= z_in) & (lane < z_in + B), fresh, window[...])
        store = pltpu.make_async_copy(window, region, sem.at[1])
        store.start()
        store.wait()


def vmem():
    return pl.BlockSpec(memory_space=pltpu.VMEM)


def smem():
    return pl.BlockSpec(memory_space=pltpu.SMEM)


def anywhere():
    return pl.BlockSpec(memory_space=pl.ANY)


def shape(*dims, dtype=f32):
    return jax.ShapeDtypeStruct(dims, dtype)


def on_device(coarse_field, fine_field, viscosity, corners, grid_slot, neighbors):
    fine = fine_field.reshape(3 * SLOTS * F, F * F)
    tiles = coarse_field.reshape(3, 32, 4, 8, 2, 128).transpose(0, 1, 2, 4, 3, 5).reshape(6144, 128)
    table, own, other, planes = pl.pallas_call(
        pack_kernel,
        out_shape=(
            shape(8, 128, dtype=i32),
            shape(3 * HALO, 128),
            shape(3 * HALO, 128),
            shape(32, 128),
        ),
        in_specs=[vmem()] * 6,
        out_specs=(vmem(), vmem(), vmem(), vmem()),
        scratch_shapes=[pltpu.SMEM((8, 128), i32), pltpu.SemaphoreType.DMA(())],
        name="pack", compiler_params=pltpu.CompilerParams(vmem_limit_bytes=24 << 20),
    )(corners.T, grid_slot[None, :], neighbors.T, fine, tiles, jnp.asarray(pack_constants()))
    halo = own + lax.ppermute(other, "gz", [(0, 1), (1, 0)])
    halo = halo.reshape(3, HALO, 128)
    above = lax.ppermute(halo[2], "gy", [(i, i + 1) for i in range(LINE_Y - 1)])
    below = lax.ppermute(halo[0], "gy", [(i + 1, i) for i in range(LINE_Y - 1)])
    payload = pl.pallas_call(
        join_kernel,
        out_shape=shape(LINE_Z, SEND, 128),
        in_specs=[vmem()] * 4,
        out_specs=vmem(),
        name="join",
        compiler_params=pltpu.CompilerParams(vmem_limit_bytes=8 << 20),
    )(halo[1], above, below, planes)
    held = lax.all_to_all(payload, "gx_1", 0, 0)
    routed = pl.pallas_call(
        route_kernel,
        out_shape=shape(PLANE, SEND, 128),
        in_specs=[smem(), vmem()],
        out_specs=vmem(),
        name="route", compiler_params=pltpu.CompilerParams(vmem_limit_bytes=8 << 20),
    )(table, held)
    received = lax.all_to_all(routed, ("gx_0", "gy"), 0, 0)
    fine_out, means = pl.pallas_call(
        update_kernel,
        out_shape=(shape(3 * SLOTS * F, F * F), shape(LINE_Z, 48, 128)),
        in_specs=[smem()] + [vmem()] * 7,
        out_specs=(vmem(), vmem()),
        scratch_shapes=[
            pltpu.VMEM((64, 768), f32),
            pltpu.VMEM((8, 256), f32),
            pltpu.VMEM((192, 256), f32),
            pltpu.VMEM((96, 128), f32),
        ],
        name="update", compiler_params=pltpu.CompilerParams(vmem_limit_bytes=16 << 20),
    )(table, received, fine, viscosity.reshape(SLOTS * F, F * F), *map(jnp.asarray, constant_matrices()))
    held_means = lax.all_to_all(means, "gx_1", 0, 0)
    back = pl.pallas_call(
        return_kernel,
        out_shape=shape(PLANE, 48, 128),
        in_specs=[smem(), vmem()],
        out_specs=vmem(),
        name="send_back", compiler_params=pltpu.CompilerParams(vmem_limit_bytes=8 << 20),
    )(table, held_means)
    returned = lax.all_to_all(back, ("gx_0", "gy"), 0, 0)
    coarse_out = pl.pallas_call(
        place_kernel,
        out_shape=shape(96, 32, 256),
        in_specs=[smem(), vmem(), anywhere()],
        out_specs=anywhere(),
        input_output_aliases={2: 0},
        scratch_shapes=[
            pltpu.VMEM((96, 8, 128), f32),
            pltpu.VMEM((768, 128), f32),
            pltpu.SemaphoreType.DMA((2,)),
        ],
        name="place", compiler_params=pltpu.CompilerParams(vmem_limit_bytes=8 << 20),
    )(table, returned, coarse_field.reshape(96, 32, 256))
    return fine_out.reshape(fine_field.shape), coarse_out.reshape(coarse_field.shape)


def solution(mesh):
    split = Mesh(
        mesh.devices.reshape(LINE_X, LINE_Z, mesh.shape["gy"], mesh.shape["gz"]), ("gx_0", "gx_1", "gy", "gz")
    )
    in_specs = (
        P(None, GX, "gy", "gz"),
        P(None, GX_GY_GZ, None, None),
        P(GX_GY_GZ, None, None),
        P(),
        P(),
        P(),
    )
    out_specs = (P(None, GX_GY_GZ, None, None), P(None, GX, "gy", "gz"))
    return jax.shard_map(
        on_device, mesh=split, in_specs=in_specs, out_specs=out_specs, check_vma=False
    )
```

```python
import functools

import jax
import jax.numpy as jnp
import numpy as np
from jax import lax
from jax.experimental import pallas as pl
from jax.experimental.pallas import tpu as pltpu
from jax.sharding import Mesh
from jax.sharding import PartitionSpec as P

B = 8
F = 16
SLOTS = 4
SIDE = B + 2
LINE_X = 4
LINE_Z = 8
LINE_Y = 4
PLANE = LINE_X * LINE_Y
PACKED = 80
SEND = 72
FIRST = SEND + 16
HIGHEST = lax.Precision.HIGHEST
step_rate = 0.15
f32 = jnp.float32
i32 = jnp.int32
GX = ("gx_0", "gx_1")
GX_GY_GZ = ("gx_0", "gx_1", "gy", "gz")

ROW_SLOT, ROW_HOME, ROW_LOW, ROW_HIGH, ROW_OWNER, ROW_ANCHOR, ROW_ROUTE, ROW_SENDS = range(8)
SELF_TARGET = 8


def tangent_matrix():
    fine = np.arange(F)
    coarse = np.arange(SIDE)
    center = fine // 2 + 1
    other = np.where(fine % 2 == 0, center - 1, center + 1)
    return 0.75 * (coarse[None] == center[:, None]) + 0.25 * (coarse[None] == other[:, None])


def constant_matrices():
    tangent = tangent_matrix()
    along_x = np.zeros((64, 40))
    for fine in range(64):
        center = fine // 2
        other = center - 1 if fine % 2 == 0 else center + 1
        along_x[fine, center] += 0.75
        along_x[fine, 32 if other < 0 else 33 if other > 31 else other] += 0.25
    faces = np.zeros((128, 3, F, F))
    for k in range(3):
        for c in range(SIDE):
            faces[k * 10 + c, k, 0, :] += tangent[:, c]
            faces[30 + k * 10 + c, k, F - 1, :] += tangent[:, c]
            faces[60 + k * 10 + c, k, :, 0] += tangent[:, c]
            faces[90 + k * 10 + c, k, :, F - 1] += tangent[:, c]
    ends = np.zeros((128, F * F))
    ends[: SIDE * SIDE] = np.einsum("sa,tb->abst", tangent, tangent).reshape(SIDE * SIDE, F * F)
    pool = np.zeros((2, F, F, 128))
    for y in range(F):
        for z in range(F):
            for half in range(2):
                pool[half, y, z, half * 64 + (y // 2) * B + z // 2] = 0.125
    return (
        along_x.astype(np.float32),
        faces.reshape(128, 3 * F * F).astype(np.float32),
        ends.astype(np.float32),
        pool.reshape(2, F * F, 128).astype(np.float32),
    )


def pack_constants():
    out = np.zeros((40, 128))
    for k in range(3):
        for y in range(B):
            out[k * B + y, 60 + 10 * k + 1 + y] = 1.0
            out[k * B + y, 90 + 10 * k + 1 + y] = 1.0
        out[k * B, 10 * k : 10 * k + 10] = 0.25
        out[k * B + B - 1, 30 + 10 * k : 40 + 10 * k] = 0.25
        out[24 + k, 10 * k : 10 * k + 10] = 0.75
        out[24 + k, [60 + 10 * k, 90 + 10 * k]] = 1.0
        out[27 + k, 30 + 10 * k : 40 + 10 * k] = 0.75
        out[27 + k, [69 + 10 * k, 99 + 10 * k]] = 1.0
    beside = np.zeros((128, 128))
    for face in range(2):
        for k in range(3):
            for c in range(SIDE):
                at = face * 30 + k * 10 + c
                edge = face * 9 + 10 * k
                beside[at, at] = 0.75
                beside[at, 60 + edge] = {0: 0.75, 1: 0.25}.get(c, 0.0)
                beside[at, 90 + edge] = {9: 0.75, 8: 0.25}.get(c, 0.0)
    lanes = np.arange(128)
    out[32] = np.where(lanes < 60, lanes % 10, np.where(lanes < 90, 0, np.where(lanes < 120, 9, -999)))
    out[33] = np.where(lanes < 60, -999, np.where(lanes < 90, 1, np.where(lanes < 120, 8, -999)))
    out[34] = np.where(lanes < 60, 1.0, 0.75)
    out[35] = 0.25
    return out.astype(np.float32), beside.astype(np.float32)


def position():
    return tuple(lax.axis_index(name) for name in GX_GY_GZ)


def make_table(corners_ref, slots_ref, near_ref, table_ref):
    my_x, my_z, my_y, my_c = position()
    cx, cy, cz = corners_ref[0:1, :], corners_ref[1:2, :], corners_ref[2:3, :]
    gs = slots_ref[0:1, :]
    grids = gs.shape[1]
    low, high = near_ref[0:1, :], near_ref[1:2, :]
    gx, gy, gz = cx >> 5, cy >> 5, cz >> 8
    box = (cx >> 3) & 3
    home = gx * LINE_Y + gy
    brick_key = (home * 2 + gz) * SLOTS + box
    word = (1 + box * 2 + home * 8 + (low + 1) * 1024).astype(f32)
    sub = lax.broadcasted_iota(i32, (32, 1), 0)
    eye = (lax.broadcasted_iota(i32, (32, 128), 0) == lax.broadcasted_iota(i32, (32, 128), 1)).astype(f32)

    def to_row(column):
        return jnp.sum(eye * column, axis=0, keepdims=True)

    def pick(match, values):
        return jnp.sum(jnp.where(match, values, 0.0), axis=1, keepdims=True)

    def device_of(j):
        return ((my_x * LINE_Z + j) * LINE_Y + my_y) * 2 + my_c

    keys = device_of(sub >> 2) * SLOTS + (sub & 3)
    held = keys == gs
    words = pick(held, word)
    high_grid = pick(held, (high + 1).astype(f32)).astype(i32)
    low_grid = words.astype(i32) >> 10
    grid_ids = lax.broadcasted_iota(i32, (1, grids), 1) + 1
    slot_plus = (gs + 1).astype(f32)
    low_slot = pick(low_grid == grid_ids, slot_plus).astype(i32)
    high_slot = pick(high_grid == grid_ids, slot_plus).astype(i32)
    devices = gs >> 2
    bit = (jnp.int32(1) << box).astype(f32)

    def boxes_on(device):
        return pick(device == devices, bit).astype(i32)

    mine = device_of(sub >> 2)
    my_mask = boxes_on(mine)
    my_box = (words.astype(i32) >> 1) & 3
    lanes = lax.broadcasted_iota(i32, (32, 128), 1)
    same_j = (sub >> 2) == (lanes >> 2)
    route_row = jnp.zeros((1, 128), f32)
    sends_row = jnp.zeros((1, 128), f32)
    near_words = []
    for side, slot in enumerate((low_slot, high_slot)):
        device = (slot - 1) >> 2
        near_mask = boxes_on(device)
        near_box = (my_box + (3, 1)[side]) & 3
        outer = (slot > 0) & (device != mine)

        def before(mask, at):
            return ((mask & ((jnp.int32(1) << at) - 1)) != 0).astype(i32)

        def after(mask, at):
            return ((mask >> (at + 1)) != 0).astype(i32)

        if side == 0:
            here, there = before(my_mask, my_box), 2 + after(near_mask, near_box)
        else:
            here, there = 2 + after(my_mask, my_box), before(near_mask, near_box)
        target = jnp.where(same_j & ((lanes & 3) == here) & outer, 1.0, 0.0)
        plane = (device >> 6) * LINE_Y + ((device >> 1) & 3)
        code = (plane * 4 + there + 1).astype(f32)
        route_row = route_row + jnp.sum(target * code, axis=0, keepdims=True)
        sends_row = sends_row + jnp.sum(target * ((sub & 3) + 1).astype(f32), axis=0, keepdims=True)
        word = jnp.where(outer, 2 + here * 4 + ((device >> 3) & 7) * 16, 1 + ((slot - 1) & 3) * 4)
        near_words.append(jnp.where(slot > 0, word, 0).astype(f32))
    owner = pick(keys == brick_key, slot_plus)
    sub8 = lax.broadcasted_iota(i32, (8, 1), 0)
    on_device = device_of(sub8) == (gs >> 2)
    in_y = cy & 31
    side_y = jnp.where(in_y == 0, 128, jnp.where(in_y == 24, 256, 0))
    homes = jnp.max(jnp.where(on_device, (home + 1 + side_y).astype(f32), 0.0), axis=1, keepdims=True)
    homes = jnp.concatenate([homes, jnp.zeros((24, 1), f32)], axis=0)
    sub24 = lax.broadcasted_iota(i32, (24, 1), 0)
    target_x = my_x * LINE_Z + my_z + jnp.where(sub24 >= 12, 1, jnp.where(sub24 >= 6, 0, -1))
    target_x = jnp.where(sub24 >= 18, -1, target_x)
    in_x = sub24 - jnp.where(sub24 >= 12, 12, jnp.where(sub24 >= 6, 6, 0))
    target_y = my_y + (in_x >> 1) - 1
    target_z = jnp.where((in_x & 1) == 0, my_c, 1 - my_c)
    near_brick = (target_x == gx) & (target_y == gy) & (target_z == gz)
    place = ((cy & 31) * 256 + (cz & 255)).astype(f32)
    anchors = jnp.max(jnp.where(near_brick, place, -1.0), axis=1, keepdims=True)
    anchors = jnp.concatenate([anchors, jnp.zeros((8, 1), f32)], axis=0)
    rows = [to_row(v) for v in (words, homes, *near_words, owner, anchors)] + [route_row, sends_row]
    for r, row in enumerate(rows):
        table_ref[r : r + 1, :] = row.astype(i32)


def pack_kernel(
    corners_ref, slots_ref, near_ref, fine_ref, brick, const,
    table_ref, own_ref, other_ref, planes_ref, window_ref,
    table, table_sem,
):
    make_table(corners_ref, slots_ref, near_ref, table_ref)
    fetch = pltpu.make_async_copy(table_ref, table, table_sem)
    fetch.start()
    own_ref[...] = jnp.zeros_like(own_ref)
    other_ref[...] = jnp.zeros_like(other_ref)
    planes_ref[...] = jnp.zeros_like(planes_ref)
    fetch.wait()
    me = lax.axis_index("gx_1")
    for e in range(4):
        s = jnp.maximum(table[ROW_SENDS, me * 4 + e] - 1, 0)
        for k in range(3):
            tile = fine_ref[pl.ds(pl.multiple_of((k * SLOTS + s) * F + (0 if e < 2 else 8), 8), 8), :]
            row = tile[0:1] if e < 2 else tile[7:8]
            for half in range(2):
                at = e * 8 + half * 3 + k
                planes_ref[at : at + 1, :] = row[:, half * 128 : half * 128 + 128]

    my_c = lax.axis_index("gz")
    lane = lax.broadcasted_iota(i32, (1, 128), 1)
    sub3 = lax.broadcasted_iota(i32, (3, 1), 0)

    def shifted(start, count, stride, z_base, valid):
        rows = jnp.concatenate(
            [brick[pl.ds(start + 8 * half, count, stride=stride), :] for half in range(2)], axis=1
        )
        rows = pltpu.roll(rows, (256 - z_base) & 255, 1)[:, :128]
        at = z_base + lane
        keep = (lane < SIDE) & (at >= 0) & (at < 256) & valid
        return jnp.where(keep, rows, 0.0)

    def tile_row(y):
        return (y >> 3) * 16 + (y & 7)

    def layers(y0):
        for t in range(SIDE):
            y = y0 - 1 + t
            valid = True if 0 < t < SIDE - 1 else (y >= 0) & (y < 32)
            yield t, jnp.clip(y, 0, 31), valid

    weights = {0: (0.75, 0), 1: (0.25, 0), SIDE - 2: (0.25, 30), SIDE - 1: (0.75, 30)}

    def ends_of(u):
        low = 0.75 * u[:, 0:1] + 0.25 * u[:, 1:2]
        high = 0.75 * u[:, 9:10] + 0.25 * u[:, 8:9]
        return low, high

    def beside_rows(dy, z_base):
        total = jnp.zeros((32, 128), f32)
        y, face = (31, 0) if dy == 1 else (0, 30)
        for k in range(3):
            u = shifted(k * 2048 + tile_row(y), 32, 64, z_base, True)
            total = total + (pltpu.roll(u, face + 10 * k, 1) if face + k else u)
        return total

    def diagonal_row(x, dy, z_base):
        y, face = (31, 0) if dy == 1 else (0, 30)
        face += 0 if x else 60
        u = shifted(x * 64 + tile_row(y), 3, 2048, z_base, True)
        row = jnp.where(sub3 == 0, u, jnp.where(sub3 == 1, pltpu.roll(u, 10, 1), pltpu.roll(u, 20, 1)))
        row = jnp.sum(row, axis=0, keepdims=True)
        return pltpu.roll(row, face, 1) if face else row

    def all_rows(y0, z_base):
        offset = lax.broadcasted_iota(i32, (256, 1), 0) - z_base
        offset = offset.astype(f32)
        window = jnp.where(offset == const[32:33, :], const[34:35, :], 0.0)
        window = window + jnp.where(offset == const[33:34, :], const[35:36, :], 0.0)
        start = (y0 >> 3) * 16
        low_y, high_y = jnp.maximum(y0 - 1, 0), jnp.minimum(y0 + B, 31)
        sides = []
        for half in range(2):
            parts = [brick[pl.ds(pl.multiple_of(n * 64 + start + half * 8, 8), 8), :] for n in range(96)]
            for y in (low_y, high_y):
                parts.append(brick[pl.ds(tile_row(y) + half * 8, 96, stride=64), :])
            sides.append(jnp.concatenate(parts, axis=0))
        cells = jnp.dot(
            jnp.concatenate(sides, axis=1), window, precision=HIGHEST, preferred_element_type=f32
        )
        inner = cells[:768].reshape(3, 32, B, 128)
        total = inner[0] * const[0:8, :][None]
        total = total + inner[1] * const[8:16, :][None]
        total = total + inner[2] * const[16:24, :][None]
        rows = jnp.sum(total, axis=1)
        for k in range(3):
            low = jnp.where(y0 > 0, const[24 + k : 25 + k, :], 0.0)
            high = jnp.where(y0 < 24, const[27 + k : 28 + k, :], 0.0)
            rows = rows + low * cells[768 + 32 * k : 800 + 32 * k] + high * cells[864 + 32 * k : 896 + 32 * k]
        return rows

    def edge_rows(x, y0, z_base, with_row):
        flat = jnp.zeros((3, 128), f32)
        row = jnp.zeros((3, 128), f32)
        for t, y, valid in layers(y0):
            u = shifted(x * 64 + tile_row(y), 3, 2048, z_base, valid)
            flat = flat + (pltpu.roll(u, 10 * t, 1) if t else u)
            if with_row:
                low, high = ends_of(u)
                row = jnp.where(lane == 60 + 10 * sub3 + t, low, row)
                row = jnp.where(lane == 90 + 10 * sub3 + t, high, row)
                if t in weights:
                    w, face = weights[t]
                    spread = jnp.where(
                        sub3 == 0,
                        pltpu.roll(u, face, 1) if face else u,
                        jnp.where(sub3 == 1, pltpu.roll(u, face + 10, 1), pltpu.roll(u, face + 20, 1)),
                    )
                    row = row + w * spread
        return flat, jnp.sum(row, axis=0, keepdims=True)

    for dz in range(2):
        out = other_ref if dz else own_ref
        z_shift = 256 * (1 - 2 * my_c) if dz else 0
        for dy in (-1, 0, 1):
            for dx in (0, -1, 1):
                place = table[ROW_ANCHOR, (dx + 1) * 6 + (dy + 1) * 2 + dz]
                y0, z0 = place >> 8, place & 255
                z_base = z0 - 1 + z_shift
                near = place >= 0
                if dy == 1:
                    near &= y0 == 0
                if dy == -1:
                    near &= y0 == 24
                if dz:
                    near &= z0 == jnp.where(my_c == 0, 0, 248)

                @pl.when(near)
                def _(out=out, dz=dz, dx=dx, dy=dy, y0=y0, z0=z0, z_base=z_base):
                    if dy and dx:
                        out[38:39, :] += diagonal_row(0 if dx == -1 else 31, dy, z_base)
                    elif dy:
                        out[48:80, :] += beside_rows(dy, z_base)
                    elif dx:
                        x, at = (0, 44) if dx == -1 else (31, 40)
                        flat, row = edge_rows(x, y0, z_base, True)
                        out[at : at + 3, :] = 0.75 * flat
                        out[at + 3 : at + 4, :] = row
                    else:
                        out[0:32, :] = all_rows(y0, z_base)
                        for x, at in ((0, 32), (31, 35)):
                            flat, _row = edge_rows(x, y0, z_base, False)
                            out[at : at + 3, :] = 0.25 * flat
                        if dz == 0:
                            start = (y0 >> 3) * 16 + (z0 >> 7) * 8
                            for n in range(96):
                                tile = brick[pl.ds(pl.multiple_of(n * 64 + start, 8), 8), :]
                                window_ref[n * 8 : n * 8 + 8, :] = tile


def split_slot(slot):
    device = slot >> 2
    return device >> 6, (device >> 3) & 7, (device >> 1) & 3, slot & 3


def join_kernel(own, other, planes, out):
    total = own[...] + other[...]
    sub = lax.broadcasted_iota(i32, (8, 1), 0)
    tiles = []
    for e in range(4):
        pair = jnp.where(sub == 6, total[40 + 2 * e : 41 + 2 * e], total[41 + 2 * e : 42 + 2 * e])
        tiles.append(jnp.where(sub < 6, planes[e * 8 : e * 8 + 8, :], pair))
    two = total[48:64] + pltpu.roll(total[64:80], 64, 1)
    payload = jnp.concatenate([total[:40]] + tiles + [two], axis=0)
    for j in range(PLANE):
        out[j] = payload


def route_kernel(table, held, beside_ref, out, rows, spread):
    sub = lax.broadcasted_iota(i32, (8, 1), 0)
    lane = lax.broadcasted_iota(i32, (1, 128), 1)

    def line_of(gx):
        return (jnp.clip(gx, 0, 31) >> 3) * LINE_Y

    def read(j):
        code = jnp.maximum(table[ROW_HOME, j] - 1, 0)
        home, edge = code & 127, code >> 7
        gx, gy = home >> 2, home & 3
        near_y = jnp.where(edge == 1, gy - 1, gy + 1)
        used = (edge > 0) & (near_y >= 0) & (near_y < LINE_Y)
        start = jnp.where(edge == 2, 30, 0)
        keep = (lane >= start) & (lane < start + 30) & used
        return gx, gy, jnp.clip(near_y, 0, LINE_Y - 1), edge, keep

    for j in range(LINE_Z):
        gx, _, near_y, _, keep = read(j)
        both = held[line_of(gx) + near_y, SEND:FIRST]
        rows[j * 32 : j * 32 + 16, :] = jnp.where(keep, both, 0.0)
        rows[j * 32 + 16 : j * 32 + 32, :] = jnp.where(keep, pltpu.roll(both, 64, 1), 0.0)
        for side in range(2):
            row = held[line_of(gx + (1 if side else -1)) + near_y, 32:40][6:7]
            at = LINE_Z * 32 + j * 2 + side
            rows[at : at + 1, :] = jnp.where(keep, pltpu.roll(row, 68, 1) if side else row, 0.0)
    spread[...] = jnp.dot(rows[...], beside_ref[...], precision=HIGHEST, preferred_element_type=f32)

    for j in range(LINE_Z):
        gx, gy, _, edge, _ = read(j)
        home_at = line_of(gx) + gy
        shift = jnp.where(edge == 2, 60, 0)
        kept = (lane >= jnp.where(edge == 2, 90, 0)) & (lane < jnp.where(edge == 2, 100, SIDE))

        def flats(row):
            return [jnp.where(kept, pltpu.roll(row, (shift + 128 - 10 * k) & 127, 1), 0.0) for k in range(3)]

        out[j, 0:32] = held[home_at, 0:32] + spread[j * 32 : j * 32 + 32, :]
        ends = held[home_at, 32:40]
        for i, row in enumerate(flats(rows[j * 32 : j * 32 + 1, :]) + flats(rows[j * 32 + 31 : j * 32 + 32, :])):
            ends = ends + jnp.where(sub == i, 0.25 * row, 0.0)
        out[j, 32:40] = ends
        for side in range(2):
            at = LINE_Z * 32 + j * 2 + side
            added = [0.75 * row for row in flats(rows[at : at + 1, :])] + [spread[at : at + 1, :]]
            source = line_of(gx + (1 if side else -1)) + gy
            for half in range(2):
                e = side * 2 + half
                code = jnp.maximum(table[ROW_ROUTE, j * 4 + e] - 1, 0)
                start = pl.multiple_of(40 + (code & 3) * 8, 8)
                tile = held[source, 40 + e * 8 : 48 + e * 8]
                tile = tile + jnp.where(sub == 6, added[2 * half], jnp.where(sub == 7, added[2 * half + 1], 0.0))
                out[j, 40 + e * 8 : 48 + e * 8] = jnp.where(sub < 6, held[code >> 2, pl.ds(start, 8)], tile)


def update_kernel(
    table, rcv, fine_ref, visc_ref, along_x, faces, ends, pool,
    fine_out, means_out,
    sums, planes, advanced, pooled,
):
    me = lax.axis_index("gx_1")
    gx = (jnp.maximum(table[ROW_HOME, me] - 1, 0) & 127) >> 2
    at_home, at_low, at_high = gx & 7, (gx + 7) & 7, (gx + 1) & 7
    sub8 = lax.broadcasted_iota(i32, (8, 1), 0)

    def piece_rows(at, tile, inside):
        pair = [jnp.where(inside, rcv[at, tile + 8 * i : tile + 8 * i + 8], 0.0) for i in range(2)]
        return pair[0][6:7], pair[0][7:8], pair[1][6:7], pair[1][7:8]

    low = piece_rows(at_low, 40, gx > 0)
    high = piece_rows(at_high, 56, gx < 31)
    beyond = jnp.where(sub8 == 0, low[3], jnp.where(sub8 == 1, high[3], 0.0))
    body = jnp.concatenate([rcv[at_home, 0:32], beyond], axis=0)
    dot = functools.partial(jnp.dot, precision=HIGHEST, preferred_element_type=f32)
    sums[...] = dot(dot(along_x[...], body), faces[...])
    flat = rcv[at_home, 32:40]
    for i, row in enumerate(low[:3] + high[:3]):
        flat = flat + jnp.where(sub8 == i, row, 0.0)
    planes[...] = dot(flat, ends[...])
    lane = lax.broadcasted_iota(i32, (1, F * F), 1)
    sub = lax.broadcasted_iota(i32, (F, 1), 0)
    lane_z = lane & (F - 1)
    for s in range(SLOTS):
        word = table[ROW_SLOT, me * 4 + s]
        active = (word & 1) == 1
        box_start = pl.multiple_of(((word >> 1) & 3) * F, F)
        low_word = table[ROW_LOW, me * 4 + s]
        high_word = table[ROW_HIGH, me * 4 + s]
        low_tile = rcv[low_word >> 4, pl.ds(pl.multiple_of(40 + ((low_word >> 2) & 3) * 8, 8), 8)]
        high_tile = rcv[high_word >> 4, pl.ds(pl.multiple_of(40 + ((high_word >> 2) & 3) * 8, 8), 8)]
        visc = step_rate * visc_ref[s * F : s * F + F, :]
        for k in range(3):
            row = (k * SLOTS + s) * F
            cells = fine_ref[row : row + F, :]
            lower = jnp.concatenate([low_tile[k : k + 1], low_tile[3 + k : 4 + k]], axis=1)
            upper = jnp.concatenate([high_tile[k : k + 1], high_tile[3 + k : 4 + k]], axis=1)
            low_row = pl.multiple_of((k * SLOTS + ((low_word >> 2) & 3)) * F + 8, 8)
            high_row = pl.multiple_of((k * SLOTS + ((high_word >> 2) & 3)) * F, 8)
            lower = jnp.where((low_word & 3) == 1, fine_ref[pl.ds(low_row, 8), :][7:8], lower)
            upper = jnp.where((high_word & 3) == 1, fine_ref[pl.ds(high_row, 8), :][0:1], upper)
            lower = jnp.where(low_word > 0, lower, planes[k : k + 1, :])
            upper = jnp.where(high_word > 0, upper, planes[3 + k : 4 + k, :])
            total = sums[pl.ds(box_start, F), k * 256 : k * 256 + 256] - 6.0 * cells
            total = total + jnp.where(sub == 0, lower, pltpu.roll(cells, 1, 0))
            total = total + jnp.where(sub == F - 1, upper, pltpu.roll(cells, F - 1, 0))
            total = total + jnp.where(lane < F, 0.0, pltpu.roll(cells, F, 1))
            total = total + jnp.where(lane >= F * F - F, 0.0, pltpu.roll(cells, F * F - F, 1))
            total = total + jnp.where(lane_z == 0, 0.0, pltpu.roll(cells, 1, 1))
            total = total + jnp.where(lane_z == F - 1, 0.0, pltpu.roll(cells, F * F - 1, 1))
            result = cells + visc * total
            fine_out[row : row + F, :] = jnp.where(active, result, 0.0)
            at = s * 48 + k * F
            advanced[at : at + F, :] = result
    for p in range(2):
        at = p * 96
        pooled[p * 48 : p * 48 + 48, :] = dot(advanced[at : at + 48, :], pool[0]) + dot(
            advanced[at + 48 : at + 96, :], pool[1]
        )
    means = pooled[pl.ds(0, 48, stride=2), :] + pooled[pl.ds(1, 48, stride=2), :]
    for j in range(PLANE):
        means_out[j] = means


def return_kernel(table, held, out):
    first = lax.broadcasted_iota(i32, (1, 128), 1) < 64
    for j in range(LINE_Z):
        for p in range(2):
            picks = []
            for h in range(2):
                x, _, y, local = split_slot(jnp.maximum(table[ROW_OWNER, j * 4 + 2 * p + h] - 1, 0))
                start = pl.multiple_of((local >> 1) * 24, 8)
                rows = held[x * LINE_Y + y, pl.ds(start, 24)]
                picks.append(jnp.where((local & 1) == h, rows, pltpu.roll(rows, 64, 1)))
            out[j, p * 24 : p * 24 + 24] = jnp.where(first, picks[0], picks[1])


def place_kernel(table, rcv, window, coarse_ref, coarse_out, spread, sem):
    me = lax.axis_index("gx_1")
    place = table[ROW_ANCHOR, SELF_TARGET]

    @pl.when(place >= 0)
    def _():
        y0 = pl.multiple_of(place >> 8, 8)
        z0 = place & 255
        z_tile = pl.multiple_of((z0 >> 7) * 128, 128)
        z_in = z0 & 127
        region = coarse_out.at[:, pl.ds(y0, 8), pl.ds(z_tile, 128)]
        for i in range(SLOTS):
            _, at, _, _ = split_slot(jnp.maximum(table[ROW_OWNER, me * 4 + i] - 1, 0))
            for k in range(3):
                start = ((i // 2) * 3 + k) * 8
                values = rcv[at, start : start + 8]
                for b in range(B):
                    shift = (z_in + 256 - (b * B + 64 * (i % 2))) & 127
                    spread[pl.ds((k * 32 + i * B) * B + b, B, stride=B), :] = pltpu.roll(values, shift, 1)
        lane = lax.broadcasted_iota(i32, (1, 128), 1)
        spread[...] = jnp.where((lane >= z_in) & (lane < z_in + B), spread[...], window[...])
        store = pltpu.make_async_copy(spread.reshape(96, 8, 128), region, sem)
        store.start()
        store.wait()


def vmem():
    return pl.BlockSpec(memory_space=pltpu.VMEM)


def smem():
    return pl.BlockSpec(memory_space=pltpu.SMEM)


def anywhere():
    return pl.BlockSpec(memory_space=pl.ANY)


def shape(*dims, dtype=f32):
    return jax.ShapeDtypeStruct(dims, dtype)


def on_device(coarse_field, fine_field, viscosity, corners, grid_slot, neighbors):
    fine = fine_field.reshape(3 * SLOTS * F, F * F)
    tiles = coarse_field.reshape(3, 32, 4, 8, 2, 128).transpose(0, 1, 2, 4, 3, 5).reshape(6144, 128)
    pack_const, beside = map(jnp.asarray, pack_constants())
    table, own, other, planes, window = pl.pallas_call(
        pack_kernel,
        out_shape=(
            shape(8, 128, dtype=i32),
            shape(PACKED, 128),
            shape(PACKED, 128),
            shape(32, 128),
            shape(768, 128),
        ),
        in_specs=[vmem()] * 6,
        out_specs=(vmem(),) * 5,
        scratch_shapes=[pltpu.SMEM((8, 128), i32), pltpu.SemaphoreType.DMA(())],
        name="pack", compiler_params=pltpu.CompilerParams(vmem_limit_bytes=24 << 20),
    )(corners.T, grid_slot[None, :], neighbors.T, fine, tiles, pack_const)
    other = lax.ppermute(other, "gz", [(0, 1), (1, 0)])
    payload = pl.pallas_call(
        join_kernel,
        out_shape=shape(PLANE, FIRST, 128),
        in_specs=[vmem()] * 3,
        out_specs=vmem(),
        name="join",
        compiler_params=pltpu.CompilerParams(vmem_limit_bytes=8 << 20),
    )(own, other, planes)
    held = lax.all_to_all(payload, ("gx_0", "gy"), 0, 0)
    routed = pl.pallas_call(
        route_kernel,
        out_shape=shape(LINE_Z, SEND, 128),
        in_specs=[smem(), vmem(), vmem()],
        out_specs=vmem(),
        scratch_shapes=[pltpu.VMEM((LINE_Z * 34, 128), f32)] * 2,
        name="route",
        compiler_params=pltpu.CompilerParams(vmem_limit_bytes=8 << 20),
    )(table, held, beside)
    received = lax.all_to_all(routed, "gx_1", 0, 0)
    fine_out, means = pl.pallas_call(
        update_kernel,
        out_shape=(shape(3 * SLOTS * F, F * F), shape(PLANE, 48, 128)),
        in_specs=[smem()] + [vmem()] * 7,
        out_specs=(vmem(), vmem()),
        scratch_shapes=[
            pltpu.VMEM((64, 768), f32),
            pltpu.VMEM((8, 256), f32),
            pltpu.VMEM((192, 256), f32),
            pltpu.VMEM((96, 128), f32),
        ],
        name="update", compiler_params=pltpu.CompilerParams(vmem_limit_bytes=16 << 20),
    )(table, received, fine, viscosity.reshape(SLOTS * F, F * F), *map(jnp.asarray, constant_matrices()))
    held_means = lax.all_to_all(means, ("gx_0", "gy"), 0, 0)
    back = pl.pallas_call(
        return_kernel,
        out_shape=shape(LINE_Z, 48, 128),
        in_specs=[smem(), vmem()],
        out_specs=vmem(),
        name="send_back", compiler_params=pltpu.CompilerParams(vmem_limit_bytes=8 << 20),
    )(table, held_means)
    returned = lax.all_to_all(back, "gx_1", 0, 0)
    coarse_out = pl.pallas_call(
        place_kernel,
        out_shape=shape(96, 32, 256),
        in_specs=[smem(), vmem(), vmem(), anywhere()],
        out_specs=anywhere(),
        input_output_aliases={3: 0},
        scratch_shapes=[pltpu.VMEM((768, 128), f32), pltpu.SemaphoreType.DMA(())],
        name="place", compiler_params=pltpu.CompilerParams(vmem_limit_bytes=8 << 20),
    )(table, returned, window, coarse_field.reshape(96, 32, 256))
    return fine_out.reshape(fine_field.shape), coarse_out.reshape(coarse_field.shape)


def solution(mesh):
    split = Mesh(
        mesh.devices.reshape(LINE_X, LINE_Z, mesh.shape["gy"], mesh.shape["gz"]), ("gx_0", "gx_1", "gy", "gz")
    )
    in_specs = (
        P(None, GX, "gy", "gz"),
        P(None, GX_GY_GZ, None, None),
        P(GX_GY_GZ, None, None),
        P(),
        P(),
        P(),
    )
    out_specs = (P(None, GX_GY_GZ, None, None), P(None, GX, "gy", "gz"))
    return jax.shard_map(
        on_device, mesh=split, in_specs=in_specs, out_specs=out_specs, check_vma=False
    )
```

```python
import jax
import jax.numpy as jnp
import numpy as np
from jax import lax
from jax.experimental import pallas as pl
from jax.experimental.pallas import tpu as pltpu
from jax.sharding import Mesh
from jax.sharding import PartitionSpec as P

B = 8
F = 16
SLOTS = 4
SIDE = B + 2
LINE_X = 4
LINE_Z = 8
LINE_Y = 4
PLANE = LINE_X * LINE_Y
PACKED = 80
PAIRED = 72
FIRST = 88
SEND = 64
step_rate = 0.15
f32 = jnp.float32
i32 = jnp.int32
GX = ("gx_0", "gx_1")
GX_GY_GZ = ("gx_0", "gx_1", "gy", "gz")

ROW_SLOT, ROW_HOME, ROW_LOW, ROW_HIGH, ROW_OWNER, ROW_ANCHOR, ROW_ROUTE, ROW_SENDS = range(8)
SELF_TARGET = 8


def tangent_matrix():
    fine = np.arange(F)
    coarse = np.arange(SIDE)
    center = fine // 2 + 1
    other = np.where(fine % 2 == 0, center - 1, center + 1)
    return 0.75 * (coarse[None] == center[:, None]) + 0.25 * (coarse[None] == other[:, None])


def constant_matrices():
    tangent = tangent_matrix()
    along_x = np.zeros((64, 40))
    for fine in range(64):
        center = fine // 2
        other = center - 1 if fine % 2 == 0 else center + 1
        along_x[fine, center] += 0.75
        along_x[fine, 32 if other < 0 else 33 if other > 31 else other] += 0.25
    faces = np.zeros((128, 3, F, F))
    for k in range(3):
        for c in range(SIDE):
            faces[k * 10 + c, k, 0, :] += tangent[:, c]
            faces[30 + k * 10 + c, k, F - 1, :] += tangent[:, c]
            faces[60 + k * 10 + c, k, :, 0] += tangent[:, c]
            faces[90 + k * 10 + c, k, :, F - 1] += tangent[:, c]
    ends = np.zeros((128, F * F))
    ends[: SIDE * SIDE] = np.einsum("sa,tb->abst", tangent, tangent).reshape(SIDE * SIDE, F * F)
    pool = np.zeros((2, F, F, 128))
    for y in range(F):
        for z in range(F):
            for half in range(2):
                pool[half, y, z, half * 64 + (y // 2) * B + z // 2] = 0.125
    return (
        along_x.astype(np.float32),
        faces.reshape(128, 3 * F * F).astype(np.float32),
        ends.astype(np.float32),
        pool.reshape(2, F * F, 128).astype(np.float32),
    )


def pack_constants():
    out = np.zeros((40, 128))
    for k in range(3):
        for y in range(B):
            out[k * B + y, 60 + 10 * k + 1 + y] = 1.0
            out[k * B + y, 90 + 10 * k + 1 + y] = 1.0
        out[k * B, 10 * k : 10 * k + 10] = 0.25
        out[k * B + B - 1, 30 + 10 * k : 40 + 10 * k] = 0.25
        out[24 + k, 10 * k : 10 * k + 10] = 0.75
        out[24 + k, [60 + 10 * k, 90 + 10 * k]] = 1.0
        out[27 + k, 30 + 10 * k : 40 + 10 * k] = 0.75
        out[27 + k, [69 + 10 * k, 99 + 10 * k]] = 1.0
    beside = np.zeros((128, 128))
    for face in range(2):
        for k in range(3):
            for c in range(SIDE):
                at = face * 30 + k * 10 + c
                edge = face * 9 + 10 * k
                beside[at, at] = 0.75
                beside[at, 60 + edge] = {0: 0.75, 1: 0.25}.get(c, 0.0)
                beside[at, 90 + edge] = {9: 0.75, 8: 0.25}.get(c, 0.0)
    lanes = np.arange(128)
    out[32] = np.where(lanes < 60, lanes % 10, np.where(lanes < 90, 0, np.where(lanes < 120, 9, -999)))
    out[33] = np.where(lanes < 60, -999, np.where(lanes < 90, 1, np.where(lanes < 120, 8, -999)))
    out[34] = np.where(lanes < 60, 1.0, 0.75)
    out[35] = 0.25
    return out.astype(np.float32), beside.astype(np.float32)


def thirds(values):
    high = values.astype(jnp.bfloat16)
    rest = values - high.astype(f32)
    middle = rest.astype(jnp.bfloat16)
    return high, middle, (rest - middle.astype(f32)).astype(jnp.bfloat16)


def dot_right(values, weights):
    parts = [jnp.dot(part, weights, preferred_element_type=f32) for part in thirds(values)]
    return parts[0] + (parts[1] + parts[2])


def dot_left(weights, values):
    parts = [jnp.dot(weights, part, preferred_element_type=f32) for part in thirds(values)]
    return parts[0] + (parts[1] + parts[2])


def position():
    return tuple(lax.axis_index(name) for name in GX_GY_GZ)


def make_table(corners_ref, slots_ref, near_ref, table_ref):
    my_x, my_z, my_y, my_c = position()
    cx, cy, cz = corners_ref[0:1, :], corners_ref[1:2, :], corners_ref[2:3, :]
    gs = slots_ref[0:1, :]
    grids = gs.shape[1]
    low, high = near_ref[0:1, :], near_ref[1:2, :]
    gx, gy, gz = cx >> 5, cy >> 5, cz >> 8
    box = (cx >> 3) & 3
    home = gx * LINE_Y + gy
    brick_key = (home * 2 + gz) * SLOTS + box
    word = (1 + box * 2 + home * 8 + (low + 1) * 1024).astype(f32)
    sub = lax.broadcasted_iota(i32, (32, 1), 0)
    eye = (lax.broadcasted_iota(i32, (32, 128), 0) == lax.broadcasted_iota(i32, (32, 128), 1)).astype(f32)

    def to_row(column):
        return jnp.sum(eye * column, axis=0, keepdims=True)

    def pick(match, values):
        return jnp.sum(jnp.where(match, values, 0.0), axis=1, keepdims=True)

    def device_of(j):
        return ((my_x * LINE_Z + j) * LINE_Y + my_y) * 2 + my_c

    keys = device_of(sub >> 2) * SLOTS + (sub & 3)
    held = keys == gs
    words = pick(held, word)
    high_grid = pick(held, (high + 1).astype(f32)).astype(i32)
    low_grid = words.astype(i32) >> 10
    grid_ids = lax.broadcasted_iota(i32, (1, grids), 1) + 1
    slot_plus = (gs + 1).astype(f32)
    low_slot = pick(low_grid == grid_ids, slot_plus).astype(i32)
    high_slot = pick(high_grid == grid_ids, slot_plus).astype(i32)
    devices = gs >> 2
    bit = (jnp.int32(1) << box).astype(f32)

    def boxes_on(device):
        return pick(device == devices, bit).astype(i32)

    mine = device_of(sub >> 2)
    my_mask = boxes_on(mine)
    my_box = (words.astype(i32) >> 1) & 3
    lanes = lax.broadcasted_iota(i32, (32, 128), 1)
    same_j = (sub >> 2) == (lanes >> 2)
    route_row = jnp.zeros((1, 128), f32)
    sends_row = jnp.zeros((1, 128), f32)
    near_words = []
    for side, slot in enumerate((low_slot, high_slot)):
        device = (slot - 1) >> 2
        near_mask = boxes_on(device)
        near_box = (my_box + (3, 1)[side]) & 3
        outer = (slot > 0) & (device != mine)

        def before(mask, at):
            return ((mask & ((jnp.int32(1) << at) - 1)) != 0).astype(i32)

        def after(mask, at):
            return ((mask >> (at + 1)) != 0).astype(i32)

        if side == 0:
            here, there = before(my_mask, my_box), 2 + after(near_mask, near_box)
        else:
            here, there = 2 + after(my_mask, my_box), before(near_mask, near_box)
        target = jnp.where(same_j & ((lanes & 3) == here) & outer, 1.0, 0.0)
        plane = (device >> 6) * LINE_Y + ((device >> 1) & 3)
        code = (plane * 4 + there + 1).astype(f32)
        route_row = route_row + jnp.sum(target * code, axis=0, keepdims=True)
        sends_row = sends_row + jnp.sum(target * ((sub & 3) + 1).astype(f32), axis=0, keepdims=True)
        word = jnp.where(outer, 2 + here * 4 + ((device >> 3) & 7) * 16, 1 + ((slot - 1) & 3) * 4)
        near_words.append(jnp.where(slot > 0, word, 0).astype(f32))
    owner = pick(keys == brick_key, slot_plus)
    sub8 = lax.broadcasted_iota(i32, (8, 1), 0)
    on_device = device_of(sub8) == (gs >> 2)
    in_y = cy & 31
    side_y = jnp.where(in_y == 0, 128, jnp.where(in_y == 24, 256, 0))
    homes = jnp.max(jnp.where(on_device, (home + 1 + side_y).astype(f32), 0.0), axis=1, keepdims=True)
    homes = jnp.concatenate([homes, jnp.zeros((24, 1), f32)], axis=0)
    sub24 = lax.broadcasted_iota(i32, (24, 1), 0)
    target_x = my_x * LINE_Z + my_z + jnp.where(sub24 >= 12, 1, jnp.where(sub24 >= 6, 0, -1))
    target_x = jnp.where(sub24 >= 18, -1, target_x)
    in_x = sub24 - jnp.where(sub24 >= 12, 12, jnp.where(sub24 >= 6, 6, 0))
    target_y = my_y + (in_x >> 1) - 1
    target_z = jnp.where((in_x & 1) == 0, my_c, 1 - my_c)
    near_brick = (target_x == gx) & (target_y == gy) & (target_z == gz)
    place = ((cy & 31) * 256 + (cz & 255)).astype(f32)
    anchors = jnp.max(jnp.where(near_brick, place, -1.0), axis=1, keepdims=True)
    anchors = jnp.concatenate([anchors, jnp.zeros((8, 1), f32)], axis=0)
    rows = [to_row(v) for v in (words, homes, *near_words, owner, anchors)] + [route_row, sends_row]
    for r, row in enumerate(rows):
        table_ref[r : r + 1, :] = row.astype(i32)


def pack_kernel(
    corners_ref, slots_ref, near_ref, fine_ref, brick, const,
    table_ref, own_ref, other_ref, planes_ref, window_ref,
    table, table_sem,
):
    make_table(corners_ref, slots_ref, near_ref, table_ref)
    fetch = pltpu.make_async_copy(table_ref, table, table_sem)
    fetch.start()
    own_ref[...] = jnp.zeros_like(own_ref)
    other_ref[...] = jnp.zeros_like(other_ref)
    planes_ref[...] = jnp.zeros_like(planes_ref)
    fetch.wait()
    me = lax.axis_index("gx_1")
    for e in range(4):
        s = jnp.maximum(table[ROW_SENDS, me * 4 + e] - 1, 0)
        for k in range(3):
            tile = fine_ref[pl.ds(pl.multiple_of((k * SLOTS + s) * F + (0 if e < 2 else 8), 8), 8), :]
            row = tile[0:1] if e < 2 else tile[7:8]
            for half in range(2):
                at = e * 8 + half * 3 + k
                planes_ref[at : at + 1, :] = row[:, half * 128 : half * 128 + 128]

    my_c = lax.axis_index("gz")
    lane = lax.broadcasted_iota(i32, (1, 128), 1)
    sub3 = lax.broadcasted_iota(i32, (3, 1), 0)

    def shifted(start, count, stride, z_base, valid):
        rows = jnp.concatenate(
            [brick[pl.ds(start + 8 * half, count, stride=stride), :] for half in range(2)], axis=1
        )
        rows = pltpu.roll(rows, (256 - z_base) & 255, 1)[:, :128]
        at = z_base + lane
        keep = (lane < SIDE) & (at >= 0) & (at < 256) & valid
        return jnp.where(keep, rows, 0.0)

    def tile_row(y):
        return (y >> 3) * 16 + (y & 7)

    def ends_of(u):
        low = 0.75 * u[:, 0:1] + 0.25 * u[:, 1:2]
        high = 0.75 * u[:, 9:10] + 0.25 * u[:, 8:9]
        return low, high

    def beside_rows(dy, z_base):
        total = jnp.zeros((32, 128), f32)
        y, face = (31, 0) if dy == 1 else (0, 30)
        for k in range(3):
            u = shifted(k * 2048 + tile_row(y), 32, 64, z_base, True)
            total = total + (pltpu.roll(u, face + 10 * k, 1) if face + k else u)
        return total

    def diagonal_row(x, dy, z_base):
        y, face = (31, 0) if dy == 1 else (0, 30)
        face += 0 if x else 60
        u = shifted(x * 64 + tile_row(y), 3, 2048, z_base, True)
        row = jnp.where(sub3 == 0, u, jnp.where(sub3 == 1, pltpu.roll(u, 10, 1), pltpu.roll(u, 20, 1)))
        row = jnp.sum(row, axis=0, keepdims=True)
        return pltpu.roll(row, face, 1) if face else row

    def all_rows(y0, z_base):
        offset = lax.broadcasted_iota(i32, (256, 1), 0) - z_base
        offset = offset.astype(f32)
        window = jnp.where(offset == const[32:33, :], const[34:35, :], 0.0)
        window = window + jnp.where(offset == const[33:34, :], const[35:36, :], 0.0)
        start = (y0 >> 3) * 16
        low_y, high_y = jnp.maximum(y0 - 1, 0), jnp.minimum(y0 + B, 31)
        sides = []
        for half in range(2):
            parts = [brick[pl.ds(pl.multiple_of(n * 64 + start + half * 8, 8), 8), :] for n in range(96)]
            for y in (low_y, high_y):
                parts.append(brick[pl.ds(tile_row(y) + half * 8, 96, stride=64), :])
            sides.append(jnp.concatenate(parts, axis=0))
        cells = dot_right(jnp.concatenate(sides, axis=1), window.astype(jnp.bfloat16))
        inner = cells[:768].reshape(3, 32, B, 128)
        total = inner[0] * const[0:8, :][None]
        total = total + inner[1] * const[8:16, :][None]
        total = total + inner[2] * const[16:24, :][None]
        rows = jnp.sum(total, axis=1)
        for k in range(3):
            low = jnp.where(y0 > 0, const[24 + k : 25 + k, :], 0.0)
            high = jnp.where(y0 < 24, const[27 + k : 28 + k, :], 0.0)
            rows = rows + low * cells[768 + 32 * k : 800 + 32 * k] + high * cells[864 + 32 * k : 896 + 32 * k]
        flats = []
        for x in (0, 31):
            for k in range(3):
                tile = jnp.where(lane < SIDE, cells[(k * 32 + x) * B : (k * 32 + x) * B + B], 0.0)
                flat = jnp.sum(pltpu.roll(tile, SIDE, 1, stride=SIDE, stride_axis=0), axis=0, keepdims=True)
                low = cells[768 + 32 * k + x : 769 + 32 * k + x]
                high = cells[864 + 32 * k + x : 865 + 32 * k + x]
                flat = flat + jnp.where((lane < SIDE) & (y0 > 0), low, 0.0)
                flat = flat + pltpu.roll(jnp.where((lane < SIDE) & (y0 < 24), high, 0.0), 90, 1)
                flats.append(flat)
        return rows, flats

    def edge_rows(x, y0, z_base):
        start = (y0 >> 3) * 16
        tiles = []
        for k in range(3):
            at = (k * 32 + x) * 64 + start
            halves = [brick[pl.ds(pl.multiple_of(at + 8 * half, 8), 8), :] for half in range(2)]
            tiles.append(jnp.concatenate(halves, axis=1))
        u = pltpu.roll(jnp.concatenate(tiles, axis=0), (256 - z_base) & 255, 1)[:, :128]
        at = z_base + lane
        u = jnp.where((lane < SIDE) & (at >= 0) & (at < 256), u, 0.0)
        low, high = ends_of(u)
        flats, faces = [], []
        for k in range(3):
            tile = u[k * B : k * B + B]
            flats.append(jnp.sum(pltpu.roll(tile, SIDE, 1, stride=SIDE, stride_axis=0), axis=0, keepdims=True))
            tile = pltpu.roll(tile, 10 * k, 1) if k else tile
            faces.append(tile + pltpu.roll(tile, 30, 1))
        spread = jnp.where(lane < 60, jnp.concatenate(faces, axis=0), jnp.where(lane < 90, low, high))
        total = jnp.sum(spread * const[0:24, :], axis=0, keepdims=True)
        flat = jnp.where(sub3 == 0, flats[0], jnp.where(sub3 == 1, flats[1], flats[2]))
        row = jnp.zeros((3, 128), f32)
        for t, y, valid in ((0, y0 - 1, y0 > 0), (SIDE - 1, y0 + B, y0 < 24)):
            u = shifted(x * 64 + tile_row(jnp.clip(y, 0, 31)), 3, 2048, z_base, valid)
            flat = flat + (pltpu.roll(u, 10 * t, 1) if t else u)
            low, high = ends_of(u)
            row = jnp.where(lane == 60 + 10 * sub3 + t, low, row)
            row = jnp.where(lane == 90 + 10 * sub3 + t, high, row)
            face = 30 if t else 0
            spread = jnp.where(
                sub3 == 0,
                pltpu.roll(u, face, 1) if face else u,
                jnp.where(sub3 == 1, pltpu.roll(u, face + 10, 1), pltpu.roll(u, face + 20, 1)),
            )
            row = row + 0.75 * spread
        return flat, total + jnp.sum(row, axis=0, keepdims=True)

    for dz in range(2):
        out = other_ref if dz else own_ref
        z_shift = 256 * (1 - 2 * my_c) if dz else 0
        for dy in (-1, 0, 1):
            for dx in (0, -1, 1):
                place = table[ROW_ANCHOR, (dx + 1) * 6 + (dy + 1) * 2 + dz]
                y0, z0 = place >> 8, place & 255
                z_base = z0 - 1 + z_shift
                near = place >= 0
                if dy == 1:
                    near &= y0 == 0
                if dy == -1:
                    near &= y0 == 24
                if dz:
                    near &= z0 == jnp.where(my_c == 0, 0, 248)

                @pl.when(near)
                def _(out=out, dz=dz, dx=dx, dy=dy, y0=y0, z0=z0, z_base=z_base):
                    if dy and dx:
                        out[38:39, :] += diagonal_row(0 if dx == -1 else 31, dy, z_base)
                    elif dy:
                        out[48:80, :] += beside_rows(dy, z_base)
                    elif dx:
                        x, at = (0, 44) if dx == -1 else (31, 40)
                        flat, row = edge_rows(x, y0, z_base)
                        out[at : at + 3, :] = 0.75 * flat
                        out[at + 3 : at + 4, :] = row
                    else:
                        rows, flats = all_rows(y0, z_base)
                        out[0:32, :] = rows
                        for i, flat in enumerate(flats):
                            out[32 + i : 33 + i, :] = 0.25 * flat
                        if dz == 0:
                            start = (y0 >> 3) * 16 + (z0 >> 7) * 8
                            for n in range(96):
                                tile = brick[pl.ds(pl.multiple_of(n * 64 + start, 8), 8), :]
                                window_ref[n * 8 : n * 8 + 8, :] = tile


def split_slot(slot):
    device = slot >> 2
    return device >> 6, (device >> 3) & 7, (device >> 1) & 3, slot & 3


def join_kernel(own, other, planes, out):
    total = own[...] + other[...]
    sub = lax.broadcasted_iota(i32, (8, 1), 0)
    tiles = []
    for e in range(4):
        pair = jnp.where(sub == 6, total[40 + 2 * e : 41 + 2 * e], total[41 + 2 * e : 42 + 2 * e])
        tiles.append(jnp.where(sub < 6, planes[e * 8 : e * 8 + 8, :], pair))
    two = total[48:64] + pltpu.roll(total[64:80], 64, 1)
    payload = jnp.concatenate([total[:40]] + tiles + [two], axis=0)
    for j in range(PLANE):
        out[j] = payload


def route_kernel(table, held, beside_ref, out, rows, spread):
    sub = lax.broadcasted_iota(i32, (8, 1), 0)
    lane = lax.broadcasted_iota(i32, (1, 128), 1)

    def line_of(gx):
        return (jnp.clip(gx, 0, 31) >> 3) * LINE_Y

    def read(j):
        code = jnp.maximum(table[ROW_HOME, j] - 1, 0)
        home, edge = code & 127, code >> 7
        gx, gy = home >> 2, home & 3
        near_y = jnp.where(edge == 1, gy - 1, gy + 1)
        used = (edge > 0) & (near_y >= 0) & (near_y < LINE_Y)
        start = jnp.where(edge == 2, 30, 0)
        keep = (lane >= start) & (lane < start + 30) & used
        return gx, gy, jnp.clip(near_y, 0, LINE_Y - 1), edge, keep

    for j in range(LINE_Z):
        gx, _, near_y, _, keep = read(j)
        both = held[line_of(gx) + near_y, PAIRED:FIRST]
        rows[j * 32 : j * 32 + 16, :] = jnp.where(keep, both, 0.0)
        rows[j * 32 + 16 : j * 32 + 32, :] = jnp.where(keep, pltpu.roll(both, 64, 1), 0.0)
        for side in range(2):
            row = held[line_of(gx + (1 if side else -1)) + near_y, 32:40][6:7]
            at = LINE_Z * 32 + j * 2 + side
            rows[at : at + 1, :] = jnp.where(keep, pltpu.roll(row, 68, 1) if side else row, 0.0)
    spread[...] = dot_right(rows[...], beside_ref[...])

    for j in range(LINE_Z):
        gx, gy, _, edge, _ = read(j)
        home_at = line_of(gx) + gy
        shift = jnp.where(edge == 2, 60, 0)
        kept = (lane >= jnp.where(edge == 2, 90, 0)) & (lane < jnp.where(edge == 2, 100, SIDE))

        def flats(row):
            return [jnp.where(kept, pltpu.roll(row, (shift + 128 - 10 * k) & 127, 1), 0.0) for k in range(3)]

        out[j, 0:32] = held[home_at, 0:32] + spread[j * 32 : j * 32 + 32, :]
        ends = held[home_at, 32:40]
        for side in range(2):
            near = rows[j * 32 + 31 * side : j * 32 + 31 * side + 1, :]
            at = LINE_Z * 32 + j * 2 + side
            source = line_of(gx + (1 if side else -1)) + gy
            pair = [held[source, 40 + (side * 2 + half) * 8 : 48 + (side * 2 + half) * 8] for half in range(2)]
            ghosts = [ends[3 * side + k : 3 * side + k + 1] + 0.25 * row for k, row in enumerate(flats(near))]
            pieces = (pair[0][6:7], pair[0][7:8], pair[1][6:7])
            ghosts += [piece + 0.75 * row for piece, row in zip(pieces, flats(rows[at : at + 1, :]))]
            ghosts.append(pair[1][7:8] + spread[at : at + 1, :])
            tile = jnp.zeros((8, 128), f32)
            for i, row in enumerate(ghosts):
                tile = jnp.where(sub == i, row, tile)
            for half in range(2):
                e = side * 2 + half
                code = table[ROW_ROUTE, j * 4 + e] - 1
                start = pl.multiple_of(40 + (jnp.maximum(code, 0) & 3) * 8, 8)
                plane = held[jnp.maximum(code, 0) >> 2, pl.ds(start, 8)]
                if half == 0:
                    plane = jnp.where((sub < 6) & (code >= 0), plane, tile)
                out[j, 32 + e * 8 : 40 + e * 8] = plane


def update_kernel(
    table, rcv, fine_ref, visc_ref, along_x, faces, ends, pool,
    fine_out, means_out,
    sums, planes, advanced, pooled,
):
    me = lax.axis_index("gx_1")
    gx = (jnp.maximum(table[ROW_HOME, me] - 1, 0) & 127) >> 2
    at_home, at_low, at_high = gx & 7, (gx + 7) & 7, (gx + 1) & 7
    sub8 = lax.broadcasted_iota(i32, (8, 1), 0)

    low = jnp.where(gx > 0, rcv[at_low, 32:40], 0.0)
    high = jnp.where(gx < 31, rcv[at_high, 48:56], 0.0)
    beyond = jnp.where(sub8 == 0, low[6:7], jnp.where(sub8 == 1, high[6:7], 0.0))
    body = jnp.concatenate([rcv[at_home, 0:32], beyond], axis=0)
    sums[...] = dot_right(dot_left(along_x[...], body), faces[...])
    own = (rcv[at_home, 32:40], rcv[at_home, 48:56])
    flat = jnp.zeros((8, 128), f32)
    for side, other in enumerate((low, high)):
        for k in range(3):
            flat = jnp.where(sub8 == 3 * side + k, own[side][k : k + 1] + other[3 + k : 4 + k], flat)
    planes[...] = dot_right(flat, ends[...])
    lane = lax.broadcasted_iota(i32, (1, F * F), 1)
    sub = lax.broadcasted_iota(i32, (F, 1), 0)
    lane_z = lane & (F - 1)
    for s in range(SLOTS):
        word = table[ROW_SLOT, me * 4 + s]
        active = (word & 1) == 1
        box_start = pl.multiple_of(((word >> 1) & 3) * F, F)
        low_word = table[ROW_LOW, me * 4 + s]
        high_word = table[ROW_HIGH, me * 4 + s]
        low_tile = rcv[low_word >> 4, pl.ds(pl.multiple_of(32 + ((low_word >> 2) & 3) * 8, 8), 8)]
        high_tile = rcv[high_word >> 4, pl.ds(pl.multiple_of(32 + ((high_word >> 2) & 3) * 8, 8), 8)]
        visc = step_rate * visc_ref[s * F : s * F + F, :]
        for k in range(3):
            row = (k * SLOTS + s) * F
            cells = fine_ref[row : row + F, :]
            lower = jnp.concatenate([low_tile[k : k + 1], low_tile[3 + k : 4 + k]], axis=1)
            upper = jnp.concatenate([high_tile[k : k + 1], high_tile[3 + k : 4 + k]], axis=1)
            low_row = pl.multiple_of((k * SLOTS + ((low_word >> 2) & 3)) * F + 8, 8)
            high_row = pl.multiple_of((k * SLOTS + ((high_word >> 2) & 3)) * F, 8)
            lower = jnp.where((low_word & 3) == 1, fine_ref[pl.ds(low_row, 8), :][7:8], lower)
            upper = jnp.where((high_word & 3) == 1, fine_ref[pl.ds(high_row, 8), :][0:1], upper)
            lower = jnp.where(low_word > 0, lower, planes[k : k + 1, :])
            upper = jnp.where(high_word > 0, upper, planes[3 + k : 4 + k, :])
            total = sums[pl.ds(box_start, F), k * 256 : k * 256 + 256] - 6.0 * cells
            total = total + jnp.where(sub == 0, lower, pltpu.roll(cells, 1, 0))
            total = total + jnp.where(sub == F - 1, upper, pltpu.roll(cells, F - 1, 0))
            total = total + jnp.where(lane < F, 0.0, pltpu.roll(cells, F, 1))
            total = total + jnp.where(lane >= F * F - F, 0.0, pltpu.roll(cells, F * F - F, 1))
            total = total + jnp.where(lane_z == 0, 0.0, pltpu.roll(cells, 1, 1))
            total = total + jnp.where(lane_z == F - 1, 0.0, pltpu.roll(cells, F * F - 1, 1))
            result = cells + visc * total
            fine_out[row : row + F, :] = jnp.where(active, result, 0.0)
            at = s * 48 + k * F
            advanced[at : at + F, :] = result
    for p in range(2):
        at = p * 96
        pooled[p * 48 : p * 48 + 48, :] = dot_right(advanced[at : at + 48, :], pool[0]) + dot_right(
            advanced[at + 48 : at + 96, :], pool[1]
        )
    means = pooled[pl.ds(0, 48, stride=2), :] + pooled[pl.ds(1, 48, stride=2), :]
    for j in range(PLANE):
        means_out[j] = means


def return_kernel(table, held, out):
    first = lax.broadcasted_iota(i32, (1, 128), 1) < 64
    for j in range(LINE_Z):
        for p in range(2):
            picks = []
            for h in range(2):
                x, _, y, local = split_slot(jnp.maximum(table[ROW_OWNER, j * 4 + 2 * p + h] - 1, 0))
                start = pl.multiple_of((local >> 1) * 24, 8)
                rows = held[x * LINE_Y + y, pl.ds(start, 24)]
                picks.append(jnp.where((local & 1) == h, rows, pltpu.roll(rows, 64, 1)))
            out[j, p * 24 : p * 24 + 24] = jnp.where(first, picks[0], picks[1])


def place_kernel(table, rcv, window, coarse_ref, coarse_out, spread, sem):
    me = lax.axis_index("gx_1")
    place = table[ROW_ANCHOR, SELF_TARGET]

    @pl.when(place >= 0)
    def _():
        y0 = pl.multiple_of(place >> 8, 8)
        z0 = place & 255
        z_tile = pl.multiple_of((z0 >> 7) * 128, 128)
        z_in = z0 & 127
        region = coarse_out.at[:, pl.ds(y0, 8), pl.ds(z_tile, 128)]
        for i in range(SLOTS):
            _, at, _, _ = split_slot(jnp.maximum(table[ROW_OWNER, me * 4 + i] - 1, 0))
            for k in range(3):
                start = ((i // 2) * 3 + k) * 8
                values = rcv[at, start : start + 8]
                for b in range(B):
                    shift = (z_in + 256 - (b * B + 64 * (i % 2))) & 127
                    spread[pl.ds((k * 32 + i * B) * B + b, B, stride=B), :] = pltpu.roll(values, shift, 1)
        lane = lax.broadcasted_iota(i32, (1, 128), 1)
        spread[...] = jnp.where((lane >= z_in) & (lane < z_in + B), spread[...], window[...])
        store = pltpu.make_async_copy(spread.reshape(96, 8, 128), region, sem)
        store.start()
        store.wait()


def vmem():
    return pl.BlockSpec(memory_space=pltpu.VMEM)


def smem():
    return pl.BlockSpec(memory_space=pltpu.SMEM)


def anywhere():
    return pl.BlockSpec(memory_space=pl.ANY)


def shape(*dims, dtype=f32):
    return jax.ShapeDtypeStruct(dims, dtype)


def on_device(coarse_field, fine_field, viscosity, corners, grid_slot, neighbors):
    fine = fine_field.reshape(3 * SLOTS * F, F * F)
    tiles = coarse_field.reshape(3, 32, 4, 8, 2, 128).transpose(0, 1, 2, 4, 3, 5).reshape(6144, 128)
    pack_const, beside = map(jnp.asarray, pack_constants())
    beside = beside.astype(jnp.bfloat16)
    table, own, other, planes, window = pl.pallas_call(
        pack_kernel,
        out_shape=(
            shape(8, 128, dtype=i32),
            shape(PACKED, 128),
            shape(PACKED, 128),
            shape(32, 128),
            shape(768, 128),
        ),
        in_specs=[vmem()] * 6,
        out_specs=(vmem(),) * 5,
        scratch_shapes=[pltpu.SMEM((8, 128), i32), pltpu.SemaphoreType.DMA(())],
        name="pack", compiler_params=pltpu.CompilerParams(vmem_limit_bytes=24 << 20),
    )(corners.T, grid_slot[None, :], neighbors.T, fine, tiles, pack_const)
    other = lax.ppermute(other, "gz", [(0, 1), (1, 0)])
    payload = pl.pallas_call(
        join_kernel,
        out_shape=shape(PLANE, FIRST, 128),
        in_specs=[vmem()] * 3,
        out_specs=vmem(),
        name="join",
        compiler_params=pltpu.CompilerParams(vmem_limit_bytes=8 << 20),
    )(own, other, planes)
    held = lax.all_to_all(payload, ("gx_0", "gy"), 0, 0)
    routed = pl.pallas_call(
        route_kernel,
        out_shape=shape(LINE_Z, SEND, 128),
        in_specs=[smem(), vmem(), vmem()],
        out_specs=vmem(),
        scratch_shapes=[pltpu.VMEM((LINE_Z * 34, 128), f32)] * 2,
        name="route",
        compiler_params=pltpu.CompilerParams(vmem_limit_bytes=8 << 20),
    )(table, held, beside)
    received = lax.all_to_all(routed, "gx_1", 0, 0)
    fine_out, means = pl.pallas_call(
        update_kernel,
        out_shape=(shape(3 * SLOTS * F, F * F), shape(PLANE, 48, 128)),
        in_specs=[smem()] + [vmem()] * 7,
        out_specs=(vmem(), vmem()),
        scratch_shapes=[
            pltpu.VMEM((64, 768), f32),
            pltpu.VMEM((8, 256), f32),
            pltpu.VMEM((192, 256), f32),
            pltpu.VMEM((96, 128), f32),
        ],
        name="update", compiler_params=pltpu.CompilerParams(vmem_limit_bytes=16 << 20),
    )(table, received, fine, viscosity.reshape(SLOTS * F, F * F), *(jnp.asarray(m, jnp.bfloat16) for m in constant_matrices()))
    held_means = lax.all_to_all(means, ("gx_0", "gy"), 0, 0)
    back = pl.pallas_call(
        return_kernel,
        out_shape=shape(LINE_Z, 48, 128),
        in_specs=[smem(), vmem()],
        out_specs=vmem(),
        name="send_back", compiler_params=pltpu.CompilerParams(vmem_limit_bytes=8 << 20),
    )(table, held_means)
    returned = lax.all_to_all(back, "gx_1", 0, 0)
    coarse_out = pl.pallas_call(
        place_kernel,
        out_shape=shape(96, 32, 256),
        in_specs=[smem(), vmem(), vmem(), anywhere()],
        out_specs=anywhere(),
        input_output_aliases={3: 0},
        scratch_shapes=[pltpu.VMEM((768, 128), f32), pltpu.SemaphoreType.DMA(())],
        name="place", compiler_params=pltpu.CompilerParams(vmem_limit_bytes=8 << 20),
    )(table, returned, window, coarse_field.reshape(96, 32, 256))
    return fine_out.reshape(fine_field.shape), coarse_out.reshape(coarse_field.shape)


def solution(mesh):
    split = Mesh(
        mesh.devices.reshape(LINE_X, LINE_Z, mesh.shape["gy"], mesh.shape["gz"]), ("gx_0", "gx_1", "gy", "gz")
    )
    in_specs = (
        P(None, GX, "gy", "gz"),
        P(None, GX_GY_GZ, None, None),
        P(GX_GY_GZ, None, None),
        P(),
        P(),
        P(),
    )
    out_specs = (P(None, GX_GY_GZ, None, None), P(None, GX, "gy", "gz"))
    return jax.shard_map(
        on_device, mesh=split, in_specs=in_specs, out_specs=out_specs, check_vma=False
    )
```

```python
import jax
import jax.numpy as jnp
import numpy as np
from jax import lax
from jax.experimental import pallas as pl
from jax.experimental.pallas import tpu as pltpu
from jax.sharding import Mesh
from jax.sharding import PartitionSpec as P

B = 8
F = 16
SLOTS = 4
SIDE = B + 2
LINE_X = 4
LINE_Z = 8
LINE_Y = 4
PLANE = LINE_X * LINE_Y
PACKED = 80
PAIRED = 72
FIRST = 88
SEND = 64
step_rate = 0.15
f32 = jnp.float32
i32 = jnp.int32
GX = ("gx_0", "gx_1")
GX_GY_GZ = ("gx_0", "gx_1", "gy", "gz")

ROW_SLOT, ROW_HOME, ROW_LOW, ROW_HIGH, ROW_OWNER, ROW_ANCHOR, ROW_ROUTE, ROW_SENDS = range(8)
SELF_TARGET = 8


def tangent_matrix():
    fine = np.arange(F)
    coarse = np.arange(SIDE)
    center = fine // 2 + 1
    other = np.where(fine % 2 == 0, center - 1, center + 1)
    return 0.75 * (coarse[None] == center[:, None]) + 0.25 * (coarse[None] == other[:, None])


def constant_matrices():
    tangent = tangent_matrix()
    along_x = np.zeros((64, 40))
    for fine in range(64):
        center = fine // 2
        other = center - 1 if fine % 2 == 0 else center + 1
        along_x[fine, center] += 0.75
        along_x[fine, 32 if other < 0 else 33 if other > 31 else other] += 0.25
    faces = np.zeros((128, 3, F, F))
    for k in range(3):
        for c in range(SIDE):
            faces[k * 10 + c, k, 0, :] += tangent[:, c]
            faces[30 + k * 10 + c, k, F - 1, :] += tangent[:, c]
            faces[60 + k * 10 + c, k, :, 0] += tangent[:, c]
            faces[90 + k * 10 + c, k, :, F - 1] += tangent[:, c]
    ends = np.zeros((128, F * F))
    ends[: SIDE * SIDE] = np.einsum("sa,tb->abst", tangent, tangent).reshape(SIDE * SIDE, F * F)
    pool = np.zeros((2, F, F, 128))
    for y in range(F):
        for z in range(F):
            for half in range(2):
                pool[half, y, z, half * 64 + (y // 2) * B + z // 2] = 0.125
    return (
        along_x.astype(np.float32),
        faces.reshape(128, 3 * F * F).astype(np.float32),
        ends.astype(np.float32),
        pool.reshape(2, F * F, 128).astype(np.float32),
    )


def pack_constants():
    out = np.zeros((40, 128))
    for k in range(3):
        for y in range(B):
            out[k * B + y, 60 + 10 * k + 1 + y] = 1.0
            out[k * B + y, 90 + 10 * k + 1 + y] = 1.0
        out[k * B, 10 * k : 10 * k + 10] = 0.25
        out[k * B + B - 1, 30 + 10 * k : 40 + 10 * k] = 0.25
        out[24 + k, 10 * k : 10 * k + 10] = 0.75
        out[24 + k, [60 + 10 * k, 90 + 10 * k]] = 1.0
        out[27 + k, 30 + 10 * k : 40 + 10 * k] = 0.75
        out[27 + k, [69 + 10 * k, 99 + 10 * k]] = 1.0
    beside = np.zeros((128, 128))
    for face in range(2):
        for k in range(3):
            for c in range(SIDE):
                at = face * 30 + k * 10 + c
                edge = face * 9 + 10 * k
                beside[at, at] = 0.75
                beside[at, 60 + edge] = {0: 0.75, 1: 0.25}.get(c, 0.0)
                beside[at, 90 + edge] = {9: 0.75, 8: 0.25}.get(c, 0.0)
    lanes = np.arange(128)
    out[32] = np.where(lanes < 60, lanes % 10, np.where(lanes < 90, 0, np.where(lanes < 120, 9, -999)))
    out[33] = np.where(lanes < 60, -999, np.where(lanes < 90, 1, np.where(lanes < 120, 8, -999)))
    out[34] = np.where(lanes < 60, 1.0, 0.75)
    out[35] = 0.25
    return out.astype(np.float32), beside.astype(np.float32)


def thirds(values):
    high = values.astype(jnp.bfloat16)
    rest = values - high.astype(f32)
    middle = rest.astype(jnp.bfloat16)
    return high, middle, (rest - middle.astype(f32)).astype(jnp.bfloat16)


def dot_right(values, weights):
    parts = [jnp.dot(part, weights, preferred_element_type=f32) for part in thirds(values)]
    return parts[0] + (parts[1] + parts[2])


def dot_left(weights, values):
    parts = [jnp.dot(weights, part, preferred_element_type=f32) for part in thirds(values)]
    return parts[0] + (parts[1] + parts[2])


def position():
    return tuple(lax.axis_index(name) for name in GX_GY_GZ)


def make_table(corners_ref, slots_ref, near_ref, table_ref):
    my_x, my_z, my_y, my_c = position()
    cx, cy, cz = corners_ref[0:1, :], corners_ref[1:2, :], corners_ref[2:3, :]
    gs = slots_ref[0:1, :]
    grids = gs.shape[1]
    low, high = near_ref[0:1, :], near_ref[1:2, :]
    gx, gy, gz = cx >> 5, cy >> 5, cz >> 8
    box = (cx >> 3) & 3
    home = gx * LINE_Y + gy
    brick_key = (home * 2 + gz) * SLOTS + box
    word = (1 + box * 2 + home * 8 + (low + 1) * 1024).astype(f32)
    sub = lax.broadcasted_iota(i32, (32, 1), 0)
    eye = (lax.broadcasted_iota(i32, (32, 128), 0) == lax.broadcasted_iota(i32, (32, 128), 1)).astype(f32)

    def to_row(column):
        return jnp.sum(eye * column, axis=0, keepdims=True)

    def pick(match, values):
        return jnp.sum(jnp.where(match, values, 0.0), axis=1, keepdims=True)

    def device_of(j):
        return ((my_x * LINE_Z + j) * LINE_Y + my_y) * 2 + my_c

    keys = device_of(sub >> 2) * SLOTS + (sub & 3)
    held = keys == gs
    words = pick(held, word)
    high_grid = pick(held, (high + 1).astype(f32)).astype(i32)
    low_grid = words.astype(i32) >> 10
    grid_ids = lax.broadcasted_iota(i32, (1, grids), 1) + 1
    slot_plus = (gs + 1).astype(f32)
    low_slot = pick(low_grid == grid_ids, slot_plus).astype(i32)
    high_slot = pick(high_grid == grid_ids, slot_plus).astype(i32)
    devices = gs >> 2
    bit = (jnp.int32(1) << box).astype(f32)

    def boxes_on(device):
        return pick(device == devices, bit).astype(i32)

    mine = device_of(sub >> 2)
    my_mask = boxes_on(mine)
    my_box = (words.astype(i32) >> 1) & 3
    lanes = lax.broadcasted_iota(i32, (32, 128), 1)
    same_j = (sub >> 2) == (lanes >> 2)
    route_row = jnp.zeros((1, 128), f32)
    sends_row = jnp.zeros((1, 128), f32)
    near_words = []
    for side, slot in enumerate((low_slot, high_slot)):
        device = (slot - 1) >> 2
        near_mask = boxes_on(device)
        near_box = (my_box + (3, 1)[side]) & 3
        outer = (slot > 0) & (device != mine)

        def before(mask, at):
            return ((mask & ((jnp.int32(1) << at) - 1)) != 0).astype(i32)

        def after(mask, at):
            return ((mask >> (at + 1)) != 0).astype(i32)

        if side == 0:
            here, there = before(my_mask, my_box), 2 + after(near_mask, near_box)
        else:
            here, there = 2 + after(my_mask, my_box), before(near_mask, near_box)
        target = jnp.where(same_j & ((lanes & 3) == here) & outer, 1.0, 0.0)
        plane = (device >> 6) * LINE_Y + ((device >> 1) & 3)
        code = (plane * 4 + there + 1).astype(f32)
        route_row = route_row + jnp.sum(target * code, axis=0, keepdims=True)
        sends_row = sends_row + jnp.sum(target * ((sub & 3) + 1).astype(f32), axis=0, keepdims=True)
        word = jnp.where(outer, 2 + here * 4 + ((device >> 3) & 7) * 16, 1 + ((slot - 1) & 3) * 4)
        near_words.append(jnp.where(slot > 0, word, 0).astype(f32))
    owner = pick(keys == brick_key, slot_plus)
    sub8 = lax.broadcasted_iota(i32, (8, 1), 0)
    on_device = device_of(sub8) == (gs >> 2)
    in_y = cy & 31
    side_y = jnp.where(in_y == 0, 128, jnp.where(in_y == 24, 256, 0))
    homes = jnp.max(jnp.where(on_device, (home + 1 + side_y).astype(f32), 0.0), axis=1, keepdims=True)
    homes = jnp.concatenate([homes, jnp.zeros((24, 1), f32)], axis=0)
    sub24 = lax.broadcasted_iota(i32, (24, 1), 0)
    target_x = my_x * LINE_Z + my_z + jnp.where(sub24 >= 12, 1, jnp.where(sub24 >= 6, 0, -1))
    target_x = jnp.where(sub24 >= 18, -1, target_x)
    in_x = sub24 - jnp.where(sub24 >= 12, 12, jnp.where(sub24 >= 6, 6, 0))
    target_y = my_y + (in_x >> 1) - 1
    target_z = jnp.where((in_x & 1) == 0, my_c, 1 - my_c)
    near_brick = (target_x == gx) & (target_y == gy) & (target_z == gz)
    place = ((cy & 31) * 256 + (cz & 255)).astype(f32)
    anchors = jnp.max(jnp.where(near_brick, place, -1.0), axis=1, keepdims=True)
    anchors = jnp.concatenate([anchors, jnp.zeros((8, 1), f32)], axis=0)
    rows = [to_row(v) for v in (words, homes, *near_words, owner, anchors)] + [route_row, sends_row]
    for r, row in enumerate(rows):
        table_ref[r : r + 1, :] = row.astype(i32)


def pack_kernel(
    corners_ref, slots_ref, near_ref, fine_ref, brick, const,
    table_ref, own_ref, other_ref, planes_ref, window_ref,
    table, table_sem,
):
    make_table(corners_ref, slots_ref, near_ref, table_ref)
    fetch = pltpu.make_async_copy(table_ref, table, table_sem)
    fetch.start()
    own_ref[...] = jnp.zeros_like(own_ref)
    other_ref[...] = jnp.zeros_like(other_ref)
    planes_ref[...] = jnp.zeros_like(planes_ref)
    fetch.wait()
    me = lax.axis_index("gx_1")
    for e in range(4):
        s = jnp.maximum(table[ROW_SENDS, me * 4 + e] - 1, 0)
        for k in range(3):
            tile = fine_ref[pl.ds(pl.multiple_of((k * SLOTS + s) * F + (0 if e < 2 else 8), 8), 8), :]
            row = tile[0:1] if e < 2 else tile[7:8]
            for half in range(2):
                at = e * 8 + half * 3 + k
                planes_ref[at : at + 1, :] = row[:, half * 128 : half * 128 + 128]

    my_c = lax.axis_index("gz")
    lane = lax.broadcasted_iota(i32, (1, 128), 1)
    sub3 = lax.broadcasted_iota(i32, (3, 1), 0)

    def from_second(z_base):
        return z_base + ((lane - z_base) & 127) >= 128

    def window_rows(at, second):
        return jnp.where(second, brick[at(8)], brick[at(0)])

    def to_front(rows, z_base, valid):
        rows = pltpu.roll(rows, (256 - z_base) & 127, 1)
        at = z_base + lane
        return jnp.where((lane < SIDE) & (at >= 0) & (at < 256) & valid, rows, 0.0)

    def shifted(start, count, stride, z_base, valid):
        rows = window_rows(
            lambda tile: (pl.ds(start + tile, count, stride=stride), slice(None)), from_second(z_base)
        )
        return to_front(rows, z_base, valid)

    def tile_row(y):
        return (y >> 3) * 16 + (y & 7)

    def ends_of(u):
        low = 0.75 * u[:, 0:1] + 0.25 * u[:, 1:2]
        high = 0.75 * u[:, 9:10] + 0.25 * u[:, 8:9]
        return low, high

    def beside_rows(dy, z_base):
        total = jnp.zeros((32, 128), f32)
        y, face = (31, 0) if dy == 1 else (0, 30)
        for k in range(3):
            u = shifted(k * 2048 + tile_row(y), 32, 64, z_base, True)
            total = total + (pltpu.roll(u, face + 10 * k, 1) if face + k else u)
        return total

    def diagonal_row(x, dy, z_base):
        y, face = (31, 0) if dy == 1 else (0, 30)
        face += 0 if x else 60
        u = shifted(x * 64 + tile_row(y), 3, 2048, z_base, True)
        row = jnp.where(sub3 == 0, u, jnp.where(sub3 == 1, pltpu.roll(u, 10, 1), pltpu.roll(u, 20, 1)))
        row = jnp.sum(row, axis=0, keepdims=True)
        return pltpu.roll(row, face, 1) if face else row

    def all_rows(y0, z_base):
        offset = (lax.broadcasted_iota(i32, (128, 1), 0) - z_base) & 127
        offset = jnp.where((offset + z_base >= 0) & (offset + z_base < 256), offset, 500).astype(f32)
        window = jnp.where(offset == const[32:33, :], const[34:35, :], 0.0)
        window = window + jnp.where(offset == const[33:34, :], const[35:36, :], 0.0)
        start = (y0 >> 3) * 16
        low_y, high_y = jnp.maximum(y0 - 1, 0), jnp.minimum(y0 + B, 31)
        tiles = from_second(z_base)
        parts = []
        for n in range(96):
            first = n * 64 + start
            parts.append(
                window_rows(lambda tile, first=first: (pl.ds(pl.multiple_of(first + tile, 8), 8), slice(None)), tiles)
            )
        for y in (low_y, high_y):
            first = tile_row(y)
            parts.append(
                window_rows(lambda tile, first=first: (pl.ds(first + tile, 96, stride=64), slice(None)), tiles)
            )
        cells = dot_right(jnp.concatenate(parts, axis=0), window.astype(jnp.bfloat16))
        inner = cells[:768].reshape(3, 32, B, 128)
        total = inner[0] * const[0:8, :][None]
        total = total + inner[1] * const[8:16, :][None]
        total = total + inner[2] * const[16:24, :][None]
        rows = jnp.sum(total, axis=1)
        for k in range(3):
            low = jnp.where(y0 > 0, const[24 + k : 25 + k, :], 0.0)
            high = jnp.where(y0 < 24, const[27 + k : 28 + k, :], 0.0)
            rows = rows + low * cells[768 + 32 * k : 800 + 32 * k] + high * cells[864 + 32 * k : 896 + 32 * k]
        flats = []
        for x in (0, 31):
            for k in range(3):
                tile = jnp.where(lane < SIDE, cells[(k * 32 + x) * B : (k * 32 + x) * B + B], 0.0)
                flat = jnp.sum(pltpu.roll(tile, SIDE, 1, stride=SIDE, stride_axis=0), axis=0, keepdims=True)
                low = cells[768 + 32 * k + x : 769 + 32 * k + x]
                high = cells[864 + 32 * k + x : 865 + 32 * k + x]
                flat = flat + jnp.where((lane < SIDE) & (y0 > 0), low, 0.0)
                flat = flat + pltpu.roll(jnp.where((lane < SIDE) & (y0 < 24), high, 0.0), 90, 1)
                flats.append(flat)
        return rows, flats

    def edge_rows(x, y0, z_base):
        start = (y0 >> 3) * 16
        tiles = from_second(z_base)
        rows = []
        for k in range(3):
            first = (k * 32 + x) * 64 + start
            rows.append(
                window_rows(lambda tile, first=first: (pl.ds(pl.multiple_of(first + tile, 8), 8), slice(None)), tiles)
            )
        u = to_front(jnp.concatenate(rows, axis=0), z_base, True)
        low, high = ends_of(u)
        flats, faces = [], []
        for k in range(3):
            tile = u[k * B : k * B + B]
            flats.append(jnp.sum(pltpu.roll(tile, SIDE, 1, stride=SIDE, stride_axis=0), axis=0, keepdims=True))
            tile = pltpu.roll(tile, 10 * k, 1) if k else tile
            faces.append(tile + pltpu.roll(tile, 30, 1))
        spread = jnp.where(lane < 60, jnp.concatenate(faces, axis=0), jnp.where(lane < 90, low, high))
        total = jnp.sum(spread * const[0:24, :], axis=0, keepdims=True)
        flat = jnp.where(sub3 == 0, flats[0], jnp.where(sub3 == 1, flats[1], flats[2]))
        row = jnp.zeros((3, 128), f32)
        for t, y, valid in ((0, y0 - 1, y0 > 0), (SIDE - 1, y0 + B, y0 < 24)):
            u = shifted(x * 64 + tile_row(jnp.clip(y, 0, 31)), 3, 2048, z_base, valid)
            flat = flat + (pltpu.roll(u, 10 * t, 1) if t else u)
            low, high = ends_of(u)
            row = jnp.where(lane == 60 + 10 * sub3 + t, low, row)
            row = jnp.where(lane == 90 + 10 * sub3 + t, high, row)
            face = 30 if t else 0
            spread = jnp.where(
                sub3 == 0,
                pltpu.roll(u, face, 1) if face else u,
                jnp.where(sub3 == 1, pltpu.roll(u, face + 10, 1), pltpu.roll(u, face + 20, 1)),
            )
            row = row + 0.75 * spread
        return flat, total + jnp.sum(row, axis=0, keepdims=True)

    for dz in range(2):
        out = other_ref if dz else own_ref
        z_shift = 256 * (1 - 2 * my_c) if dz else 0
        for dy in (-1, 0, 1):
            for dx in (0, -1, 1):
                place = table[ROW_ANCHOR, (dx + 1) * 6 + (dy + 1) * 2 + dz]
                y0, z0 = place >> 8, place & 255
                z_base = z0 - 1 + z_shift
                near = place >= 0
                if dy == 1:
                    near &= y0 == 0
                if dy == -1:
                    near &= y0 == 24
                if dz:
                    near &= z0 == jnp.where(my_c == 0, 0, 248)

                @pl.when(near)
                def _(out=out, dz=dz, dx=dx, dy=dy, y0=y0, z0=z0, z_base=z_base):
                    if dy and dx:
                        out[38:39, :] += diagonal_row(0 if dx == -1 else 31, dy, z_base)
                    elif dy:
                        out[48:80, :] += beside_rows(dy, z_base)
                    elif dx:
                        x, at = (0, 44) if dx == -1 else (31, 40)
                        flat, row = edge_rows(x, y0, z_base)
                        out[at : at + 3, :] = 0.75 * flat
                        out[at + 3 : at + 4, :] = row
                    else:
                        rows, flats = all_rows(y0, z_base)
                        out[0:32, :] = rows
                        for i, flat in enumerate(flats):
                            out[32 + i : 33 + i, :] = 0.25 * flat
                        if dz == 0:
                            start = (y0 >> 3) * 16 + (z0 >> 7) * 8
                            for n in range(96):
                                tile = brick[pl.ds(pl.multiple_of(n * 64 + start, 8), 8), :]
                                window_ref[n * 8 : n * 8 + 8, :] = tile


def split_slot(slot):
    device = slot >> 2
    return device >> 6, (device >> 3) & 7, (device >> 1) & 3, slot & 3


def join_kernel(own, other, planes, out):
    total = own[...] + other[...]
    sub = lax.broadcasted_iota(i32, (8, 1), 0)
    tiles = []
    for e in range(4):
        pair = jnp.where(sub == 6, total[40 + 2 * e : 41 + 2 * e], total[41 + 2 * e : 42 + 2 * e])
        tiles.append(jnp.where(sub < 6, planes[e * 8 : e * 8 + 8, :], pair))
    two = total[48:64] + pltpu.roll(total[64:80], 64, 1)
    payload = jnp.concatenate([total[:40]] + tiles + [two], axis=0)
    for j in range(PLANE):
        out[j] = payload


def route_kernel(table, held, beside_ref, out, rows, spread):
    sub = lax.broadcasted_iota(i32, (8, 1), 0)
    lane = lax.broadcasted_iota(i32, (1, 128), 1)

    def line_of(gx):
        return (jnp.clip(gx, 0, 31) >> 3) * LINE_Y

    def read(j):
        code = jnp.maximum(table[ROW_HOME, j] - 1, 0)
        home, edge = code & 127, code >> 7
        gx, gy = home >> 2, home & 3
        near_y = jnp.where(edge == 1, gy - 1, gy + 1)
        used = (edge > 0) & (near_y >= 0) & (near_y < LINE_Y)
        start = jnp.where(edge == 2, 30, 0)
        keep = (lane >= start) & (lane < start + 30) & used
        return gx, gy, jnp.clip(near_y, 0, LINE_Y - 1), edge, keep

    for j in range(LINE_Z):
        gx, _, near_y, _, keep = read(j)
        both = held[line_of(gx) + near_y, PAIRED:FIRST]
        rows[j * 32 : j * 32 + 16, :] = jnp.where(keep, both, 0.0)
        rows[j * 32 + 16 : j * 32 + 32, :] = jnp.where(keep, pltpu.roll(both, 64, 1), 0.0)
        for side in range(2):
            row = held[line_of(gx + (1 if side else -1)) + near_y, 32:40][6:7]
            at = LINE_Z * 32 + j * 2 + side
            rows[at : at + 1, :] = jnp.where(keep, pltpu.roll(row, 68, 1) if side else row, 0.0)
    spread[...] = dot_right(rows[...], beside_ref[...])

    for j in range(LINE_Z):
        gx, gy, _, edge, _ = read(j)
        home_at = line_of(gx) + gy
        shift = jnp.where(edge == 2, 60, 0)
        kept = (lane >= jnp.where(edge == 2, 90, 0)) & (lane < jnp.where(edge == 2, 100, SIDE))

        def flats(row):
            return [jnp.where(kept, pltpu.roll(row, (shift + 128 - 10 * k) & 127, 1), 0.0) for k in range(3)]

        out[j, 0:32] = held[home_at, 0:32] + spread[j * 32 : j * 32 + 32, :]
        ends = held[home_at, 32:40]
        for side in range(2):
            near = rows[j * 32 + 31 * side : j * 32 + 31 * side + 1, :]
            at = LINE_Z * 32 + j * 2 + side
            source = line_of(gx + (1 if side else -1)) + gy
            pair = [held[source, 40 + (side * 2 + half) * 8 : 48 + (side * 2 + half) * 8] for half in range(2)]
            ghosts = [ends[3 * side + k : 3 * side + k + 1] + 0.25 * row for k, row in enumerate(flats(near))]
            pieces = (pair[0][6:7], pair[0][7:8], pair[1][6:7])
            ghosts += [piece + 0.75 * row for piece, row in zip(pieces, flats(rows[at : at + 1, :]))]
            ghosts.append(pair[1][7:8] + spread[at : at + 1, :])
            tile = jnp.zeros((8, 128), f32)
            for i, row in enumerate(ghosts):
                tile = jnp.where(sub == i, row, tile)
            for half in range(2):
                e = side * 2 + half
                code = table[ROW_ROUTE, j * 4 + e] - 1
                start = pl.multiple_of(40 + (jnp.maximum(code, 0) & 3) * 8, 8)
                plane = held[jnp.maximum(code, 0) >> 2, pl.ds(start, 8)]
                if half == 0:
                    plane = jnp.where((sub < 6) & (code >= 0), plane, tile)
                out[j, 32 + e * 8 : 40 + e * 8] = plane


def update_kernel(
    table, rcv, fine_ref, visc_ref, along_x, faces, ends, pool,
    fine_out, means_out,
    sums, planes, advanced, pooled, kept, sem,
):
    me = lax.axis_index("gx_1")
    gx = (jnp.maximum(table[ROW_HOME, me] - 1, 0) & 127) >> 2
    at_home, at_low, at_high = gx & 7, (gx + 7) & 7, (gx + 1) & 7
    sub8 = lax.broadcasted_iota(i32, (8, 1), 0)

    low = jnp.where(gx > 0, rcv[at_low, 32:40], 0.0)
    high = jnp.where(gx < 31, rcv[at_high, 48:56], 0.0)
    beyond = jnp.where(sub8 == 0, low[6:7], jnp.where(sub8 == 1, high[6:7], 0.0))
    body = jnp.concatenate([rcv[at_home, 0:32], beyond], axis=0)
    sums[...] = dot_right(dot_left(along_x[...], body), faces[...])
    own = (rcv[at_home, 32:40], rcv[at_home, 48:56])
    flat = jnp.zeros((8, 128), f32)
    for side, other in enumerate((low, high)):
        for k in range(3):
            flat = jnp.where(sub8 == 3 * side + k, own[side][k : k + 1] + other[3 + k : 4 + k], flat)
    planes[...] = dot_right(flat, ends[...])
    lane = lax.broadcasted_iota(i32, (1, F * F), 1)
    sub = lax.broadcasted_iota(i32, (F, 1), 0)
    lane_z = lane & (F - 1)
    for s in range(SLOTS):
        word = table[ROW_SLOT, me * 4 + s]
        active = (word & 1) == 1
        box_start = pl.multiple_of(((word >> 1) & 3) * F, F)
        low_word = table[ROW_LOW, me * 4 + s]
        high_word = table[ROW_HIGH, me * 4 + s]
        low_tile = rcv[low_word >> 4, pl.ds(pl.multiple_of(32 + ((low_word >> 2) & 3) * 8, 8), 8)]
        high_tile = rcv[high_word >> 4, pl.ds(pl.multiple_of(32 + ((high_word >> 2) & 3) * 8, 8), 8)]
        visc = step_rate * visc_ref[s * F : s * F + F, :]
        for k in range(3):
            row = (k * SLOTS + s) * F
            cells = fine_ref[row : row + F, :]
            lower = jnp.concatenate([low_tile[k : k + 1], low_tile[3 + k : 4 + k]], axis=1)
            upper = jnp.concatenate([high_tile[k : k + 1], high_tile[3 + k : 4 + k]], axis=1)
            low_row = pl.multiple_of((k * SLOTS + ((low_word >> 2) & 3)) * F + 8, 8)
            high_row = pl.multiple_of((k * SLOTS + ((high_word >> 2) & 3)) * F, 8)
            lower = jnp.where((low_word & 3) == 1, fine_ref[pl.ds(low_row, 8), :][7:8], lower)
            upper = jnp.where((high_word & 3) == 1, fine_ref[pl.ds(high_row, 8), :][0:1], upper)
            lower = jnp.where(low_word > 0, lower, planes[k : k + 1, :])
            upper = jnp.where(high_word > 0, upper, planes[3 + k : 4 + k, :])
            total = sums[pl.ds(box_start, F), k * 256 : k * 256 + 256] - 6.0 * cells
            total = total + jnp.where(sub == 0, lower, pltpu.roll(cells, 1, 0))
            total = total + jnp.where(sub == F - 1, upper, pltpu.roll(cells, F - 1, 0))
            total = total + jnp.where(lane < F, 0.0, pltpu.roll(cells, F, 1))
            total = total + jnp.where(lane >= F * F - F, 0.0, pltpu.roll(cells, F * F - F, 1))
            total = total + jnp.where(lane_z == 0, 0.0, pltpu.roll(cells, 1, 1))
            total = total + jnp.where(lane_z == F - 1, 0.0, pltpu.roll(cells, F * F - 1, 1))
            result = cells + visc * total
            kept[row : row + F, :] = jnp.where(active, result, 0.0)
            at = s * 48 + k * F
            advanced[at : at + F, :] = result
    store = pltpu.make_async_copy(kept, fine_out, sem)
    store.start()
    for p in range(2):
        at = p * 96
        pooled[p * 48 : p * 48 + 48, :] = dot_right(advanced[at : at + 48, :], pool[0]) + dot_right(
            advanced[at + 48 : at + 96, :], pool[1]
        )
    means = pooled[pl.ds(0, 48, stride=2), :] + pooled[pl.ds(1, 48, stride=2), :]
    for j in range(PLANE):
        means_out[j] = means
    store.wait()


def return_kernel(table, held, out):
    first = lax.broadcasted_iota(i32, (1, 128), 1) < 64
    for j in range(LINE_Z):
        for p in range(2):
            picks = []
            for h in range(2):
                x, _, y, local = split_slot(jnp.maximum(table[ROW_OWNER, j * 4 + 2 * p + h] - 1, 0))
                start = pl.multiple_of((local >> 1) * 24, 8)
                rows = held[x * LINE_Y + y, pl.ds(start, 24)]
                picks.append(jnp.where((local & 1) == h, rows, pltpu.roll(rows, 64, 1)))
            out[j, p * 24 : p * 24 + 24] = jnp.where(first, picks[0], picks[1])


def place_kernel(table, rcv, window, coarse_ref, coarse_out, spread, sem):
    me = lax.axis_index("gx_1")
    place = table[ROW_ANCHOR, SELF_TARGET]

    @pl.when(place >= 0)
    def _():
        y0 = pl.multiple_of(place >> 8, 8)
        z0 = place & 255
        z_tile = pl.multiple_of((z0 >> 7) * 128, 128)
        z_in = z0 & 127
        lane = lax.broadcasted_iota(i32, (1, 128), 1)
        owners = [split_slot(jnp.maximum(table[ROW_OWNER, me * 4 + i] - 1, 0))[1] for i in range(SLOTS)]
        stores = []
        for k in range(3):
            for i in range(SLOTS):
                start = ((i // 2) * 3 + k) * 8
                values = rcv[owners[i], start : start + 8]
                for b in range(B):
                    shift = (z_in + 256 - (b * B + 64 * (i % 2))) & 127
                    spread[pl.ds((k * 32 + i * B) * B + b, B, stride=B), :] = pltpu.roll(values, shift, 1)
            rows = pl.ds(k * 256, 256)
            spread[rows, :] = jnp.where((lane >= z_in) & (lane < z_in + B), spread[rows, :], window[rows, :])
            part = pl.ds(k * 32, 32)
            stores.append(
                pltpu.make_async_copy(
                    spread.reshape(96, 8, 128).at[part],
                    coarse_out.at[part, pl.ds(y0, 8), pl.ds(z_tile, 128)],
                    sem.at[k],
                )
            )
            stores[-1].start()
        for store in stores:
            store.wait()


def vmem():
    return pl.BlockSpec(memory_space=pltpu.VMEM)


def smem():
    return pl.BlockSpec(memory_space=pltpu.SMEM)


def anywhere():
    return pl.BlockSpec(memory_space=pl.ANY)


def shape(*dims, dtype=f32):
    return jax.ShapeDtypeStruct(dims, dtype)


def on_device(coarse_field, fine_field, viscosity, corners, grid_slot, neighbors):
    fine = fine_field.reshape(3 * SLOTS * F, F * F)
    tiles = coarse_field.reshape(3, 32, 4, 8, 2, 128).transpose(0, 1, 2, 4, 3, 5).reshape(6144, 128)
    pack_const, beside = map(jnp.asarray, pack_constants())
    beside = beside.astype(jnp.bfloat16)
    table, own, other, planes, window = pl.pallas_call(
        pack_kernel,
        out_shape=(
            shape(8, 128, dtype=i32),
            shape(PACKED, 128),
            shape(PACKED, 128),
            shape(32, 128),
            shape(768, 128),
        ),
        in_specs=[vmem()] * 6,
        out_specs=(vmem(),) * 5,
        scratch_shapes=[pltpu.SMEM((8, 128), i32), pltpu.SemaphoreType.DMA(())],
        name="pack", compiler_params=pltpu.CompilerParams(vmem_limit_bytes=24 << 20),
    )(corners.T, grid_slot[None, :], neighbors.T, fine, tiles, pack_const)
    other = lax.ppermute(other, "gz", [(0, 1), (1, 0)])
    payload = pl.pallas_call(
        join_kernel,
        out_shape=shape(PLANE, FIRST, 128),
        in_specs=[vmem()] * 3,
        out_specs=vmem(),
        name="join",
        compiler_params=pltpu.CompilerParams(vmem_limit_bytes=8 << 20),
    )(own, other, planes)
    held = lax.all_to_all(payload, ("gx_0", "gy"), 0, 0)
    routed = pl.pallas_call(
        route_kernel,
        out_shape=shape(LINE_Z, SEND, 128),
        in_specs=[smem(), vmem(), vmem()],
        out_specs=vmem(),
        scratch_shapes=[pltpu.VMEM((LINE_Z * 34, 128), f32)] * 2,
        name="route",
        compiler_params=pltpu.CompilerParams(vmem_limit_bytes=8 << 20),
    )(table, held, beside)
    received = lax.all_to_all(routed, "gx_1", 0, 0)
    fine_out, means = pl.pallas_call(
        update_kernel,
        out_shape=(shape(3 * SLOTS * F, F * F), shape(PLANE, 48, 128)),
        in_specs=[smem()] + [vmem()] * 7,
        out_specs=(anywhere(), vmem()),
        scratch_shapes=[
            pltpu.VMEM((64, 768), f32),
            pltpu.VMEM((8, 256), f32),
            pltpu.VMEM((192, 256), f32),
            pltpu.VMEM((96, 128), f32),
            pltpu.VMEM((192, 256), f32),
            pltpu.SemaphoreType.DMA(()),
        ],
        name="update", compiler_params=pltpu.CompilerParams(vmem_limit_bytes=16 << 20),
    )(table, received, fine, viscosity.reshape(SLOTS * F, F * F), *(jnp.asarray(m, jnp.bfloat16) for m in constant_matrices()))
    held_means = lax.all_to_all(means, ("gx_0", "gy"), 0, 0)
    back = pl.pallas_call(
        return_kernel,
        out_shape=shape(LINE_Z, 48, 128),
        in_specs=[smem(), vmem()],
        out_specs=vmem(),
        name="send_back", compiler_params=pltpu.CompilerParams(vmem_limit_bytes=8 << 20),
    )(table, held_means)
    returned = lax.all_to_all(back, "gx_1", 0, 0)
    coarse_out = pl.pallas_call(
        place_kernel,
        out_shape=shape(96, 32, 256),
        in_specs=[smem(), vmem(), vmem(), anywhere()],
        out_specs=anywhere(),
        input_output_aliases={3: 0},
        scratch_shapes=[pltpu.VMEM((768, 128), f32), pltpu.SemaphoreType.DMA((3,))],
        name="place", compiler_params=pltpu.CompilerParams(vmem_limit_bytes=8 << 20),
    )(table, returned, window, coarse_field.reshape(96, 32, 256))
    return fine_out.reshape(fine_field.shape), coarse_out.reshape(coarse_field.shape)


def solution(mesh):
    split = Mesh(
        mesh.devices.reshape(LINE_X, LINE_Z, mesh.shape["gy"], mesh.shape["gz"]), ("gx_0", "gx_1", "gy", "gz")
    )
    in_specs = (
        P(None, GX, "gy", "gz"),
        P(None, GX_GY_GZ, None, None),
        P(GX_GY_GZ, None, None),
        P(),
        P(),
        P(),
    )
    out_specs = (P(None, GX_GY_GZ, None, None), P(None, GX, "gy", "gz"))
    return jax.shard_map(
        on_device, mesh=split, in_specs=in_specs, out_specs=out_specs, check_vma=False
    )
```

```python
import jax
import jax.numpy as jnp
import numpy as np
from jax import lax
from jax.experimental import pallas as pl
from jax.experimental.pallas import tpu as pltpu
from jax.sharding import Mesh
from jax.sharding import PartitionSpec as P

B = 8
F = 16
SLOTS = 4
SIDE = B + 2
LINE_X = 4
LINE_Z = 8
LINE_Y = 4
PLANE = LINE_X * LINE_Y
PACKED = 80
PAIRED = 72
FIRST = 88
SEND = 56
step_rate = 0.15
f32 = jnp.float32
i32 = jnp.int32
GX = ("gx_0", "gx_1")
GX_GY_GZ = ("gx_0", "gx_1", "gy", "gz")

ROW_SLOT, ROW_HOME, ROW_LOW, ROW_HIGH, ROW_OWNER, ROW_ANCHOR, ROW_ROUTE, ROW_SENDS = range(8)
SELF_TARGET = 8


def tangent_matrix():
    fine = np.arange(F)
    coarse = np.arange(SIDE)
    center = fine // 2 + 1
    other = np.where(fine % 2 == 0, center - 1, center + 1)
    return 0.75 * (coarse[None] == center[:, None]) + 0.25 * (coarse[None] == other[:, None])


def constant_matrices():
    tangent = tangent_matrix()
    along_x = np.zeros((64, 40))
    for fine in range(64):
        center = fine // 2
        other = center - 1 if fine % 2 == 0 else center + 1
        along_x[fine, center] += 0.75
        along_x[fine, 32 if other < 0 else 33 if other > 31 else other] += 0.25
    faces = np.zeros((128, 3, F, F))
    for k in range(3):
        for c in range(SIDE):
            faces[k * 10 + c, k, 0, :] += tangent[:, c]
            faces[30 + k * 10 + c, k, F - 1, :] += tangent[:, c]
            faces[60 + k * 10 + c, k, :, 0] += tangent[:, c]
            faces[90 + k * 10 + c, k, :, F - 1] += tangent[:, c]
    ends = np.zeros((128, F * F))
    ends[: SIDE * SIDE] = np.einsum("sa,tb->abst", tangent, tangent).reshape(SIDE * SIDE, F * F)
    pool = np.zeros((2, F, F, 128))
    for y in range(F):
        for z in range(F):
            for half in range(2):
                pool[half, y, z, half * 64 + (y // 2) * B + z // 2] = 0.125
    return (
        along_x.astype(np.float32),
        faces.reshape(128, 3 * F * F).astype(np.float32),
        ends.astype(np.float32),
        pool.reshape(2, F * F, 128).astype(np.float32),
    )


def pack_constants():
    out = np.zeros((40, 128))
    for k in range(3):
        for y in range(B):
            out[k * B + y, 60 + 10 * k + 1 + y] = 1.0
            out[k * B + y, 90 + 10 * k + 1 + y] = 1.0
        out[k * B, 10 * k : 10 * k + 10] = 0.25
        out[k * B + B - 1, 30 + 10 * k : 40 + 10 * k] = 0.25
        out[24 + k, 10 * k : 10 * k + 10] = 0.75
        out[24 + k, [60 + 10 * k, 90 + 10 * k]] = 1.0
        out[27 + k, 30 + 10 * k : 40 + 10 * k] = 0.75
        out[27 + k, [69 + 10 * k, 99 + 10 * k]] = 1.0
    beside = np.zeros((128, 128))
    for face in range(2):
        for k in range(3):
            for c in range(SIDE):
                at = face * 30 + k * 10 + c
                edge = face * 9 + 10 * k
                beside[at, at] = 0.75
                beside[at, 60 + edge] = {0: 0.75, 1: 0.25}.get(c, 0.0)
                beside[at, 90 + edge] = {9: 0.75, 8: 0.25}.get(c, 0.0)
    lanes = np.arange(128)
    out[32] = np.where(lanes < 60, lanes % 10, np.where(lanes < 90, 0, np.where(lanes < 120, 9, -999)))
    out[33] = np.where(lanes < 60, -999, np.where(lanes < 90, 1, np.where(lanes < 120, 8, -999)))
    out[34] = np.where(lanes < 60, 1.0, 0.75)
    out[35] = 0.25
    return out.astype(np.float32), beside.astype(np.float32)


def thirds(values):
    high = values.astype(jnp.bfloat16)
    rest = values - high.astype(f32)
    middle = rest.astype(jnp.bfloat16)
    return high, middle, (rest - middle.astype(f32)).astype(jnp.bfloat16)


def dot_right(values, weights):
    parts = [jnp.dot(part, weights, preferred_element_type=f32) for part in thirds(values)]
    return parts[0] + (parts[1] + parts[2])


def dot_left(weights, values):
    parts = [jnp.dot(weights, part, preferred_element_type=f32) for part in thirds(values)]
    return parts[0] + (parts[1] + parts[2])


def position():
    return tuple(lax.axis_index(name) for name in GX_GY_GZ)


def make_table(corners_ref, slots_ref, near_ref, table_ref):
    my_x, my_z, my_y, my_c = position()
    cx, cy, cz = corners_ref[0:1, :], corners_ref[1:2, :], corners_ref[2:3, :]
    gs = slots_ref[0:1, :]
    grids = gs.shape[1]
    low, high = near_ref[0:1, :], near_ref[1:2, :]
    gx, gy, gz = cx >> 5, cy >> 5, cz >> 8
    box = (cx >> 3) & 3
    home = gx * LINE_Y + gy
    brick_key = (home * 2 + gz) * SLOTS + box
    word = (1 + box * 2 + home * 8 + (low + 1) * 1024).astype(f32)
    sub = lax.broadcasted_iota(i32, (32, 1), 0)
    eye = (lax.broadcasted_iota(i32, (32, 128), 0) == lax.broadcasted_iota(i32, (32, 128), 1)).astype(f32)

    def to_row(column):
        return jnp.sum(eye * column, axis=0, keepdims=True)

    def pick(match, values):
        return jnp.sum(jnp.where(match, values, 0.0), axis=1, keepdims=True)

    def device_of(j):
        return ((my_x * LINE_Z + j) * LINE_Y + my_y) * 2 + my_c

    keys = device_of(sub >> 2) * SLOTS + (sub & 3)
    held = keys == gs
    words = pick(held, word)
    high_grid = pick(held, (high + 1).astype(f32)).astype(i32)
    low_grid = words.astype(i32) >> 10
    grid_ids = lax.broadcasted_iota(i32, (1, grids), 1) + 1
    slot_plus = (gs + 1).astype(f32)
    low_slot = pick(low_grid == grid_ids, slot_plus).astype(i32)
    high_slot = pick(high_grid == grid_ids, slot_plus).astype(i32)
    devices = gs >> 2
    bit = (jnp.int32(1) << box).astype(f32)

    def boxes_on(device):
        return pick(device == devices, bit).astype(i32)

    mine = device_of(sub >> 2)
    my_mask = boxes_on(mine)
    my_box = (words.astype(i32) >> 1) & 3
    lanes = lax.broadcasted_iota(i32, (32, 128), 1)
    same_j = (sub >> 2) == (lanes >> 2)
    route_row = jnp.zeros((1, 128), f32)
    sends_row = jnp.zeros((1, 128), f32)
    near_words = []
    for side, slot in enumerate((low_slot, high_slot)):
        device = (slot - 1) >> 2
        near_mask = boxes_on(device)
        near_box = (my_box + (3, 1)[side]) & 3
        outer = (slot > 0) & (device != mine)

        def before(mask, at):
            return ((mask & ((jnp.int32(1) << at) - 1)) != 0).astype(i32)

        def after(mask, at):
            return ((mask >> (at + 1)) != 0).astype(i32)

        if side == 0:
            here, there = before(my_mask, my_box), 2 + after(near_mask, near_box)
        else:
            here, there = 2 + after(my_mask, my_box), before(near_mask, near_box)
        target = jnp.where(same_j & ((lanes & 3) == here) & outer, 1.0, 0.0)
        plane = (device >> 6) * LINE_Y + ((device >> 1) & 3)
        code = (plane * 4 + there + near_box * 64 + 1).astype(f32)
        route_row = route_row + jnp.sum(target * code, axis=0, keepdims=True)
        sends_row = sends_row + jnp.sum(target * ((sub & 3) + 1).astype(f32), axis=0, keepdims=True)
        word = jnp.where(outer, 2 + here * 4 + ((device >> 3) & 7) * 16, 1 + ((slot - 1) & 3) * 4)
        near_words.append(jnp.where(slot > 0, word, 0).astype(f32))
    owner = pick(keys == brick_key, slot_plus)
    sub8 = lax.broadcasted_iota(i32, (8, 1), 0)
    on_device = device_of(sub8) == (gs >> 2)
    in_y = cy & 31
    side_y = jnp.where(in_y == 0, 128, jnp.where(in_y == 24, 256, 0))
    homes = jnp.max(jnp.where(on_device, (home + 1 + side_y).astype(f32), 0.0), axis=1, keepdims=True)
    homes = jnp.concatenate([homes, jnp.zeros((24, 1), f32)], axis=0)
    sub24 = lax.broadcasted_iota(i32, (24, 1), 0)
    target_x = my_x * LINE_Z + my_z + jnp.where(sub24 >= 12, 1, jnp.where(sub24 >= 6, 0, -1))
    target_x = jnp.where(sub24 >= 18, -1, target_x)
    in_x = sub24 - jnp.where(sub24 >= 12, 12, jnp.where(sub24 >= 6, 6, 0))
    target_y = my_y + (in_x >> 1) - 1
    target_z = jnp.where((in_x & 1) == 0, my_c, 1 - my_c)
    near_brick = (target_x == gx) & (target_y == gy) & (target_z == gz)
    place = ((cy & 31) * 256 + (cz & 255)).astype(f32)
    anchors = jnp.max(jnp.where(near_brick, place, -1.0), axis=1, keepdims=True)
    anchors = jnp.concatenate([anchors, jnp.zeros((8, 1), f32)], axis=0)
    rows = [to_row(v) for v in (words, homes, *near_words, owner, anchors)] + [route_row, sends_row]
    for r, row in enumerate(rows):
        table_ref[r : r + 1, :] = row.astype(i32)


def pack_kernel(
    corners_ref, slots_ref, near_ref, fine_ref, brick, const,
    table_ref, own_ref, other_ref, planes_ref, window_ref,
    table, table_sem,
):
    make_table(corners_ref, slots_ref, near_ref, table_ref)
    fetch = pltpu.make_async_copy(table_ref, table, table_sem)
    fetch.start()
    own_ref[...] = jnp.zeros_like(own_ref)
    other_ref[...] = jnp.zeros_like(other_ref)
    planes_ref[...] = jnp.zeros_like(planes_ref)
    fetch.wait()
    me = lax.axis_index("gx_1")
    for e in range(4):
        s = jnp.maximum(table[ROW_SENDS, me * 4 + e] - 1, 0)
        for k in range(3):
            tile = fine_ref[pl.ds(pl.multiple_of((k * SLOTS + s) * F + (0 if e < 2 else 8), 8), 8), :]
            row = tile[0:1] if e < 2 else tile[7:8]
            for half in range(2):
                at = e * 8 + half * 3 + k
                planes_ref[at : at + 1, :] = row[:, half * 128 : half * 128 + 128]

    my_c = lax.axis_index("gz")
    lane = lax.broadcasted_iota(i32, (1, 128), 1)
    sub3 = lax.broadcasted_iota(i32, (3, 1), 0)

    def from_second(z_base):
        return z_base + ((lane - z_base) & 127) >= 128

    def window_rows(at, second):
        return jnp.where(second, brick[at(8)], brick[at(0)])

    def to_front(rows, z_base, valid):
        rows = pltpu.roll(rows, (256 - z_base) & 127, 1)
        at = z_base + lane
        return jnp.where((lane < SIDE) & (at >= 0) & (at < 256) & valid, rows, 0.0)

    def shifted(start, count, stride, z_base, valid):
        rows = window_rows(
            lambda tile: (pl.ds(start + tile, count, stride=stride), slice(None)), from_second(z_base)
        )
        return to_front(rows, z_base, valid)

    def tile_row(y):
        return (y >> 3) * 16 + (y & 7)

    def ends_of(u):
        low = 0.75 * u[:, 0:1] + 0.25 * u[:, 1:2]
        high = 0.75 * u[:, 9:10] + 0.25 * u[:, 8:9]
        return low, high

    def beside_rows(dy, z_base):
        total = jnp.zeros((32, 128), f32)
        y, face = (31, 0) if dy == 1 else (0, 30)
        for k in range(3):
            u = shifted(k * 2048 + tile_row(y), 32, 64, z_base, True)
            total = total + (pltpu.roll(u, face + 10 * k, 1) if face + k else u)
        return total

    def diagonal_row(x, dy, z_base):
        y, face = (31, 0) if dy == 1 else (0, 30)
        face += 0 if x else 60
        u = shifted(x * 64 + tile_row(y), 3, 2048, z_base, True)
        row = jnp.where(sub3 == 0, u, jnp.where(sub3 == 1, pltpu.roll(u, 10, 1), pltpu.roll(u, 20, 1)))
        row = jnp.sum(row, axis=0, keepdims=True)
        return pltpu.roll(row, face, 1) if face else row

    def all_rows(y0, z_base):
        offset = (lax.broadcasted_iota(i32, (128, 1), 0) - z_base) & 127
        offset = jnp.where((offset + z_base >= 0) & (offset + z_base < 256), offset, 500).astype(f32)
        window = jnp.where(offset == const[32:33, :], const[34:35, :], 0.0)
        window = window + jnp.where(offset == const[33:34, :], const[35:36, :], 0.0)
        start = (y0 >> 3) * 16
        low_y, high_y = jnp.maximum(y0 - 1, 0), jnp.minimum(y0 + B, 31)
        tiles = from_second(z_base)
        parts = []
        for n in range(96):
            first = n * 64 + start
            parts.append(
                window_rows(lambda tile, first=first: (pl.ds(pl.multiple_of(first + tile, 8), 8), slice(None)), tiles)
            )
        for y in (low_y, high_y):
            first = tile_row(y)
            parts.append(
                window_rows(lambda tile, first=first: (pl.ds(first + tile, 96, stride=64), slice(None)), tiles)
            )
        cells = dot_right(jnp.concatenate(parts, axis=0), window.astype(jnp.bfloat16))
        inner = cells[:768].reshape(3, 32, B, 128)
        total = inner[0] * const[0:8, :][None]
        total = total + inner[1] * const[8:16, :][None]
        total = total + inner[2] * const[16:24, :][None]
        rows = jnp.sum(total, axis=1)
        for k in range(3):
            low = jnp.where(y0 > 0, const[24 + k : 25 + k, :], 0.0)
            high = jnp.where(y0 < 24, const[27 + k : 28 + k, :], 0.0)
            rows = rows + low * cells[768 + 32 * k : 800 + 32 * k] + high * cells[864 + 32 * k : 896 + 32 * k]
        flats = []
        for x in (0, 31):
            for k in range(3):
                tile = jnp.where(lane < SIDE, cells[(k * 32 + x) * B : (k * 32 + x) * B + B], 0.0)
                flat = jnp.sum(pltpu.roll(tile, SIDE, 1, stride=SIDE, stride_axis=0), axis=0, keepdims=True)
                low = cells[768 + 32 * k + x : 769 + 32 * k + x]
                high = cells[864 + 32 * k + x : 865 + 32 * k + x]
                flat = flat + jnp.where((lane < SIDE) & (y0 > 0), low, 0.0)
                flat = flat + pltpu.roll(jnp.where((lane < SIDE) & (y0 < 24), high, 0.0), 90, 1)
                flats.append(flat)
        return rows, flats

    def edge_rows(x, y0, z_base):
        start = (y0 >> 3) * 16
        tiles = from_second(z_base)
        rows = []
        for k in range(3):
            first = (k * 32 + x) * 64 + start
            rows.append(
                window_rows(lambda tile, first=first: (pl.ds(pl.multiple_of(first + tile, 8), 8), slice(None)), tiles)
            )
        u = to_front(jnp.concatenate(rows, axis=0), z_base, True)
        low, high = ends_of(u)
        flats, faces = [], []
        for k in range(3):
            tile = u[k * B : k * B + B]
            flats.append(jnp.sum(pltpu.roll(tile, SIDE, 1, stride=SIDE, stride_axis=0), axis=0, keepdims=True))
            tile = pltpu.roll(tile, 10 * k, 1) if k else tile
            faces.append(tile + pltpu.roll(tile, 30, 1))
        spread = jnp.where(lane < 60, jnp.concatenate(faces, axis=0), jnp.where(lane < 90, low, high))
        total = jnp.sum(spread * const[0:24, :], axis=0, keepdims=True)
        flat = jnp.where(sub3 == 0, flats[0], jnp.where(sub3 == 1, flats[1], flats[2]))
        row = jnp.zeros((3, 128), f32)
        for t, y, valid in ((0, y0 - 1, y0 > 0), (SIDE - 1, y0 + B, y0 < 24)):
            u = shifted(x * 64 + tile_row(jnp.clip(y, 0, 31)), 3, 2048, z_base, valid)
            flat = flat + (pltpu.roll(u, 10 * t, 1) if t else u)
            low, high = ends_of(u)
            row = jnp.where(lane == 60 + 10 * sub3 + t, low, row)
            row = jnp.where(lane == 90 + 10 * sub3 + t, high, row)
            face = 30 if t else 0
            spread = jnp.where(
                sub3 == 0,
                pltpu.roll(u, face, 1) if face else u,
                jnp.where(sub3 == 1, pltpu.roll(u, face + 10, 1), pltpu.roll(u, face + 20, 1)),
            )
            row = row + 0.75 * spread
        return flat, total + jnp.sum(row, axis=0, keepdims=True)

    for dz in range(2):
        out = other_ref if dz else own_ref
        z_shift = 256 * (1 - 2 * my_c) if dz else 0
        for dy in (-1, 0, 1):
            for dx in (0, -1, 1):
                place = table[ROW_ANCHOR, (dx + 1) * 6 + (dy + 1) * 2 + dz]
                y0, z0 = place >> 8, place & 255
                z_base = z0 - 1 + z_shift
                near = place >= 0
                if dy == 1:
                    near &= y0 == 0
                if dy == -1:
                    near &= y0 == 24
                if dz:
                    near &= z0 == jnp.where(my_c == 0, 0, 248)

                @pl.when(near)
                def _(out=out, dz=dz, dx=dx, dy=dy, y0=y0, z0=z0, z_base=z_base):
                    if dy and dx:
                        out[38:39, :] += diagonal_row(0 if dx == -1 else 31, dy, z_base)
                    elif dy:
                        out[48:80, :] += beside_rows(dy, z_base)
                    elif dx:
                        x, at = (0, 44) if dx == -1 else (31, 40)
                        flat, row = edge_rows(x, y0, z_base)
                        out[at : at + 3, :] = 0.75 * flat
                        out[at + 3 : at + 4, :] = row
                    else:
                        rows, flats = all_rows(y0, z_base)
                        out[0:32, :] = rows
                        for i, flat in enumerate(flats):
                            out[32 + i : 33 + i, :] = 0.25 * flat
                        if dz == 0:
                            start = (y0 >> 3) * 16 + (z0 >> 7) * 8
                            for n in range(96):
                                tile = brick[pl.ds(pl.multiple_of(n * 64 + start, 8), 8), :]
                                window_ref[n * 8 : n * 8 + 8, :] = tile


def split_slot(slot):
    device = slot >> 2
    return device >> 6, (device >> 3) & 7, (device >> 1) & 3, slot & 3


def join_kernel(own, other, planes, out):
    total = own[...] + other[...]
    sub = lax.broadcasted_iota(i32, (8, 1), 0)
    tiles = []
    for e in range(4):
        pair = jnp.where(sub == 6, total[40 + 2 * e : 41 + 2 * e], total[41 + 2 * e : 42 + 2 * e])
        tiles.append(jnp.where(sub < 6, planes[e * 8 : e * 8 + 8, :], pair))
    two = total[48:64] + pltpu.roll(total[64:80], 64, 1)
    payload = jnp.concatenate([total[:40]] + tiles + [two], axis=0)
    for j in range(PLANE):
        out[j] = payload


def route_kernel(table, held, beside_ref, out, rows, spread):
    sub = lax.broadcasted_iota(i32, (8, 1), 0)
    lane = lax.broadcasted_iota(i32, (1, 128), 1)

    def line_of(gx):
        return (jnp.clip(gx, 0, 31) >> 3) * LINE_Y

    def read(j):
        code = jnp.maximum(table[ROW_HOME, j] - 1, 0)
        home, edge = code & 127, code >> 7
        gx, gy = home >> 2, home & 3
        near_y = jnp.where(edge == 1, gy - 1, gy + 1)
        used = (edge > 0) & (near_y >= 0) & (near_y < LINE_Y)
        start = jnp.where(edge == 2, 30, 0)
        keep = (lane >= start) & (lane < start + 30) & used
        return gx, gy, jnp.clip(near_y, 0, LINE_Y - 1), edge, keep

    for j in range(LINE_Z):
        gx, _, near_y, _, keep = read(j)
        both = held[line_of(gx) + near_y, PAIRED:FIRST]
        rows[j * 32 : j * 32 + 16, :] = jnp.where(keep, both, 0.0)
        rows[j * 32 + 16 : j * 32 + 32, :] = jnp.where(keep, pltpu.roll(both, 64, 1), 0.0)
        for side in range(2):
            row = held[line_of(gx + (1 if side else -1)) + near_y, 32:40][6:7]
            at = LINE_Z * 32 + j * 2 + side
            rows[at : at + 1, :] = jnp.where(keep, pltpu.roll(row, 68, 1) if side else row, 0.0)
    spread[...] = dot_right(rows[...], beside_ref[...])

    for j in range(LINE_Z):
        gx, gy, _, edge, _ = read(j)
        home_at = line_of(gx) + gy
        shift = jnp.where(edge == 2, 60, 0)
        kept = (lane >= jnp.where(edge == 2, 90, 0)) & (lane < jnp.where(edge == 2, 100, SIDE))

        def flats(row):
            return [jnp.where(kept, pltpu.roll(row, (shift + 128 - 10 * k) & 127, 1), 0.0) for k in range(3)]

        out[j, 0:32] = held[home_at, 0:32] + spread[j * 32 : j * 32 + 32, :]
        ends = held[home_at, 32:40]
        for side in range(2):
            near = rows[j * 32 + 31 * side : j * 32 + 31 * side + 1, :]
            at = LINE_Z * 32 + j * 2 + side
            source = line_of(gx + (1 if side else -1)) + gy
            pair = [held[source, 40 + (side * 2 + half) * 8 : 48 + (side * 2 + half) * 8] for half in range(2)]
            ghosts = [ends[3 * side + k : 3 * side + k + 1] + 0.25 * row for k, row in enumerate(flats(near))]
            pieces = (pair[0][6:7], pair[0][7:8], pair[1][6:7])
            ghosts += [piece + 0.75 * row for piece, row in zip(pieces, flats(rows[at : at + 1, :]))]
            ghosts.append(pair[1][7:8] + spread[at : at + 1, :])
            tile = jnp.zeros((8, 128), f32)
            for i, row in enumerate(ghosts):
                tile = jnp.where(sub == i, row, tile)
            for half in range(2):
                code = table[ROW_ROUTE, j * 4 + side * 2 + half] - 1
                used = code >= 0
                code = jnp.maximum(code, 0)
                plane = held[(code >> 2) & 15, pl.ds(pl.multiple_of(40 + (code & 3) * 8, 8), 8)]
                if half == 0:
                    out[j, 32 + side * 8 : 40 + side * 8] = jnp.where((sub < 6) & used, plane, tile)
                elif side == 1:
                    out[j, 48:56] = plane
                else:
                    between = pl.ds(pl.multiple_of((code >> 6) * 8, 8), 8)
                    inner = (sub >= 1) & (sub <= 6) & used
                    out[j, between] = jnp.where(inner, pltpu.roll(plane, 1, 0), out[j, between])


def update_kernel(
    table, rcv, fine_ref, visc_ref, along_x, faces, ends, pool,
    fine_out, means_out,
    sums, planes, advanced, pooled, kept, sem,
):
    me = lax.axis_index("gx_1")
    gx = (jnp.maximum(table[ROW_HOME, me] - 1, 0) & 127) >> 2
    at_home, at_low, at_high = gx & 7, (gx + 7) & 7, (gx + 1) & 7
    sub8 = lax.broadcasted_iota(i32, (8, 1), 0)

    low = jnp.where(gx > 0, rcv[at_low, 32:40], 0.0)
    high = jnp.where(gx < 31, rcv[at_high, 40:48], 0.0)
    beyond = jnp.where(sub8 == 0, low[6:7], jnp.where(sub8 == 1, high[6:7], 0.0))
    body = jnp.concatenate([rcv[at_home, 0:32], beyond], axis=0)
    sums[...] = dot_right(dot_left(along_x[...], body), faces[...])
    own = (rcv[at_home, 32:40], rcv[at_home, 40:48])
    flat = jnp.zeros((8, 128), f32)
    for side, other in enumerate((low, high)):
        for k in range(3):
            flat = jnp.where(sub8 == 3 * side + k, own[side][k : k + 1] + other[3 + k : 4 + k], flat)
    planes[...] = dot_right(flat, ends[...])
    lane = lax.broadcasted_iota(i32, (1, F * F), 1)
    sub = lax.broadcasted_iota(i32, (F, 1), 0)
    lane_z = lane & (F - 1)
    for s in range(SLOTS):
        word = table[ROW_SLOT, me * 4 + s]
        active = (word & 1) == 1
        box_start = pl.multiple_of(((word >> 1) & 3) * F, F)
        low_word = table[ROW_LOW, me * 4 + s]
        high_word = table[ROW_HIGH, me * 4 + s]
        second = (low_word & 7) == 6
        low_at = jnp.where(second, (((word >> 1) & 3) + 3) & 3, 4) * 8
        low_tile = rcv[low_word >> 4, pl.ds(pl.multiple_of(low_at, 8), 8)]
        low_tile = jnp.where(second, pltpu.roll(low_tile, 7, 0), low_tile)
        high_at = jnp.where((high_word & 15) == 14, 48, 40)
        high_tile = rcv[high_word >> 4, pl.ds(pl.multiple_of(high_at, 8), 8)]
        visc = step_rate * visc_ref[s * F : s * F + F, :]
        for k in range(3):
            row = (k * SLOTS + s) * F
            cells = fine_ref[row : row + F, :]
            lower = jnp.concatenate([low_tile[k : k + 1], low_tile[3 + k : 4 + k]], axis=1)
            upper = jnp.concatenate([high_tile[k : k + 1], high_tile[3 + k : 4 + k]], axis=1)
            low_row = pl.multiple_of((k * SLOTS + ((low_word >> 2) & 3)) * F + 8, 8)
            high_row = pl.multiple_of((k * SLOTS + ((high_word >> 2) & 3)) * F, 8)
            lower = jnp.where((low_word & 3) == 1, fine_ref[pl.ds(low_row, 8), :][7:8], lower)
            upper = jnp.where((high_word & 3) == 1, fine_ref[pl.ds(high_row, 8), :][0:1], upper)
            lower = jnp.where(low_word > 0, lower, planes[k : k + 1, :])
            upper = jnp.where(high_word > 0, upper, planes[3 + k : 4 + k, :])
            total = sums[pl.ds(box_start, F), k * 256 : k * 256 + 256] - 6.0 * cells
            total = total + jnp.where(sub == 0, lower, pltpu.roll(cells, 1, 0))
            total = total + jnp.where(sub == F - 1, upper, pltpu.roll(cells, F - 1, 0))
            total = total + jnp.where(lane < F, 0.0, pltpu.roll(cells, F, 1))
            total = total + jnp.where(lane >= F * F - F, 0.0, pltpu.roll(cells, F * F - F, 1))
            total = total + jnp.where(lane_z == 0, 0.0, pltpu.roll(cells, 1, 1))
            total = total + jnp.where(lane_z == F - 1, 0.0, pltpu.roll(cells, F * F - 1, 1))
            result = cells + visc * total
            kept[row : row + F, :] = jnp.where(active, result, 0.0)
            at = s * 48 + k * F
            advanced[at : at + F, :] = result
    store = pltpu.make_async_copy(kept, fine_out, sem)
    store.start()
    for p in range(2):
        at = p * 96
        pooled[p * 48 : p * 48 + 48, :] = dot_right(advanced[at : at + 48, :], pool[0]) + dot_right(
            advanced[at + 48 : at + 96, :], pool[1]
        )
    means = pooled[pl.ds(0, 48, stride=2), :] + pooled[pl.ds(1, 48, stride=2), :]
    for j in range(PLANE):
        means_out[j] = means
    store.wait()


def return_kernel(table, held, out):
    first = lax.broadcasted_iota(i32, (1, 128), 1) < 64
    for j in range(LINE_Z):
        for p in range(2):
            picks = []
            for h in range(2):
                x, _, y, local = split_slot(jnp.maximum(table[ROW_OWNER, j * 4 + 2 * p + h] - 1, 0))
                start = pl.multiple_of((local >> 1) * 24, 8)
                rows = held[x * LINE_Y + y, pl.ds(start, 24)]
                picks.append(jnp.where((local & 1) == h, rows, pltpu.roll(rows, 64, 1)))
            out[j, p * 24 : p * 24 + 24] = jnp.where(first, picks[0], picks[1])


def place_kernel(table, rcv, window, coarse_ref, coarse_out, spread, sem):
    me = lax.axis_index("gx_1")
    place = table[ROW_ANCHOR, SELF_TARGET]

    @pl.when(place >= 0)
    def _():
        y0 = pl.multiple_of(place >> 8, 8)
        z0 = place & 255
        z_tile = pl.multiple_of((z0 >> 7) * 128, 128)
        z_in = z0 & 127
        lane = lax.broadcasted_iota(i32, (1, 128), 1)
        owners = [split_slot(jnp.maximum(table[ROW_OWNER, me * 4 + i] - 1, 0))[1] for i in range(SLOTS)]
        stores = []
        for k in range(3):
            for i in range(SLOTS):
                start = ((i // 2) * 3 + k) * 8
                values = rcv[owners[i], start : start + 8]
                for b in range(B):
                    shift = (z_in + 256 - (b * B + 64 * (i % 2))) & 127
                    spread[pl.ds((k * 32 + i * B) * B + b, B, stride=B), :] = pltpu.roll(values, shift, 1)
            rows = pl.ds(k * 256, 256)
            spread[rows, :] = jnp.where((lane >= z_in) & (lane < z_in + B), spread[rows, :], window[rows, :])
            part = pl.ds(k * 32, 32)
            stores.append(
                pltpu.make_async_copy(
                    spread.reshape(96, 8, 128).at[part],
                    coarse_out.at[part, pl.ds(y0, 8), pl.ds(z_tile, 128)],
                    sem.at[k],
                )
            )
            stores[-1].start()
        for store in stores:
            store.wait()


def vmem():
    return pl.BlockSpec(memory_space=pltpu.VMEM)


def smem():
    return pl.BlockSpec(memory_space=pltpu.SMEM)


def anywhere():
    return pl.BlockSpec(memory_space=pl.ANY)


def shape(*dims, dtype=f32):
    return jax.ShapeDtypeStruct(dims, dtype)


def on_device(coarse_field, fine_field, viscosity, corners, grid_slot, neighbors):
    fine = fine_field.reshape(3 * SLOTS * F, F * F)
    tiles = coarse_field.reshape(3, 32, 4, 8, 2, 128).transpose(0, 1, 2, 4, 3, 5).reshape(6144, 128)
    pack_const, beside = map(jnp.asarray, pack_constants())
    beside = beside.astype(jnp.bfloat16)
    table, own, other, planes, window = pl.pallas_call(
        pack_kernel,
        out_shape=(
            shape(8, 128, dtype=i32),
            shape(PACKED, 128),
            shape(PACKED, 128),
            shape(32, 128),
            shape(768, 128),
        ),
        in_specs=[vmem()] * 6,
        out_specs=(vmem(),) * 5,
        scratch_shapes=[pltpu.SMEM((8, 128), i32), pltpu.SemaphoreType.DMA(())],
        name="pack", compiler_params=pltpu.CompilerParams(vmem_limit_bytes=24 << 20),
    )(corners.T, grid_slot[None, :], neighbors.T, fine, tiles, pack_const)
    other = lax.ppermute(other, "gz", [(0, 1), (1, 0)])
    payload = pl.pallas_call(
        join_kernel,
        out_shape=shape(PLANE, FIRST, 128),
        in_specs=[vmem()] * 3,
        out_specs=vmem(),
        name="join",
        compiler_params=pltpu.CompilerParams(vmem_limit_bytes=8 << 20),
    )(own, other, planes)
    held = lax.all_to_all(payload, ("gx_0", "gy"), 0, 0)
    routed = pl.pallas_call(
        route_kernel,
        out_shape=shape(LINE_Z, SEND, 128),
        in_specs=[smem(), vmem(), vmem()],
        out_specs=vmem(),
        scratch_shapes=[pltpu.VMEM((LINE_Z * 34, 128), f32)] * 2,
        name="route",
        compiler_params=pltpu.CompilerParams(vmem_limit_bytes=8 << 20),
    )(table, held, beside)
    received = lax.all_to_all(routed, "gx_1", 0, 0)
    fine_out, means = pl.pallas_call(
        update_kernel,
        out_shape=(shape(3 * SLOTS * F, F * F), shape(PLANE, 48, 128)),
        in_specs=[smem()] + [vmem()] * 7,
        out_specs=(anywhere(), vmem()),
        scratch_shapes=[
            pltpu.VMEM((64, 768), f32),
            pltpu.VMEM((8, 256), f32),
            pltpu.VMEM((192, 256), f32),
            pltpu.VMEM((96, 128), f32),
            pltpu.VMEM((192, 256), f32),
            pltpu.SemaphoreType.DMA(()),
        ],
        name="update", compiler_params=pltpu.CompilerParams(vmem_limit_bytes=16 << 20),
    )(table, received, fine, viscosity.reshape(SLOTS * F, F * F), *(jnp.asarray(m, jnp.bfloat16) for m in constant_matrices()))
    held_means = lax.all_to_all(means, ("gx_0", "gy"), 0, 0)
    back = pl.pallas_call(
        return_kernel,
        out_shape=shape(LINE_Z, 48, 128),
        in_specs=[smem(), vmem()],
        out_specs=vmem(),
        name="send_back", compiler_params=pltpu.CompilerParams(vmem_limit_bytes=8 << 20),
    )(table, held_means)
    returned = lax.all_to_all(back, "gx_1", 0, 0)
    coarse_out = pl.pallas_call(
        place_kernel,
        out_shape=shape(96, 32, 256),
        in_specs=[smem(), vmem(), vmem(), anywhere()],
        out_specs=anywhere(),
        input_output_aliases={3: 0},
        scratch_shapes=[pltpu.VMEM((768, 128), f32), pltpu.SemaphoreType.DMA((3,))],
        name="place", compiler_params=pltpu.CompilerParams(vmem_limit_bytes=8 << 20),
    )(table, returned, window, coarse_field.reshape(96, 32, 256))
    return fine_out.reshape(fine_field.shape), coarse_out.reshape(coarse_field.shape)


def solution(mesh):
    split = Mesh(
        mesh.devices.reshape(LINE_X, LINE_Z, mesh.shape["gy"], mesh.shape["gz"]), ("gx_0", "gx_1", "gy", "gz")
    )
    in_specs = (
        P(None, GX, "gy", "gz"),
        P(None, GX_GY_GZ, None, None),
        P(GX_GY_GZ, None, None),
        P(),
        P(),
        P(),
    )
    out_specs = (P(None, GX_GY_GZ, None, None), P(None, GX, "gy", "gz"))
    return jax.shard_map(
        on_device, mesh=split, in_specs=in_specs, out_specs=out_specs, check_vma=False
    )
```

```python
import jax
import jax.numpy as jnp
import numpy as np
from jax import lax
from jax.experimental import pallas as pl
from jax.experimental.pallas import tpu as pltpu
from jax.sharding import Mesh
from jax.sharding import PartitionSpec as P

B = 8
F = 16
SLOTS = 4
SIDE = B + 2
LINE_X = 4
LINE_Z = 8
LINE_Y = 4
PLANE = LINE_X * LINE_Y
PACKED = 80
PAIRED = 72
FIRST = 88
SEND = 56
step_rate = 0.15
f32 = jnp.float32
i32 = jnp.int32
GX = ("gx_0", "gx_1")
GX_GY_GZ = ("gx_0", "gx_1", "gy", "gz")

ROW_SLOT, ROW_HOME, ROW_LOW, ROW_HIGH, ROW_OWNER, ROW_ANCHOR, ROW_ROUTE, ROW_SENDS = range(8)
SELF_TARGET = 8


def tangent_matrix():
    fine = np.arange(F)
    coarse = np.arange(SIDE)
    center = fine // 2 + 1
    other = np.where(fine % 2 == 0, center - 1, center + 1)
    return 0.75 * (coarse[None] == center[:, None]) + 0.25 * (coarse[None] == other[:, None])


def constant_matrices():
    tangent = tangent_matrix()
    along_x = np.zeros((64, 40))
    for fine in range(64):
        center = fine // 2
        other = center - 1 if fine % 2 == 0 else center + 1
        along_x[fine, center] += 0.75
        along_x[fine, 32 if other < 0 else 33 if other > 31 else other] += 0.25
    faces = np.zeros((128, 3, F, F))
    for k in range(3):
        for c in range(SIDE):
            faces[k * 10 + c, k, 0, :] += tangent[:, c]
            faces[30 + k * 10 + c, k, F - 1, :] += tangent[:, c]
            faces[60 + k * 10 + c, k, :, 0] += tangent[:, c]
            faces[90 + k * 10 + c, k, :, F - 1] += tangent[:, c]
    ends = np.zeros((128, F * F))
    ends[: SIDE * SIDE] = np.einsum("sa,tb->abst", tangent, tangent).reshape(SIDE * SIDE, F * F)
    pool = np.zeros((2, F, F, 128))
    for y in range(F):
        for z in range(F):
            for half in range(2):
                pool[half, y, z, half * 64 + (y // 2) * B + z // 2] = 0.125
    return (
        along_x.astype(np.float32),
        faces.reshape(128, 3 * F * F).astype(np.float32),
        ends.astype(np.float32),
        pool.reshape(2, F * F, 128).astype(np.float32),
    )


def pack_constants():
    out = np.zeros((40, 128))
    for k in range(3):
        for y in range(B):
            out[k * B + y, 60 + 10 * k + 1 + y] = 1.0
            out[k * B + y, 90 + 10 * k + 1 + y] = 1.0
        out[k * B, 10 * k : 10 * k + 10] = 0.25
        out[k * B + B - 1, 30 + 10 * k : 40 + 10 * k] = 0.25
        out[24 + k, 10 * k : 10 * k + 10] = 0.75
        out[24 + k, [60 + 10 * k, 90 + 10 * k]] = 1.0
        out[27 + k, 30 + 10 * k : 40 + 10 * k] = 0.75
        out[27 + k, [69 + 10 * k, 99 + 10 * k]] = 1.0
    beside = np.zeros((128, 128))
    for face in range(2):
        for k in range(3):
            for c in range(SIDE):
                at = face * 30 + k * 10 + c
                edge = face * 9 + 10 * k
                beside[at, at] = 0.75
                beside[at, 60 + edge] = {0: 0.75, 1: 0.25}.get(c, 0.0)
                beside[at, 90 + edge] = {9: 0.75, 8: 0.25}.get(c, 0.0)
    lanes = np.arange(128)
    out[32] = np.where(lanes < 60, lanes % 10, np.where(lanes < 90, 0, np.where(lanes < 120, 9, -999)))
    out[33] = np.where(lanes < 60, -999, np.where(lanes < 90, 1, np.where(lanes < 120, 8, -999)))
    out[34] = np.where(lanes < 60, 1.0, 0.75)
    out[35] = 0.25
    return out.astype(np.float32), beside.astype(np.float32)


def thirds(values):
    high = values.astype(jnp.bfloat16)
    rest = values - high.astype(f32)
    middle = rest.astype(jnp.bfloat16)
    return high, middle, (rest - middle.astype(f32)).astype(jnp.bfloat16)


def dot_right(values, weights):
    parts = [jnp.dot(part, weights, preferred_element_type=f32) for part in thirds(values)]
    return parts[0] + (parts[1] + parts[2])


def dot_left(weights, values):
    parts = [jnp.dot(weights, part, preferred_element_type=f32) for part in thirds(values)]
    return parts[0] + (parts[1] + parts[2])


def position():
    return tuple(lax.axis_index(name) for name in GX_GY_GZ)


def make_table(corners_ref, slots_ref, near_ref, table_ref):
    my_x, my_z, my_y, my_c = position()
    cx, cy, cz = corners_ref[0:1, :], corners_ref[1:2, :], corners_ref[2:3, :]
    gs = slots_ref[0:1, :]
    grids = gs.shape[1]
    low, high = near_ref[0:1, :], near_ref[1:2, :]
    gx, gy, gz = cx >> 5, cy >> 5, cz >> 8
    box = (cx >> 3) & 3
    home = gx * LINE_Y + gy
    brick_key = (home * 2 + gz) * SLOTS + box
    word = (1 + box * 2 + home * 8 + (low + 1) * 1024).astype(f32)
    sub = lax.broadcasted_iota(i32, (32, 1), 0)
    eye = (lax.broadcasted_iota(i32, (32, 128), 0) == lax.broadcasted_iota(i32, (32, 128), 1)).astype(f32)

    def to_row(column):
        return jnp.sum(eye * column, axis=0, keepdims=True)

    def pick(match, values):
        return jnp.sum(jnp.where(match, values, 0.0), axis=1, keepdims=True)

    def device_of(j):
        return ((my_x * LINE_Z + j) * LINE_Y + my_y) * 2 + my_c

    keys = device_of(sub >> 2) * SLOTS + (sub & 3)
    held = keys == gs
    words = pick(held, word)
    high_grid = pick(held, (high + 1).astype(f32)).astype(i32)
    low_grid = words.astype(i32) >> 10
    grid_ids = lax.broadcasted_iota(i32, (1, grids), 1) + 1
    slot_plus = (gs + 1).astype(f32)
    low_slot = pick(low_grid == grid_ids, slot_plus).astype(i32)
    high_slot = pick(high_grid == grid_ids, slot_plus).astype(i32)
    devices = gs >> 2
    bit = (jnp.int32(1) << box).astype(f32)

    def boxes_on(device):
        return pick(device == devices, bit).astype(i32)

    mine = device_of(sub >> 2)
    my_mask = boxes_on(mine)
    my_box = (words.astype(i32) >> 1) & 3
    lanes = lax.broadcasted_iota(i32, (32, 128), 1)
    same_j = (sub >> 2) == (lanes >> 2)
    route_row = jnp.zeros((1, 128), f32)
    sends_row = jnp.zeros((1, 128), f32)
    near_words = []
    for side, slot in enumerate((low_slot, high_slot)):
        device = (slot - 1) >> 2
        near_mask = boxes_on(device)
        near_box = (my_box + (3, 1)[side]) & 3
        outer = (slot > 0) & (device != mine)

        def before(mask, at):
            return ((mask & ((jnp.int32(1) << at) - 1)) != 0).astype(i32)

        def after(mask, at):
            return ((mask >> (at + 1)) != 0).astype(i32)

        if side == 0:
            here, there = before(my_mask, my_box), 2 + after(near_mask, near_box)
        else:
            here, there = 2 + after(my_mask, my_box), before(near_mask, near_box)
        target = jnp.where(same_j & ((lanes & 3) == here) & outer, 1.0, 0.0)
        plane = (device >> 6) * LINE_Y + ((device >> 1) & 3)
        code = (plane * 4 + there + near_box * 64 + 1).astype(f32)
        route_row = route_row + jnp.sum(target * code, axis=0, keepdims=True)
        sends_row = sends_row + jnp.sum(target * ((sub & 3) + 1).astype(f32), axis=0, keepdims=True)
        word = jnp.where(outer, 2 + here * 4 + ((device >> 3) & 7) * 16, 1 + ((slot - 1) & 3) * 4)
        near_words.append(jnp.where(slot > 0, word, 0).astype(f32))
    owner = pick(keys == brick_key, slot_plus)
    sub8 = lax.broadcasted_iota(i32, (8, 1), 0)
    on_device = device_of(sub8) == (gs >> 2)
    in_y = cy & 31
    side_y = jnp.where(in_y == 0, 128, jnp.where(in_y == 24, 256, 0))
    homes = jnp.max(jnp.where(on_device, (home + 1 + side_y).astype(f32), 0.0), axis=1, keepdims=True)
    homes = jnp.concatenate([homes, jnp.zeros((24, 1), f32)], axis=0)
    sub24 = lax.broadcasted_iota(i32, (24, 1), 0)
    target_x = my_x * LINE_Z + my_z + jnp.where(sub24 >= 12, 1, jnp.where(sub24 >= 6, 0, -1))
    target_x = jnp.where(sub24 >= 18, -1, target_x)
    in_x = sub24 - jnp.where(sub24 >= 12, 12, jnp.where(sub24 >= 6, 6, 0))
    target_y = my_y + (in_x >> 1) - 1
    target_z = jnp.where((in_x & 1) == 0, my_c, 1 - my_c)
    near_brick = (target_x == gx) & (target_y == gy) & (target_z == gz)
    place = ((cy & 31) * 256 + (cz & 255)).astype(f32)
    anchors = jnp.max(jnp.where(near_brick, place, -1.0), axis=1, keepdims=True)
    anchors = jnp.concatenate([anchors, jnp.zeros((8, 1), f32)], axis=0)
    rows = [to_row(v) for v in (words, homes, *near_words, owner, anchors)] + [route_row, sends_row]
    for r, row in enumerate(rows):
        table_ref[r : r + 1, :] = row.astype(i32)


def pack_kernel(
    corners_ref, slots_ref, near_ref, fine_ref, brick, const, table_ref, other_ref, planes_ref, table, table_sem
):
    make_table(corners_ref, slots_ref, near_ref, table_ref)
    fetch = pltpu.make_async_copy(table_ref, table, table_sem)
    fetch.start()
    planes_ref[...] = jnp.zeros_like(planes_ref)
    fetch.wait()
    me = lax.axis_index("gx_1")
    for e in range(4):
        s = jnp.maximum(table[ROW_SENDS, me * 4 + e] - 1, 0)
        for k in range(3):
            tile = fine_ref[pl.ds(pl.multiple_of((k * SLOTS + s) * F + (0 if e < 2 else 8), 8), 8), :]
            row = tile[0:1] if e < 2 else tile[7:8]
            for half in range(2):
                at = e * 8 + half * 3 + k
                planes_ref[at : at + 1, :] = row[:, half * 128 : half * 128 + 128]

    pack_rows(table, brick, const, other_ref, None, 1)


def pack_own_kernel(table, brick, const, own_ref, window_ref):
    pack_rows(table, brick, const, own_ref, window_ref, 0)


def pack_rows(table, brick, const, out, window_ref, dz):
    out[...] = jnp.zeros_like(out)
    my_c = lax.axis_index("gz")
    lane = lax.broadcasted_iota(i32, (1, 128), 1)
    sub3 = lax.broadcasted_iota(i32, (3, 1), 0)

    def from_second(z_base):
        return z_base + ((lane - z_base) & 127) >= 128

    def window_rows(at, second):
        return jnp.where(second, brick[at(8)], brick[at(0)])

    def to_front(rows, z_base, valid):
        rows = pltpu.roll(rows, (256 - z_base) & 127, 1)
        at = z_base + lane
        return jnp.where((lane < SIDE) & (at >= 0) & (at < 256) & valid, rows, 0.0)

    def shifted(start, count, stride, z_base, valid):
        rows = window_rows(
            lambda tile: (pl.ds(start + tile, count, stride=stride), slice(None)), from_second(z_base)
        )
        return to_front(rows, z_base, valid)

    def tile_row(y):
        return (y >> 3) * 16 + (y & 7)

    def ends_of(u):
        low = 0.75 * u[:, 0:1] + 0.25 * u[:, 1:2]
        high = 0.75 * u[:, 9:10] + 0.25 * u[:, 8:9]
        return low, high

    def beside_rows(dy, z_base):
        total = jnp.zeros((32, 128), f32)
        y, face = (31, 0) if dy == 1 else (0, 30)
        for k in range(3):
            u = shifted(k * 2048 + tile_row(y), 32, 64, z_base, True)
            total = total + (pltpu.roll(u, face + 10 * k, 1) if face + k else u)
        return total

    def diagonal_row(x, dy, z_base):
        y, face = (31, 0) if dy == 1 else (0, 30)
        face += 0 if x else 60
        u = shifted(x * 64 + tile_row(y), 3, 2048, z_base, True)
        row = jnp.where(sub3 == 0, u, jnp.where(sub3 == 1, pltpu.roll(u, 10, 1), pltpu.roll(u, 20, 1)))
        row = jnp.sum(row, axis=0, keepdims=True)
        return pltpu.roll(row, face, 1) if face else row

    def all_rows(y0, z_base):
        offset = (lax.broadcasted_iota(i32, (128, 1), 0) - z_base) & 127
        offset = jnp.where((offset + z_base >= 0) & (offset + z_base < 256), offset, 500).astype(f32)
        window = jnp.where(offset == const[32:33, :], const[34:35, :], 0.0)
        window = window + jnp.where(offset == const[33:34, :], const[35:36, :], 0.0)
        start = (y0 >> 3) * 16
        low_y, high_y = jnp.maximum(y0 - 1, 0), jnp.minimum(y0 + B, 31)
        tiles = from_second(z_base)
        parts = []
        for n in range(96):
            first = n * 64 + start
            parts.append(
                window_rows(lambda tile, first=first: (pl.ds(pl.multiple_of(first + tile, 8), 8), slice(None)), tiles)
            )
        for y in (low_y, high_y):
            first = tile_row(y)
            parts.append(
                window_rows(lambda tile, first=first: (pl.ds(first + tile, 96, stride=64), slice(None)), tiles)
            )
        cells = dot_right(jnp.concatenate(parts, axis=0), window.astype(jnp.bfloat16))
        inner = cells[:768].reshape(3, 32, B, 128)
        total = inner[0] * const[0:8, :][None]
        total = total + inner[1] * const[8:16, :][None]
        total = total + inner[2] * const[16:24, :][None]
        rows = jnp.sum(total, axis=1)
        for k in range(3):
            low = jnp.where(y0 > 0, const[24 + k : 25 + k, :], 0.0)
            high = jnp.where(y0 < 24, const[27 + k : 28 + k, :], 0.0)
            rows = rows + low * cells[768 + 32 * k : 800 + 32 * k] + high * cells[864 + 32 * k : 896 + 32 * k]
        flats = []
        for x in (0, 31):
            for k in range(3):
                tile = jnp.where(lane < SIDE, cells[(k * 32 + x) * B : (k * 32 + x) * B + B], 0.0)
                flat = jnp.sum(pltpu.roll(tile, SIDE, 1, stride=SIDE, stride_axis=0), axis=0, keepdims=True)
                low = cells[768 + 32 * k + x : 769 + 32 * k + x]
                high = cells[864 + 32 * k + x : 865 + 32 * k + x]
                flat = flat + jnp.where((lane < SIDE) & (y0 > 0), low, 0.0)
                flat = flat + pltpu.roll(jnp.where((lane < SIDE) & (y0 < 24), high, 0.0), 90, 1)
                flats.append(flat)
        return rows, flats

    def edge_rows(x, y0, z_base):
        start = (y0 >> 3) * 16
        tiles = from_second(z_base)
        rows = []
        for k in range(3):
            first = (k * 32 + x) * 64 + start
            rows.append(
                window_rows(lambda tile, first=first: (pl.ds(pl.multiple_of(first + tile, 8), 8), slice(None)), tiles)
            )
        u = to_front(jnp.concatenate(rows, axis=0), z_base, True)
        low, high = ends_of(u)
        flats, faces = [], []
        for k in range(3):
            tile = u[k * B : k * B + B]
            flats.append(jnp.sum(pltpu.roll(tile, SIDE, 1, stride=SIDE, stride_axis=0), axis=0, keepdims=True))
            tile = pltpu.roll(tile, 10 * k, 1) if k else tile
            faces.append(tile + pltpu.roll(tile, 30, 1))
        spread = jnp.where(lane < 60, jnp.concatenate(faces, axis=0), jnp.where(lane < 90, low, high))
        total = jnp.sum(spread * const[0:24, :], axis=0, keepdims=True)
        flat = jnp.where(sub3 == 0, flats[0], jnp.where(sub3 == 1, flats[1], flats[2]))
        row = jnp.zeros((3, 128), f32)
        for t, y, valid in ((0, y0 - 1, y0 > 0), (SIDE - 1, y0 + B, y0 < 24)):
            u = shifted(x * 64 + tile_row(jnp.clip(y, 0, 31)), 3, 2048, z_base, valid)
            flat = flat + (pltpu.roll(u, 10 * t, 1) if t else u)
            low, high = ends_of(u)
            row = jnp.where(lane == 60 + 10 * sub3 + t, low, row)
            row = jnp.where(lane == 90 + 10 * sub3 + t, high, row)
            face = 30 if t else 0
            spread = jnp.where(
                sub3 == 0,
                pltpu.roll(u, face, 1) if face else u,
                jnp.where(sub3 == 1, pltpu.roll(u, face + 10, 1), pltpu.roll(u, face + 20, 1)),
            )
            row = row + 0.75 * spread
        return flat, total + jnp.sum(row, axis=0, keepdims=True)

    z_shift = 256 * (1 - 2 * my_c) if dz else 0
    for dy in (-1, 0, 1):
        for dx in (0, -1, 1):
            place = table[ROW_ANCHOR, (dx + 1) * 6 + (dy + 1) * 2 + dz]
            y0, z0 = place >> 8, place & 255
            z_base = z0 - 1 + z_shift
            near = place >= 0
            if dy == 1:
                near &= y0 == 0
            if dy == -1:
                near &= y0 == 24
            if dz:
                near &= z0 == jnp.where(my_c == 0, 0, 248)

            @pl.when(near)
            def _(out=out, dz=dz, dx=dx, dy=dy, y0=y0, z0=z0, z_base=z_base):
                if dy and dx:
                    out[38:39, :] += diagonal_row(0 if dx == -1 else 31, dy, z_base)
                elif dy:
                    out[48:80, :] += beside_rows(dy, z_base)
                elif dx:
                    x, at = (0, 44) if dx == -1 else (31, 40)
                    flat, row = edge_rows(x, y0, z_base)
                    out[at : at + 3, :] = 0.75 * flat
                    out[at + 3 : at + 4, :] = row
                else:
                    rows, flats = all_rows(y0, z_base)
                    out[0:32, :] = rows
                    for i, flat in enumerate(flats):
                        out[32 + i : 33 + i, :] = 0.25 * flat
                    if dz == 0:
                        start = (y0 >> 3) * 16 + (z0 >> 7) * 8
                        for n in range(96):
                            tile = brick[pl.ds(pl.multiple_of(n * 64 + start, 8), 8), :]
                            window_ref[n * 8 : n * 8 + 8, :] = tile


def split_slot(slot):
    device = slot >> 2
    return device >> 6, (device >> 3) & 7, (device >> 1) & 3, slot & 3


def join_kernel(own, other, planes, out):
    total = own[...] + other[...]
    sub = lax.broadcasted_iota(i32, (8, 1), 0)
    tiles = []
    for e in range(4):
        pair = jnp.where(sub == 6, total[40 + 2 * e : 41 + 2 * e], total[41 + 2 * e : 42 + 2 * e])
        tiles.append(jnp.where(sub < 6, planes[e * 8 : e * 8 + 8, :], pair))
    two = total[48:64] + pltpu.roll(total[64:80], 64, 1)
    payload = jnp.concatenate([total[:40]] + tiles + [two], axis=0)
    for j in range(PLANE):
        out[j] = payload


def route_kernel(table, held, beside_ref, out, rows, spread):
    sub = lax.broadcasted_iota(i32, (8, 1), 0)
    lane = lax.broadcasted_iota(i32, (1, 128), 1)

    def line_of(gx):
        return (jnp.clip(gx, 0, 31) >> 3) * LINE_Y

    def read(j):
        code = jnp.maximum(table[ROW_HOME, j] - 1, 0)
        home, edge = code & 127, code >> 7
        gx, gy = home >> 2, home & 3
        near_y = jnp.where(edge == 1, gy - 1, gy + 1)
        used = (edge > 0) & (near_y >= 0) & (near_y < LINE_Y)
        start = jnp.where(edge == 2, 30, 0)
        keep = (lane >= start) & (lane < start + 30) & used
        return gx, gy, jnp.clip(near_y, 0, LINE_Y - 1), edge, keep

    for j in range(LINE_Z):
        gx, _, near_y, _, keep = read(j)
        both = held[line_of(gx) + near_y, PAIRED:FIRST]
        rows[j * 32 : j * 32 + 16, :] = jnp.where(keep, both, 0.0)
        rows[j * 32 + 16 : j * 32 + 32, :] = jnp.where(keep, pltpu.roll(both, 64, 1), 0.0)
        for side in range(2):
            row = held[line_of(gx + (1 if side else -1)) + near_y, 32:40][6:7]
            at = LINE_Z * 32 + j * 2 + side
            rows[at : at + 1, :] = jnp.where(keep, pltpu.roll(row, 68, 1) if side else row, 0.0)
    spread[...] = dot_right(rows[...], beside_ref[...])

    for j in range(LINE_Z):
        gx, gy, _, edge, _ = read(j)
        home_at = line_of(gx) + gy
        shift = jnp.where(edge == 2, 60, 0)
        kept = (lane >= jnp.where(edge == 2, 90, 0)) & (lane < jnp.where(edge == 2, 100, SIDE))

        def flats(row):
            return [jnp.where(kept, pltpu.roll(row, (shift + 128 - 10 * k) & 127, 1), 0.0) for k in range(3)]

        out[j, 0:32] = held[home_at, 0:32] + spread[j * 32 : j * 32 + 32, :]
        ends = held[home_at, 32:40]
        for side in range(2):
            near = rows[j * 32 + 31 * side : j * 32 + 31 * side + 1, :]
            at = LINE_Z * 32 + j * 2 + side
            source = line_of(gx + (1 if side else -1)) + gy
            pair = [held[source, 40 + (side * 2 + half) * 8 : 48 + (side * 2 + half) * 8] for half in range(2)]
            ghosts = [ends[3 * side + k : 3 * side + k + 1] + 0.25 * row for k, row in enumerate(flats(near))]
            pieces = (pair[0][6:7], pair[0][7:8], pair[1][6:7])
            ghosts += [piece + 0.75 * row for piece, row in zip(pieces, flats(rows[at : at + 1, :]))]
            ghosts.append(pair[1][7:8] + spread[at : at + 1, :])
            tile = jnp.zeros((8, 128), f32)
            for i, row in enumerate(ghosts):
                tile = jnp.where(sub == i, row, tile)
            for half in range(2):
                code = table[ROW_ROUTE, j * 4 + side * 2 + half] - 1
                used = code >= 0
                code = jnp.maximum(code, 0)
                plane = held[(code >> 2) & 15, pl.ds(pl.multiple_of(40 + (code & 3) * 8, 8), 8)]
                if half == 0:
                    out[j, 32 + side * 8 : 40 + side * 8] = jnp.where((sub < 6) & used, plane, tile)
                elif side == 1:
                    out[j, 48:56] = plane
                else:
                    between = pl.ds(pl.multiple_of((code >> 6) * 8, 8), 8)
                    inner = (sub >= 1) & (sub <= 6) & used
                    out[j, between] = jnp.where(inner, pltpu.roll(plane, 1, 0), out[j, between])


def update_kernel(
    table, rcv, fine_ref, visc_ref, along_x, faces, ends, pool,
    fine_out, means_out,
    sums, planes, advanced, pooled, kept, sem,
):
    me = lax.axis_index("gx_1")
    gx = (jnp.maximum(table[ROW_HOME, me] - 1, 0) & 127) >> 2
    at_home, at_low, at_high = gx & 7, (gx + 7) & 7, (gx + 1) & 7
    sub8 = lax.broadcasted_iota(i32, (8, 1), 0)

    low = jnp.where(gx > 0, rcv[at_low, 32:40], 0.0)
    high = jnp.where(gx < 31, rcv[at_high, 40:48], 0.0)
    beyond = jnp.where(sub8 == 0, low[6:7], jnp.where(sub8 == 1, high[6:7], 0.0))
    body = jnp.concatenate([rcv[at_home, 0:32], beyond], axis=0)
    sums[...] = dot_right(dot_left(along_x[...], body), faces[...])
    own = (rcv[at_home, 32:40], rcv[at_home, 40:48])
    flat = jnp.zeros((8, 128), f32)
    for side, other in enumerate((low, high)):
        for k in range(3):
            flat = jnp.where(sub8 == 3 * side + k, own[side][k : k + 1] + other[3 + k : 4 + k], flat)
    planes[...] = dot_right(flat, ends[...])
    lane = lax.broadcasted_iota(i32, (1, F * F), 1)
    sub = lax.broadcasted_iota(i32, (F, 1), 0)
    lane_z = lane & (F - 1)
    for s in range(SLOTS):
        word = table[ROW_SLOT, me * 4 + s]
        active = (word & 1) == 1
        box_start = pl.multiple_of(((word >> 1) & 3) * F, F)
        low_word = table[ROW_LOW, me * 4 + s]
        high_word = table[ROW_HIGH, me * 4 + s]
        second = (low_word & 7) == 6
        low_at = jnp.where(second, (((word >> 1) & 3) + 3) & 3, 4) * 8
        low_tile = rcv[low_word >> 4, pl.ds(pl.multiple_of(low_at, 8), 8)]
        low_tile = jnp.where(second, pltpu.roll(low_tile, 7, 0), low_tile)
        high_at = jnp.where((high_word & 15) == 14, 48, 40)
        high_tile = rcv[high_word >> 4, pl.ds(pl.multiple_of(high_at, 8), 8)]
        visc = step_rate * visc_ref[s * F : s * F + F, :]
        for k in range(3):
            row = (k * SLOTS + s) * F
            cells = fine_ref[row : row + F, :]
            lower = jnp.concatenate([low_tile[k : k + 1], low_tile[3 + k : 4 + k]], axis=1)
            upper = jnp.concatenate([high_tile[k : k + 1], high_tile[3 + k : 4 + k]], axis=1)
            low_row = pl.multiple_of((k * SLOTS + ((low_word >> 2) & 3)) * F + 8, 8)
            high_row = pl.multiple_of((k * SLOTS + ((high_word >> 2) & 3)) * F, 8)
            lower = jnp.where((low_word & 3) == 1, fine_ref[pl.ds(low_row, 8), :][7:8], lower)
            upper = jnp.where((high_word & 3) == 1, fine_ref[pl.ds(high_row, 8), :][0:1], upper)
            lower = jnp.where(low_word > 0, lower, planes[k : k + 1, :])
            upper = jnp.where(high_word > 0, upper, planes[3 + k : 4 + k, :])
            total = sums[pl.ds(box_start, F), k * 256 : k * 256 + 256] - 6.0 * cells
            total = total + jnp.where(sub == 0, lower, pltpu.roll(cells, 1, 0))
            total = total + jnp.where(sub == F - 1, upper, pltpu.roll(cells, F - 1, 0))
            total = total + jnp.where(lane < F, 0.0, pltpu.roll(cells, F, 1))
            total = total + jnp.where(lane >= F * F - F, 0.0, pltpu.roll(cells, F * F - F, 1))
            total = total + jnp.where(lane_z == 0, 0.0, pltpu.roll(cells, 1, 1))
            total = total + jnp.where(lane_z == F - 1, 0.0, pltpu.roll(cells, F * F - 1, 1))
            result = cells + visc * total
            kept[row : row + F, :] = jnp.where(active, result, 0.0)
            at = s * 48 + k * F
            advanced[at : at + F, :] = result
    store = pltpu.make_async_copy(kept, fine_out, sem)
    store.start()
    for p in range(2):
        at = p * 96
        pooled[p * 48 : p * 48 + 48, :] = dot_right(advanced[at : at + 48, :], pool[0]) + dot_right(
            advanced[at + 48 : at + 96, :], pool[1]
        )
    means = pooled[pl.ds(0, 48, stride=2), :] + pooled[pl.ds(1, 48, stride=2), :]
    for j in range(PLANE):
        means_out[j] = means
    store.wait()


def return_kernel(table, held, out):
    first = lax.broadcasted_iota(i32, (1, 128), 1) < 64
    for j in range(LINE_Z):
        for p in range(2):
            picks = []
            for h in range(2):
                x, _, y, local = split_slot(jnp.maximum(table[ROW_OWNER, j * 4 + 2 * p + h] - 1, 0))
                start = pl.multiple_of((local >> 1) * 24, 8)
                rows = held[x * LINE_Y + y, pl.ds(start, 24)]
                picks.append(jnp.where((local & 1) == h, rows, pltpu.roll(rows, 64, 1)))
            out[j, p * 24 : p * 24 + 24] = jnp.where(first, picks[0], picks[1])


def place_kernel(table, rcv, window, coarse_ref, coarse_out, spread, sem):
    me = lax.axis_index("gx_1")
    place = table[ROW_ANCHOR, SELF_TARGET]

    @pl.when(place >= 0)
    def _():
        y0 = pl.multiple_of(place >> 8, 8)
        z0 = place & 255
        z_tile = pl.multiple_of((z0 >> 7) * 128, 128)
        z_in = z0 & 127
        lane = lax.broadcasted_iota(i32, (1, 128), 1)
        owners = [split_slot(jnp.maximum(table[ROW_OWNER, me * 4 + i] - 1, 0))[1] for i in range(SLOTS)]
        stores = []
        for k in range(3):
            for i in range(SLOTS):
                start = ((i // 2) * 3 + k) * 8
                values = rcv[owners[i], start : start + 8]
                for b in range(B):
                    shift = (z_in + 256 - (b * B + 64 * (i % 2))) & 127
                    spread[pl.ds((k * 32 + i * B) * B + b, B, stride=B), :] = pltpu.roll(values, shift, 1)
            rows = pl.ds(k * 256, 256)
            spread[rows, :] = jnp.where((lane >= z_in) & (lane < z_in + B), spread[rows, :], window[rows, :])
            part = pl.ds(k * 32, 32)
            stores.append(
                pltpu.make_async_copy(
                    spread.reshape(96, 8, 128).at[part],
                    coarse_out.at[part, pl.ds(y0, 8), pl.ds(z_tile, 128)],
                    sem.at[k],
                )
            )
            stores[-1].start()
        for store in stores:
            store.wait()


def vmem():
    return pl.BlockSpec(memory_space=pltpu.VMEM)


def smem():
    return pl.BlockSpec(memory_space=pltpu.SMEM)


def anywhere():
    return pl.BlockSpec(memory_space=pl.ANY)


def shape(*dims, dtype=f32):
    return jax.ShapeDtypeStruct(dims, dtype)


def on_device(coarse_field, fine_field, viscosity, corners, grid_slot, neighbors):
    fine = fine_field.reshape(3 * SLOTS * F, F * F)
    tiles = coarse_field.reshape(3, 32, 4, 8, 2, 128).transpose(0, 1, 2, 4, 3, 5).reshape(6144, 128)
    pack_const, beside = map(jnp.asarray, pack_constants())
    beside = beside.astype(jnp.bfloat16)
    table, other, planes = pl.pallas_call(
        pack_kernel,
        out_shape=(shape(8, 128, dtype=i32), shape(PACKED, 128), shape(32, 128)),
        in_specs=[vmem()] * 6,
        out_specs=(vmem(),) * 3,
        scratch_shapes=[pltpu.SMEM((8, 128), i32), pltpu.SemaphoreType.DMA(())],
        name="pack",
        compiler_params=pltpu.CompilerParams(vmem_limit_bytes=24 << 20),
    )(corners.T, grid_slot[None, :], neighbors.T, fine, tiles, pack_const)
    other = lax.ppermute(other, "gz", [(0, 1), (1, 0)])
    own, window = pl.pallas_call(
        pack_own_kernel,
        out_shape=(shape(PACKED, 128), shape(768, 128)),
        in_specs=[smem(), vmem(), vmem()],
        out_specs=(vmem(),) * 2,
        name="pack_own",
        compiler_params=pltpu.CompilerParams(vmem_limit_bytes=24 << 20),
        cost_estimate=pl.CostEstimate(flops=1 << 24, bytes_accessed=1 << 20, transcendentals=0),
    )(table, tiles, pack_const)
    payload = pl.pallas_call(
        join_kernel,
        out_shape=shape(PLANE, FIRST, 128),
        in_specs=[vmem()] * 3,
        out_specs=vmem(),
        name="join",
        compiler_params=pltpu.CompilerParams(vmem_limit_bytes=8 << 20),
    )(own, other, planes)
    held = lax.all_to_all(payload, ("gx_0", "gy"), 0, 0)
    routed = pl.pallas_call(
        route_kernel,
        out_shape=shape(LINE_Z, SEND, 128),
        in_specs=[smem(), vmem(), vmem()],
        out_specs=vmem(),
        scratch_shapes=[pltpu.VMEM((LINE_Z * 34, 128), f32)] * 2,
        name="route",
        compiler_params=pltpu.CompilerParams(vmem_limit_bytes=8 << 20),
    )(table, held, beside)
    received = lax.all_to_all(routed, "gx_1", 0, 0)
    fine_out, means = pl.pallas_call(
        update_kernel,
        out_shape=(shape(3 * SLOTS * F, F * F), shape(PLANE, 48, 128)),
        in_specs=[smem()] + [vmem()] * 7,
        out_specs=(anywhere(), vmem()),
        scratch_shapes=[
            pltpu.VMEM((64, 768), f32),
            pltpu.VMEM((8, 256), f32),
            pltpu.VMEM((192, 256), f32),
            pltpu.VMEM((96, 128), f32),
            pltpu.VMEM((192, 256), f32),
            pltpu.SemaphoreType.DMA(()),
        ],
        name="update", compiler_params=pltpu.CompilerParams(vmem_limit_bytes=16 << 20),
    )(table, received, fine, viscosity.reshape(SLOTS * F, F * F), *(jnp.asarray(m, jnp.bfloat16) for m in constant_matrices()))
    held_means = lax.all_to_all(means, ("gx_0", "gy"), 0, 0)
    back = pl.pallas_call(
        return_kernel,
        out_shape=shape(LINE_Z, 48, 128),
        in_specs=[smem(), vmem()],
        out_specs=vmem(),
        name="send_back", compiler_params=pltpu.CompilerParams(vmem_limit_bytes=8 << 20),
    )(table, held_means)
    returned = lax.all_to_all(back, "gx_1", 0, 0)
    coarse_out = pl.pallas_call(
        place_kernel,
        out_shape=shape(96, 32, 256),
        in_specs=[smem(), vmem(), vmem(), anywhere()],
        out_specs=anywhere(),
        input_output_aliases={3: 0},
        scratch_shapes=[pltpu.VMEM((768, 128), f32), pltpu.SemaphoreType.DMA((3,))],
        name="place", compiler_params=pltpu.CompilerParams(vmem_limit_bytes=8 << 20),
    )(table, returned, window, coarse_field.reshape(96, 32, 256))
    return fine_out.reshape(fine_field.shape), coarse_out.reshape(coarse_field.shape)


def solution(mesh):
    split = Mesh(
        mesh.devices.reshape(LINE_X, LINE_Z, mesh.shape["gy"], mesh.shape["gz"]), ("gx_0", "gx_1", "gy", "gz")
    )
    in_specs = (
        P(None, GX, "gy", "gz"),
        P(None, GX_GY_GZ, None, None),
        P(GX_GY_GZ, None, None),
        P(),
        P(),
        P(),
    )
    out_specs = (P(None, GX_GY_GZ, None, None), P(None, GX, "gy", "gz"))
    return jax.shard_map(
        on_device, mesh=split, in_specs=in_specs, out_specs=out_specs, check_vma=False
    )
```

```python
import jax
import jax.numpy as jnp
import numpy as np
from jax import lax
from jax.experimental import pallas as pl
from jax.experimental.pallas import tpu as pltpu
from jax.sharding import Mesh
from jax.sharding import PartitionSpec as P

B = 8
F = 16
SLOTS = 4
SIDE = B + 2
LINE_X = 4
LINE_Z = 8
LINE_Y = 4
PLANE = LINE_X * LINE_Y
PACKED = 80
PAIRED = 72
FIRST = 88
SEND = 56
step_rate = 0.15
f32 = jnp.float32
i32 = jnp.int32
GX = ("gx_0", "gx_1")
GX_GY_GZ = ("gx_0", "gx_1", "gy", "gz")

ROW_SLOT, ROW_HOME, ROW_LOW, ROW_HIGH, ROW_OWNER, ROW_ANCHOR, ROW_ROUTE, ROW_SENDS = range(8)
SELF_TARGET = 8


def tangent_matrix():
    fine = np.arange(F)
    coarse = np.arange(SIDE)
    center = fine // 2 + 1
    other = np.where(fine % 2 == 0, center - 1, center + 1)
    return 0.75 * (coarse[None] == center[:, None]) + 0.25 * (coarse[None] == other[:, None])


def constant_matrices():
    tangent = tangent_matrix()
    along_x = np.zeros((64, 40))
    for fine in range(64):
        center = fine // 2
        other = center - 1 if fine % 2 == 0 else center + 1
        along_x[fine, center] += 0.75
        along_x[fine, 32 if other < 0 else 33 if other > 31 else other] += 0.25
    faces = np.zeros((128, 3, F, F))
    for k in range(3):
        for c in range(SIDE):
            faces[k * 10 + c, k, 0, :] += tangent[:, c]
            faces[30 + k * 10 + c, k, F - 1, :] += tangent[:, c]
            faces[60 + k * 10 + c, k, :, 0] += tangent[:, c]
            faces[90 + k * 10 + c, k, :, F - 1] += tangent[:, c]
    ends = np.zeros((128, F * F))
    ends[: SIDE * SIDE] = np.einsum("sa,tb->abst", tangent, tangent).reshape(SIDE * SIDE, F * F)
    pool = np.zeros((2, F, F, 128))
    for y in range(F):
        for z in range(F):
            for half in range(2):
                pool[half, y, z, half * 64 + (y // 2) * B + z // 2] = 0.125
    return (
        along_x.astype(np.float32),
        faces.reshape(128, 3 * F * F).astype(np.float32),
        ends.astype(np.float32),
        pool.reshape(2, F * F, 128).astype(np.float32),
    )


def pack_constants():
    out = np.zeros((40, 128))
    for k in range(3):
        for y in range(B):
            out[k * B + y, 60 + 10 * k + 1 + y] = 1.0
            out[k * B + y, 90 + 10 * k + 1 + y] = 1.0
        out[k * B, 10 * k : 10 * k + 10] = 0.25
        out[k * B + B - 1, 30 + 10 * k : 40 + 10 * k] = 0.25
        out[24 + k, 10 * k : 10 * k + 10] = 0.75
        out[24 + k, [60 + 10 * k, 90 + 10 * k]] = 1.0
        out[27 + k, 30 + 10 * k : 40 + 10 * k] = 0.75
        out[27 + k, [69 + 10 * k, 99 + 10 * k]] = 1.0
    beside = np.zeros((128, 128))
    for face in range(2):
        for k in range(3):
            for c in range(SIDE):
                at = face * 30 + k * 10 + c
                edge = face * 9 + 10 * k
                beside[at, at] = 0.75
                beside[at, 60 + edge] = {0: 0.75, 1: 0.25}.get(c, 0.0)
                beside[at, 90 + edge] = {9: 0.75, 8: 0.25}.get(c, 0.0)
    lanes = np.arange(128)
    out[32] = np.where(lanes < 60, lanes % 10, np.where(lanes < 90, 0, np.where(lanes < 120, 9, -999)))
    out[33] = np.where(lanes < 60, -999, np.where(lanes < 90, 1, np.where(lanes < 120, 8, -999)))
    out[34] = np.where(lanes < 60, 1.0, 0.75)
    out[35] = 0.25
    return out.astype(np.float32), beside.astype(np.float32)


def thirds(values):
    high = values.astype(jnp.bfloat16)
    rest = values - high.astype(f32)
    middle = rest.astype(jnp.bfloat16)
    return high, middle, (rest - middle.astype(f32)).astype(jnp.bfloat16)


def dot_right(values, weights, pieces=2):
    parts = [jnp.dot(part, weights, preferred_element_type=f32) for part in thirds(values)[:pieces]]
    return sum(parts[1:], parts[0])


def dot_left(weights, values):
    parts = [jnp.dot(weights, part, preferred_element_type=f32) for part in thirds(values)[:2]]
    return sum(parts[1:], parts[0])


def position():
    return tuple(lax.axis_index(name) for name in GX_GY_GZ)


def make_table(corners_ref, slots_ref, near_ref, table_ref):
    my_x, my_z, my_y, my_c = position()
    cx, cy, cz = corners_ref[0:1, :], corners_ref[1:2, :], corners_ref[2:3, :]
    gs = slots_ref[0:1, :]
    grids = gs.shape[1]
    low, high = near_ref[0:1, :], near_ref[1:2, :]
    gx, gy, gz = cx >> 5, cy >> 5, cz >> 8
    box = (cx >> 3) & 3
    home = gx * LINE_Y + gy
    brick_key = (home * 2 + gz) * SLOTS + box
    word = (1 + box * 2 + home * 8 + (low + 1) * 1024).astype(f32)
    sub = lax.broadcasted_iota(i32, (32, 1), 0)
    eye = (lax.broadcasted_iota(i32, (32, 128), 0) == lax.broadcasted_iota(i32, (32, 128), 1)).astype(f32)

    def to_row(column):
        return jnp.sum(eye * column, axis=0, keepdims=True)

    def pick(match, values):
        return jnp.sum(jnp.where(match, values, 0.0), axis=1, keepdims=True)

    def device_of(j):
        return ((my_x * LINE_Z + j) * LINE_Y + my_y) * 2 + my_c

    keys = device_of(sub >> 2) * SLOTS + (sub & 3)
    held = keys == gs
    words = pick(held, word)
    high_grid = pick(held, (high + 1).astype(f32)).astype(i32)
    low_grid = words.astype(i32) >> 10
    grid_ids = lax.broadcasted_iota(i32, (1, grids), 1) + 1
    slot_plus = (gs + 1).astype(f32)
    low_slot = pick(low_grid == grid_ids, slot_plus).astype(i32)
    high_slot = pick(high_grid == grid_ids, slot_plus).astype(i32)
    devices = gs >> 2
    bit = (jnp.int32(1) << box).astype(f32)

    def boxes_on(device):
        return pick(device == devices, bit).astype(i32)

    mine = device_of(sub >> 2)
    my_mask = boxes_on(mine)
    my_box = (words.astype(i32) >> 1) & 3
    lanes = lax.broadcasted_iota(i32, (32, 128), 1)
    same_j = (sub >> 2) == (lanes >> 2)
    route_row = jnp.zeros((1, 128), f32)
    sends_row = jnp.zeros((1, 128), f32)
    near_words = []
    for side, slot in enumerate((low_slot, high_slot)):
        device = (slot - 1) >> 2
        near_mask = boxes_on(device)
        near_box = (my_box + (3, 1)[side]) & 3
        outer = (slot > 0) & (device != mine)

        def before(mask, at):
            return ((mask & ((jnp.int32(1) << at) - 1)) != 0).astype(i32)

        def after(mask, at):
            return ((mask >> (at + 1)) != 0).astype(i32)

        if side == 0:
            here, there = before(my_mask, my_box), 2 + after(near_mask, near_box)
        else:
            here, there = 2 + after(my_mask, my_box), before(near_mask, near_box)
        target = jnp.where(same_j & ((lanes & 3) == here) & outer, 1.0, 0.0)
        plane = (device >> 6) * LINE_Y + ((device >> 1) & 3)
        code = (plane * 4 + there + near_box * 64 + 1).astype(f32)
        route_row = route_row + jnp.sum(target * code, axis=0, keepdims=True)
        sends_row = sends_row + jnp.sum(target * ((sub & 3) + 1).astype(f32), axis=0, keepdims=True)
        word = jnp.where(outer, 2 + here * 4 + ((device >> 3) & 7) * 16, 1 + ((slot - 1) & 3) * 4)
        near_words.append(jnp.where(slot > 0, word, 0).astype(f32))
    owner = pick(keys == brick_key, slot_plus)
    sub8 = lax.broadcasted_iota(i32, (8, 1), 0)
    on_device = device_of(sub8) == (gs >> 2)
    in_y = cy & 31
    side_y = jnp.where(in_y == 0, 128, jnp.where(in_y == 24, 256, 0))
    homes = jnp.max(jnp.where(on_device, (home + 1 + side_y).astype(f32), 0.0), axis=1, keepdims=True)
    homes = jnp.concatenate([homes, jnp.zeros((24, 1), f32)], axis=0)
    sub24 = lax.broadcasted_iota(i32, (24, 1), 0)
    target_x = my_x * LINE_Z + my_z + jnp.where(sub24 >= 12, 1, jnp.where(sub24 >= 6, 0, -1))
    target_x = jnp.where(sub24 >= 18, -1, target_x)
    in_x = sub24 - jnp.where(sub24 >= 12, 12, jnp.where(sub24 >= 6, 6, 0))
    target_y = my_y + (in_x >> 1) - 1
    target_z = jnp.where((in_x & 1) == 0, my_c, 1 - my_c)
    near_brick = (target_x == gx) & (target_y == gy) & (target_z == gz)
    place = ((cy & 31) * 256 + (cz & 255)).astype(f32)
    anchors = jnp.max(jnp.where(near_brick, place, -1.0), axis=1, keepdims=True)
    anchors = jnp.concatenate([anchors, jnp.zeros((8, 1), f32)], axis=0)
    rows = [to_row(v) for v in (words, homes, *near_words, owner, anchors)] + [route_row, sends_row]
    for r, row in enumerate(rows):
        table_ref[r : r + 1, :] = row.astype(i32)


def pack_kernel(
    corners_ref, slots_ref, near_ref, fine_ref, brick, const, table_ref, other_ref, planes_ref, table, table_sem
):
    make_table(corners_ref, slots_ref, near_ref, table_ref)
    fetch = pltpu.make_async_copy(table_ref, table, table_sem)
    fetch.start()
    planes_ref[...] = jnp.zeros_like(planes_ref)
    fetch.wait()
    me = lax.axis_index("gx_1")
    for e in range(4):
        s = jnp.maximum(table[ROW_SENDS, me * 4 + e] - 1, 0)
        for k in range(3):
            tile = fine_ref[pl.ds(pl.multiple_of((k * SLOTS + s) * F + (0 if e < 2 else 8), 8), 8), :]
            row = tile[0:1] if e < 2 else tile[7:8]
            for half in range(2):
                at = e * 8 + half * 3 + k
                planes_ref[at : at + 1, :] = row[:, half * 128 : half * 128 + 128]

    pack_rows(table, brick, const, other_ref, None, 1)


def pack_own_kernel(table, brick, const, own_ref, window_ref):
    pack_rows(table, brick, const, own_ref, window_ref, 0)


def pack_rows(table, brick, const, out, window_ref, dz):
    out[...] = jnp.zeros_like(out)
    my_c = lax.axis_index("gz")
    lane = lax.broadcasted_iota(i32, (1, 128), 1)
    sub3 = lax.broadcasted_iota(i32, (3, 1), 0)

    def from_second(z_base):
        return z_base + ((lane - z_base) & 127) >= 128

    def window_rows(at, second):
        return jnp.where(second, brick[at(8)], brick[at(0)])

    def to_front(rows, z_base, valid):
        rows = pltpu.roll(rows, (256 - z_base) & 127, 1)
        at = z_base + lane
        return jnp.where((lane < SIDE) & (at >= 0) & (at < 256) & valid, rows, 0.0)

    def shifted(start, count, stride, z_base, valid):
        rows = window_rows(
            lambda tile: (pl.ds(start + tile, count, stride=stride), slice(None)), from_second(z_base)
        )
        return to_front(rows, z_base, valid)

    def tile_row(y):
        return (y >> 3) * 16 + (y & 7)

    def ends_of(u):
        low = 0.75 * u[:, 0:1] + 0.25 * u[:, 1:2]
        high = 0.75 * u[:, 9:10] + 0.25 * u[:, 8:9]
        return low, high

    def beside_rows(dy, z_base):
        total = jnp.zeros((32, 128), f32)
        y, face = (31, 0) if dy == 1 else (0, 30)
        for k in range(3):
            u = shifted(k * 2048 + tile_row(y), 32, 64, z_base, True)
            total = total + (pltpu.roll(u, face + 10 * k, 1) if face + k else u)
        return total

    def diagonal_row(x, dy, z_base):
        y, face = (31, 0) if dy == 1 else (0, 30)
        face += 0 if x else 60
        u = shifted(x * 64 + tile_row(y), 3, 2048, z_base, True)
        row = jnp.where(sub3 == 0, u, jnp.where(sub3 == 1, pltpu.roll(u, 10, 1), pltpu.roll(u, 20, 1)))
        row = jnp.sum(row, axis=0, keepdims=True)
        return pltpu.roll(row, face, 1) if face else row

    def all_rows(y0, z_base):
        offset = (lax.broadcasted_iota(i32, (128, 1), 0) - z_base) & 127
        offset = jnp.where((offset + z_base >= 0) & (offset + z_base < 256), offset, 500).astype(f32)
        window = jnp.where(offset == const[32:33, :], const[34:35, :], 0.0)
        window = window + jnp.where(offset == const[33:34, :], const[35:36, :], 0.0)
        start = (y0 >> 3) * 16
        low_y, high_y = jnp.maximum(y0 - 1, 0), jnp.minimum(y0 + B, 31)
        tiles = from_second(z_base)
        parts = []
        for n in range(96):
            first = n * 64 + start
            parts.append(
                window_rows(lambda tile, first=first: (pl.ds(pl.multiple_of(first + tile, 8), 8), slice(None)), tiles)
            )
        for y in (low_y, high_y):
            first = tile_row(y)
            parts.append(
                window_rows(lambda tile, first=first: (pl.ds(first + tile, 96, stride=64), slice(None)), tiles)
            )
        cells = dot_right(jnp.concatenate(parts, axis=0), window.astype(jnp.bfloat16))
        inner = cells[:768].reshape(3, 32, B, 128)
        total = inner[0] * const[0:8, :][None]
        total = total + inner[1] * const[8:16, :][None]
        total = total + inner[2] * const[16:24, :][None]
        rows = jnp.sum(total, axis=1)
        for k in range(3):
            low = jnp.where(y0 > 0, const[24 + k : 25 + k, :], 0.0)
            high = jnp.where(y0 < 24, const[27 + k : 28 + k, :], 0.0)
            rows = rows + low * cells[768 + 32 * k : 800 + 32 * k] + high * cells[864 + 32 * k : 896 + 32 * k]
        flats = []
        for x in (0, 31):
            for k in range(3):
                tile = jnp.where(lane < SIDE, cells[(k * 32 + x) * B : (k * 32 + x) * B + B], 0.0)
                flat = jnp.sum(pltpu.roll(tile, SIDE, 1, stride=SIDE, stride_axis=0), axis=0, keepdims=True)
                low = cells[768 + 32 * k + x : 769 + 32 * k + x]
                high = cells[864 + 32 * k + x : 865 + 32 * k + x]
                flat = flat + jnp.where((lane < SIDE) & (y0 > 0), low, 0.0)
                flat = flat + pltpu.roll(jnp.where((lane < SIDE) & (y0 < 24), high, 0.0), 90, 1)
                flats.append(flat)
        return rows, flats

    def edge_rows(x, y0, z_base):
        start = (y0 >> 3) * 16
        tiles = from_second(z_base)
        rows = []
        for k in range(3):
            first = (k * 32 + x) * 64 + start
            rows.append(
                window_rows(lambda tile, first=first: (pl.ds(pl.multiple_of(first + tile, 8), 8), slice(None)), tiles)
            )
        u = to_front(jnp.concatenate(rows, axis=0), z_base, True)
        low, high = ends_of(u)
        flats, faces = [], []
        for k in range(3):
            tile = u[k * B : k * B + B]
            flats.append(jnp.sum(pltpu.roll(tile, SIDE, 1, stride=SIDE, stride_axis=0), axis=0, keepdims=True))
            tile = pltpu.roll(tile, 10 * k, 1) if k else tile
            faces.append(tile + pltpu.roll(tile, 30, 1))
        spread = jnp.where(lane < 60, jnp.concatenate(faces, axis=0), jnp.where(lane < 90, low, high))
        total = jnp.sum(spread * const[0:24, :], axis=0, keepdims=True)
        flat = jnp.where(sub3 == 0, flats[0], jnp.where(sub3 == 1, flats[1], flats[2]))
        row = jnp.zeros((3, 128), f32)
        for t, y, valid in ((0, y0 - 1, y0 > 0), (SIDE - 1, y0 + B, y0 < 24)):
            u = shifted(x * 64 + tile_row(jnp.clip(y, 0, 31)), 3, 2048, z_base, valid)
            flat = flat + (pltpu.roll(u, 10 * t, 1) if t else u)
            low, high = ends_of(u)
            row = jnp.where(lane == 60 + 10 * sub3 + t, low, row)
            row = jnp.where(lane == 90 + 10 * sub3 + t, high, row)
            face = 30 if t else 0
            spread = jnp.where(
                sub3 == 0,
                pltpu.roll(u, face, 1) if face else u,
                jnp.where(sub3 == 1, pltpu.roll(u, face + 10, 1), pltpu.roll(u, face + 20, 1)),
            )
            row = row + 0.75 * spread
        return flat, total + jnp.sum(row, axis=0, keepdims=True)

    z_shift = 256 * (1 - 2 * my_c) if dz else 0
    for dy in (-1, 0, 1):
        for dx in (0, -1, 1):
            place = table[ROW_ANCHOR, (dx + 1) * 6 + (dy + 1) * 2 + dz]
            y0, z0 = place >> 8, place & 255
            z_base = z0 - 1 + z_shift
            near = place >= 0
            if dy == 1:
                near &= y0 == 0
            if dy == -1:
                near &= y0 == 24
            if dz:
                near &= z0 == jnp.where(my_c == 0, 0, 248)

            @pl.when(near)
            def _(out=out, dz=dz, dx=dx, dy=dy, y0=y0, z0=z0, z_base=z_base):
                if dy and dx:
                    out[38:39, :] += diagonal_row(0 if dx == -1 else 31, dy, z_base)
                elif dy:
                    out[48:80, :] += beside_rows(dy, z_base)
                elif dx:
                    x, at = (0, 44) if dx == -1 else (31, 40)
                    flat, row = edge_rows(x, y0, z_base)
                    out[at : at + 3, :] = 0.75 * flat
                    out[at + 3 : at + 4, :] = row
                else:
                    rows, flats = all_rows(y0, z_base)
                    out[0:32, :] = rows
                    for i, flat in enumerate(flats):
                        out[32 + i : 33 + i, :] = 0.25 * flat
                    if dz == 0:
                        start = (y0 >> 3) * 16 + (z0 >> 7) * 8
                        for n in range(96):
                            tile = brick[pl.ds(pl.multiple_of(n * 64 + start, 8), 8), :]
                            window_ref[n * 8 : n * 8 + 8, :] = tile


def split_slot(slot):
    device = slot >> 2
    return device >> 6, (device >> 3) & 7, (device >> 1) & 3, slot & 3


def join_kernel(own, other, planes, out):
    total = own[...] + other[...]
    sub = lax.broadcasted_iota(i32, (8, 1), 0)
    tiles = []
    for e in range(4):
        pair = jnp.where(sub == 6, total[40 + 2 * e : 41 + 2 * e], total[41 + 2 * e : 42 + 2 * e])
        tiles.append(jnp.where(sub < 6, planes[e * 8 : e * 8 + 8, :], pair))
    two = total[48:64] + pltpu.roll(total[64:80], 64, 1)
    payload = jnp.concatenate([total[:40]] + tiles + [two], axis=0)
    for j in range(PLANE):
        out[j] = payload


def route_kernel(table, held, beside_ref, out, rows, spread):
    sub = lax.broadcasted_iota(i32, (8, 1), 0)
    lane = lax.broadcasted_iota(i32, (1, 128), 1)

    def line_of(gx):
        return (jnp.clip(gx, 0, 31) >> 3) * LINE_Y

    def read(j):
        code = jnp.maximum(table[ROW_HOME, j] - 1, 0)
        home, edge = code & 127, code >> 7
        gx, gy = home >> 2, home & 3
        near_y = jnp.where(edge == 1, gy - 1, gy + 1)
        used = (edge > 0) & (near_y >= 0) & (near_y < LINE_Y)
        start = jnp.where(edge == 2, 30, 0)
        keep = (lane >= start) & (lane < start + 30) & used
        return gx, gy, jnp.clip(near_y, 0, LINE_Y - 1), edge, keep

    for j in range(LINE_Z):
        gx, _, near_y, _, keep = read(j)
        both = held[line_of(gx) + near_y, PAIRED:FIRST]
        rows[j * 32 : j * 32 + 16, :] = jnp.where(keep, both, 0.0)
        rows[j * 32 + 16 : j * 32 + 32, :] = jnp.where(keep, pltpu.roll(both, 64, 1), 0.0)
        for side in range(2):
            row = held[line_of(gx + (1 if side else -1)) + near_y, 32:40][6:7]
            at = LINE_Z * 32 + j * 2 + side
            rows[at : at + 1, :] = jnp.where(keep, pltpu.roll(row, 68, 1) if side else row, 0.0)
    spread[...] = dot_right(rows[...], beside_ref[...])

    for j in range(LINE_Z):
        gx, gy, _, edge, _ = read(j)
        home_at = line_of(gx) + gy
        shift = jnp.where(edge == 2, 60, 0)
        kept = (lane >= jnp.where(edge == 2, 90, 0)) & (lane < jnp.where(edge == 2, 100, SIDE))

        def flats(row):
            return [jnp.where(kept, pltpu.roll(row, (shift + 128 - 10 * k) & 127, 1), 0.0) for k in range(3)]

        out[j, 0:32] = held[home_at, 0:32] + spread[j * 32 : j * 32 + 32, :]
        ends = held[home_at, 32:40]
        for side in range(2):
            near = rows[j * 32 + 31 * side : j * 32 + 31 * side + 1, :]
            at = LINE_Z * 32 + j * 2 + side
            source = line_of(gx + (1 if side else -1)) + gy
            pair = [held[source, 40 + (side * 2 + half) * 8 : 48 + (side * 2 + half) * 8] for half in range(2)]
            ghosts = [ends[3 * side + k : 3 * side + k + 1] + 0.25 * row for k, row in enumerate(flats(near))]
            pieces = (pair[0][6:7], pair[0][7:8], pair[1][6:7])
            ghosts += [piece + 0.75 * row for piece, row in zip(pieces, flats(rows[at : at + 1, :]))]
            ghosts.append(pair[1][7:8] + spread[at : at + 1, :])
            tile = jnp.zeros((8, 128), f32)
            for i, row in enumerate(ghosts):
                tile = jnp.where(sub == i, row, tile)
            for half in range(2):
                code = table[ROW_ROUTE, j * 4 + side * 2 + half] - 1
                used = code >= 0
                code = jnp.maximum(code, 0)
                plane = held[(code >> 2) & 15, pl.ds(pl.multiple_of(40 + (code & 3) * 8, 8), 8)]
                if half == 0:
                    out[j, 32 + side * 8 : 40 + side * 8] = jnp.where((sub < 6) & used, plane, tile)
                elif side == 1:
                    out[j, 48:56] = plane
                else:
                    between = pl.ds(pl.multiple_of((code >> 6) * 8, 8), 8)
                    inner = (sub >= 1) & (sub <= 6) & used
                    out[j, between] = jnp.where(inner, pltpu.roll(plane, 1, 0), out[j, between])


def update_kernel(
    table, rcv, fine_ref, visc_ref, along_x, faces, ends, pool,
    fine_out, means_out,
    sums, planes, advanced, pooled, kept, sem,
):
    me = lax.axis_index("gx_1")
    gx = (jnp.maximum(table[ROW_HOME, me] - 1, 0) & 127) >> 2
    at_home, at_low, at_high = gx & 7, (gx + 7) & 7, (gx + 1) & 7
    sub8 = lax.broadcasted_iota(i32, (8, 1), 0)

    low = jnp.where(gx > 0, rcv[at_low, 32:40], 0.0)
    high = jnp.where(gx < 31, rcv[at_high, 40:48], 0.0)
    beyond = jnp.where(sub8 == 0, low[6:7], jnp.where(sub8 == 1, high[6:7], 0.0))
    body = jnp.concatenate([rcv[at_home, 0:32], beyond], axis=0)
    sums[...] = dot_right(dot_left(along_x[...], body), faces[...])
    own = (rcv[at_home, 32:40], rcv[at_home, 40:48])
    flat = jnp.zeros((8, 128), f32)
    for side, other in enumerate((low, high)):
        for k in range(3):
            flat = jnp.where(sub8 == 3 * side + k, own[side][k : k + 1] + other[3 + k : 4 + k], flat)
    planes[...] = dot_right(flat, ends[...])
    lane = lax.broadcasted_iota(i32, (1, F * F), 1)
    sub = lax.broadcasted_iota(i32, (F, 1), 0)
    lane_z = lane & (F - 1)
    for s in range(SLOTS):
        word = table[ROW_SLOT, me * 4 + s]
        active = (word & 1) == 1
        box_start = pl.multiple_of(((word >> 1) & 3) * F, F)
        low_word = table[ROW_LOW, me * 4 + s]
        high_word = table[ROW_HIGH, me * 4 + s]
        second = (low_word & 7) == 6
        low_at = jnp.where(second, (((word >> 1) & 3) + 3) & 3, 4) * 8
        low_tile = rcv[low_word >> 4, pl.ds(pl.multiple_of(low_at, 8), 8)]
        low_tile = jnp.where(second, pltpu.roll(low_tile, 7, 0), low_tile)
        high_at = jnp.where((high_word & 15) == 14, 48, 40)
        high_tile = rcv[high_word >> 4, pl.ds(pl.multiple_of(high_at, 8), 8)]
        visc = step_rate * visc_ref[s * F : s * F + F, :]
        for k in range(3):
            row = (k * SLOTS + s) * F
            cells = fine_ref[row : row + F, :]
            lower = jnp.concatenate([low_tile[k : k + 1], low_tile[3 + k : 4 + k]], axis=1)
            upper = jnp.concatenate([high_tile[k : k + 1], high_tile[3 + k : 4 + k]], axis=1)
            low_row = pl.multiple_of((k * SLOTS + ((low_word >> 2) & 3)) * F + 8, 8)
            high_row = pl.multiple_of((k * SLOTS + ((high_word >> 2) & 3)) * F, 8)
            lower = jnp.where((low_word & 3) == 1, fine_ref[pl.ds(low_row, 8), :][7:8], lower)
            upper = jnp.where((high_word & 3) == 1, fine_ref[pl.ds(high_row, 8), :][0:1], upper)
            lower = jnp.where(low_word > 0, lower, planes[k : k + 1, :])
            upper = jnp.where(high_word > 0, upper, planes[3 + k : 4 + k, :])
            total = sums[pl.ds(box_start, F), k * 256 : k * 256 + 256] - 6.0 * cells
            total = total + jnp.where(sub == 0, lower, pltpu.roll(cells, 1, 0))
            total = total + jnp.where(sub == F - 1, upper, pltpu.roll(cells, F - 1, 0))
            total = total + jnp.where(lane < F, 0.0, pltpu.roll(cells, F, 1))
            total = total + jnp.where(lane >= F * F - F, 0.0, pltpu.roll(cells, F * F - F, 1))
            total = total + jnp.where(lane_z == 0, 0.0, pltpu.roll(cells, 1, 1))
            total = total + jnp.where(lane_z == F - 1, 0.0, pltpu.roll(cells, F * F - 1, 1))
            result = cells + visc * total
            kept[row : row + F, :] = jnp.where(active, result, 0.0)
            at = s * 48 + k * F
            advanced[at : at + F, :] = result
    store = pltpu.make_async_copy(kept, fine_out, sem)
    store.start()
    for p in range(2):
        at = p * 96
        pooled[p * 48 : p * 48 + 48, :] = dot_right(advanced[at : at + 48, :], pool[0], 3) + dot_right(
            advanced[at + 48 : at + 96, :], pool[1], 3
        )
    means = pooled[pl.ds(0, 48, stride=2), :] + pooled[pl.ds(1, 48, stride=2), :]
    for j in range(PLANE):
        means_out[j] = means
    store.wait()


def return_kernel(table, held, out):
    first = lax.broadcasted_iota(i32, (1, 128), 1) < 64
    for j in range(LINE_Z):
        for p in range(2):
            picks = []
            for h in range(2):
                x, _, y, local = split_slot(jnp.maximum(table[ROW_OWNER, j * 4 + 2 * p + h] - 1, 0))
                start = pl.multiple_of((local >> 1) * 24, 8)
                rows = held[x * LINE_Y + y, pl.ds(start, 24)]
                picks.append(jnp.where((local & 1) == h, rows, pltpu.roll(rows, 64, 1)))
            out[j, p * 24 : p * 24 + 24] = jnp.where(first, picks[0], picks[1])


def place_kernel(table, rcv, window, coarse_ref, coarse_out, spread, sem):
    me = lax.axis_index("gx_1")
    place = table[ROW_ANCHOR, SELF_TARGET]

    @pl.when(place >= 0)
    def _():
        y0 = pl.multiple_of(place >> 8, 8)
        z0 = place & 255
        z_tile = pl.multiple_of((z0 >> 7) * 128, 128)
        z_in = z0 & 127
        lane = lax.broadcasted_iota(i32, (1, 128), 1)
        owners = [split_slot(jnp.maximum(table[ROW_OWNER, me * 4 + i] - 1, 0))[1] for i in range(SLOTS)]
        stores = []
        for k in range(3):
            for i in range(SLOTS):
                start = ((i // 2) * 3 + k) * 8
                values = rcv[owners[i], start : start + 8]
                for b in range(B):
                    shift = (z_in + 256 - (b * B + 64 * (i % 2))) & 127
                    spread[pl.ds((k * 32 + i * B) * B + b, B, stride=B), :] = pltpu.roll(values, shift, 1)
            rows = pl.ds(k * 256, 256)
            spread[rows, :] = jnp.where((lane >= z_in) & (lane < z_in + B), spread[rows, :], window[rows, :])
            part = pl.ds(k * 32, 32)
            stores.append(
                pltpu.make_async_copy(
                    spread.reshape(96, 8, 128).at[part],
                    coarse_out.at[part, pl.ds(y0, 8), pl.ds(z_tile, 128)],
                    sem.at[k],
                )
            )
            stores[-1].start()
        for store in stores:
            store.wait()


def vmem():
    return pl.BlockSpec(memory_space=pltpu.VMEM)


def smem():
    return pl.BlockSpec(memory_space=pltpu.SMEM)


def anywhere():
    return pl.BlockSpec(memory_space=pl.ANY)


def shape(*dims, dtype=f32):
    return jax.ShapeDtypeStruct(dims, dtype)


def on_device(coarse_field, fine_field, viscosity, corners, grid_slot, neighbors):
    fine = fine_field.reshape(3 * SLOTS * F, F * F)
    tiles = coarse_field.reshape(3, 32, 4, 8, 2, 128).transpose(0, 1, 2, 4, 3, 5).reshape(6144, 128)
    pack_const, beside = map(jnp.asarray, pack_constants())
    beside = beside.astype(jnp.bfloat16)
    table, other, planes = pl.pallas_call(
        pack_kernel,
        out_shape=(shape(8, 128, dtype=i32), shape(PACKED, 128), shape(32, 128)),
        in_specs=[vmem()] * 6,
        out_specs=(vmem(),) * 3,
        scratch_shapes=[pltpu.SMEM((8, 128), i32), pltpu.SemaphoreType.DMA(())],
        name="pack",
        compiler_params=pltpu.CompilerParams(vmem_limit_bytes=24 << 20),
    )(corners.T, grid_slot[None, :], neighbors.T, fine, tiles, pack_const)
    other = lax.ppermute(other, "gz", [(0, 1), (1, 0)])
    own, window = pl.pallas_call(
        pack_own_kernel,
        out_shape=(shape(PACKED, 128), shape(768, 128)),
        in_specs=[smem(), vmem(), vmem()],
        out_specs=(vmem(),) * 2,
        name="pack_own",
        compiler_params=pltpu.CompilerParams(vmem_limit_bytes=24 << 20),
        cost_estimate=pl.CostEstimate(flops=1 << 24, bytes_accessed=1 << 20, transcendentals=0),
    )(table, tiles, pack_const)
    payload = pl.pallas_call(
        join_kernel,
        out_shape=shape(PLANE, FIRST, 128),
        in_specs=[vmem()] * 3,
        out_specs=vmem(),
        name="join",
        compiler_params=pltpu.CompilerParams(vmem_limit_bytes=8 << 20),
    )(own, other, planes)
    held = lax.all_to_all(payload, ("gx_0", "gy"), 0, 0)
    routed = pl.pallas_call(
        route_kernel,
        out_shape=shape(LINE_Z, SEND, 128),
        in_specs=[smem(), vmem(), vmem()],
        out_specs=vmem(),
        scratch_shapes=[pltpu.VMEM((LINE_Z * 34, 128), f32)] * 2,
        name="route",
        compiler_params=pltpu.CompilerParams(vmem_limit_bytes=8 << 20),
    )(table, held, beside)
    received = lax.all_to_all(routed, "gx_1", 0, 0)
    fine_out, means = pl.pallas_call(
        update_kernel,
        out_shape=(shape(3 * SLOTS * F, F * F), shape(PLANE, 48, 128)),
        in_specs=[smem()] + [vmem()] * 7,
        out_specs=(anywhere(), vmem()),
        scratch_shapes=[
            pltpu.VMEM((64, 768), f32),
            pltpu.VMEM((8, 256), f32),
            pltpu.VMEM((192, 256), f32),
            pltpu.VMEM((96, 128), f32),
            pltpu.VMEM((192, 256), f32),
            pltpu.SemaphoreType.DMA(()),
        ],
        name="update", compiler_params=pltpu.CompilerParams(vmem_limit_bytes=16 << 20),
    )(table, received, fine, viscosity.reshape(SLOTS * F, F * F), *(jnp.asarray(m, jnp.bfloat16) for m in constant_matrices()))
    held_means = lax.all_to_all(means, ("gx_0", "gy"), 0, 0)
    back = pl.pallas_call(
        return_kernel,
        out_shape=shape(LINE_Z, 48, 128),
        in_specs=[smem(), vmem()],
        out_specs=vmem(),
        name="send_back", compiler_params=pltpu.CompilerParams(vmem_limit_bytes=8 << 20),
    )(table, held_means)
    returned = lax.all_to_all(back, "gx_1", 0, 0)
    coarse_out = pl.pallas_call(
        place_kernel,
        out_shape=shape(96, 32, 256),
        in_specs=[smem(), vmem(), vmem(), anywhere()],
        out_specs=anywhere(),
        input_output_aliases={3: 0},
        scratch_shapes=[pltpu.VMEM((768, 128), f32), pltpu.SemaphoreType.DMA((3,))],
        name="place", compiler_params=pltpu.CompilerParams(vmem_limit_bytes=8 << 20),
    )(table, returned, window, coarse_field.reshape(96, 32, 256))
    return fine_out.reshape(fine_field.shape), coarse_out.reshape(coarse_field.shape)


def solution(mesh):
    split = Mesh(
        mesh.devices.reshape(LINE_X, LINE_Z, mesh.shape["gy"], mesh.shape["gz"]), ("gx_0", "gx_1", "gy", "gz")
    )
    in_specs = (
        P(None, GX, "gy", "gz"),
        P(None, GX_GY_GZ, None, None),
        P(GX_GY_GZ, None, None),
        P(),
        P(),
        P(),
    )
    out_specs = (P(None, GX_GY_GZ, None, None), P(None, GX, "gy", "gz"))
    return jax.shard_map(
        on_device, mesh=split, in_specs=in_specs, out_specs=out_specs, check_vma=False
    )
```
